512 devices in a mesh: elem: 128 (over z, y, core), bucket: 4 (over x).
Axes of the slice: x: 4, y: 8, z: 8, core: 2. Of those that a mesh axis runs over, the one named last changes fastest.
Arguments:
- node_data: float32 [24, 1572864], P(None, 'elem'), may hold values from -6 to 6
- eroded: int32 [65536], P('elem'), may hold values from 0 to 2047, as said below
- bucket_map: int32 [1572864], P('elem'), may hold values from 0 to 1023, as said below
- seg_point: float32 [1024, 3, 512], P('elem', None, 'bucket'), may hold values from -3 to 3
- seg_angle: float32 [1024, 2, 512], P('elem', None, 'bucket'), may hold values from -3.140625 to 3.140625
Outputs:
- face_force: float32 [3, 393216], P(None, 'elem')
The draws below stay inside these ranges and needn't reach their ends.
Inputs may be any that keep to these rules, and one draw needn't show every extreme that they name: `eroded`: the 512 entries of one index of elem are distinct local element numbers. `bucket_map`: among the faces of the elements listed in eroded, those of one index of elem name one bucket at most 5 times; in every draw some bucket is named exactly 5 times by every index of elem.
All inputs are finite; a program needn't handle non-finite values.
Results may differ from the reference program's by a relative error of at most 0.00012.
Values sent between devices are 32-bit elements; how exact they have to be, the bound alone decides.
No kernel may reach another device: no remote copies, remote signals or barrier semaphores. Data moves between devices by JAX's collectives and lax.ppermute only.
A program may use at most 64 MiB of HBM per device.

```python
import jax
import jax.numpy as jnp
from jax import lax

ELEM_DEV = 2048
ERODE_DEV = 512
SLOT = 5
BUCKETS = 1024
SEGS = 512
FACES = 1572864
UNCOVERED = 393216
N_ELEM = 128


def erosion_plan(key):
    plan_key = jax.random.fold_in(key, 11)
    elem_key, pool_key, hot_key, fill_key = jax.random.split(plan_key, 4)
    elem_iota = jnp.arange(ELEM_DEV, dtype=jnp.int32)
    elem_scores = jax.random.randint(elem_key, (N_ELEM, ELEM_DEV), 0, 65536, dtype=jnp.int32) * ELEM_DEV + elem_iota[None, :]
    eroded = jnp.argsort(elem_scores, axis=1)[:, :ERODE_DEV].astype(jnp.int32)
    pool_size = BUCKETS * SLOT
    pool_iota = jnp.arange(pool_size, dtype=jnp.int32)
    pool_ids = pool_iota // SLOT
    hot_bucket = jax.random.randint(hot_key, (), 0, BUCKETS, dtype=jnp.int32)
    scores = jax.random.randint(pool_key, (N_ELEM, pool_size), 0, 65536, dtype=jnp.int32) * pool_size + pool_iota[None, :]
    scores = jnp.where((pool_ids == hot_bucket)[None, :], pool_iota[None, :] - pool_size, scores)
    pool_order = jnp.argsort(scores, axis=1)[:, :6 * ERODE_DEV]
    chosen = pool_ids[pool_order].astype(jnp.int32)
    background = jax.random.randint(fill_key, (N_ELEM, 6 * ELEM_DEV), 0, BUCKETS, dtype=jnp.int32)
    sides = jnp.arange(6, dtype=jnp.int32)
    face_index = (6 * eroded[:, :, None] + sides[None, None, :]).reshape(N_ELEM, 6 * ERODE_DEV)
    device_rows = jnp.broadcast_to(jnp.arange(N_ELEM, dtype=jnp.int32)[:, None], face_index.shape)
    bucket_map = background.at[device_rows, face_index].set(chosen)
    return (eroded.reshape(-1), bucket_map.reshape(-1))


def draw_eroded(key, part):
    return erosion_plan(key)[0]


def draw_bucket_map(key, part):
    return erosion_plan(key)[1]


def level_of(stream_key, dims, cuts, least, top_value):
    level = 1.0
    for axis_at, shards_of in cuts:
        heights = jax.random.uniform(jax.random.fold_in(jax.random.fold_in(stream_key, 6), axis_at), (shards_of,), jnp.float32, least / len(cuts), top_value / len(cuts))
        level = level * jnp.repeat(jnp.exp(heights), dims[axis_at] // shards_of).reshape((-1,) + (1,) * (len(dims) - 1 - axis_at))
    return level


def normal_values(own_key, shape, deviation, most, shards=(), held_as=jnp.bfloat16):
    factor_of = level_of(own_key, shape, shards, -0.22, 0.18) if shards else 1.0
    entries = jax.random.normal(own_key, shape, jnp.float32) * deviation * factor_of
    return jnp.minimum(jnp.maximum(entries, -most), most).astype(held_as)


def setup_inputs(seed: int = 0) -> dict:
    key_list = jax.random.split(jax.random.key(seed), 6)
    node_data = normal_values(key_list[0], (24, FACES), 1.0, 6.0, ((1, 128),), jnp.float32)
    eroded = draw_eroded(jax.random.fold_in(key_list[5], 71), 0)
    bucket_map = draw_bucket_map(jax.random.fold_in(key_list[5], 71), 0)
    seg_point = normal_values(key_list[3], (BUCKETS, 3, SEGS), 0.5, 3.0, ((0, 128), (2, 4)), jnp.float32)
    seg_angle = jnp.clip(jax.random.uniform(key_list[4], (BUCKETS, 2, SEGS), jnp.float32, -3.140625, 3.140625), -3.140625, 3.140625)
    return dict(node_data=node_data, eroded=eroded, bucket_map=bucket_map, seg_point=seg_point, seg_angle=seg_angle)


STIFFNESS = 20.0
DAMPING = 0.5

def face_geometry(payload):
    corner = payload[0:12].reshape(4, 3, -1)
    motion = payload[12:24].reshape(4, 3, -1)
    centroid = 0.25 * (corner[0] + corner[1] + corner[2] + corner[3])
    first_edge = corner[2] - corner[0]
    second_edge = corner[3] - corner[1]
    area_x = 0.5 * (first_edge[1] * second_edge[2] - first_edge[2] * second_edge[1])
    area_y = 0.5 * (first_edge[2] * second_edge[0] - first_edge[0] * second_edge[2])
    area_z = 0.5 * (first_edge[0] * second_edge[1] - first_edge[1] * second_edge[0])
    velocity = 0.25 * (motion[0] + motion[1] + motion[2] + motion[3])
    return jnp.concatenate([centroid, jnp.stack([area_x, area_y, area_z]), velocity], axis=0)

def unit_normal(angles):
    return jnp.stack([jnp.cos(angles[:, 0]) * jnp.sin(angles[:, 1]), jnp.sin(angles[:, 0]) * jnp.sin(angles[:, 1]), jnp.cos(angles[:, 1])], axis=1)

def penalty_terms(geometry, point, normal, stiff):
    offset = geometry[0:3, :, None] - point
    dist_sq = offset[0] * offset[0] + offset[1] * offset[1] + offset[2] * offset[2]
    gap_value = offset[0] * normal[0] + offset[1] * normal[1] + offset[2] * normal[2]
    closing = geometry[6][:, None] * normal[0] + geometry[7][:, None] * normal[1] + geometry[8][:, None] * normal[2]
    projected = jnp.abs(geometry[3][:, None] * normal[0] + geometry[4][:, None] * normal[1] + geometry[5][:, None] * normal[2])
    depth_in = jnp.maximum(-gap_value, 0.0)
    weight = jnp.exp(-0.5 * dist_sq)
    return weight * depth_in * (stiff - DAMPING * closing) * projected

def reference(node_data, eroded, bucket_map, seg_point, seg_angle):
    local = eroded.reshape(N_ELEM, ERODE_DEV)
    sides = jnp.arange(6, dtype=jnp.int32)
    face_local = (6 * local[:, :, None] + sides[None, None, :]).reshape(N_ELEM, 6 * ERODE_DEV)
    offsets = (jnp.arange(N_ELEM, dtype=jnp.int32) * (6 * ELEM_DEV)).astype(jnp.int32)
    face_global = (face_local + offsets[:, None]).reshape(-1).astype(jnp.int32)
    bucket = bucket_map[face_global]
    geometry = face_geometry(node_data[:, face_global])
    counts = jnp.zeros((BUCKETS,), jnp.float32).at[bucket].add(1.0)
    stiffness = STIFFNESS * lax.rsqrt(jnp.maximum(counts, 1.0))
    normal_all = unit_normal(seg_angle)
    block_count = UNCOVERED // 128
    geo_blocks = geometry.reshape(9, block_count, 128).transpose(1, 0, 2)
    id_blocks = bucket.reshape(block_count, 128)

    def block_force(items):
        geo, block_ids = items
        point = seg_point[block_ids].transpose(1, 0, 2)
        normal = normal_all[block_ids].transpose(1, 0, 2)
        stiff = stiffness[block_ids][:, None]
        traction = penalty_terms(geo, point, normal, stiff)
        return lax.optimization_barrier(jnp.sum(traction[None, :, :] * normal, axis=2))
    forces = lax.map(block_force, (geo_blocks, id_blocks))
    return forces.transpose(1, 0, 2).reshape(3, UNCOVERED)
```

```python
import jax
import jax.numpy as jnp
from jax import lax
from jax.experimental import pallas as pl
from jax.experimental.pallas import tpu as pltpu
from jax.sharding import PartitionSpec as P

STIFFNESS = 20.0
DAMPING = 0.5
SLOTS = 5
LANES = 128
F32 = jnp.float32
BF16 = jnp.bfloat16
NT = (((1,), (1,)), ((), ()))


def one_hot(row, size):
    numbers = lax.broadcasted_iota(jnp.int32, (size, row.shape[1]), 0)
    return jnp.where(numbers == row, 1.0, 0.0).astype(BF16)


def pack_kernel(eroded_ref, map_ref, node_hbm, out_ref, code_ref, node_ref, row_ref, lo_hot, col_ref,
                rank_ref, slot_ref, left_ref, right_ref, sum_ref, geo_ref, sem):
    copy = pltpu.make_async_copy(node_hbm, node_ref, sem)
    copy.start()
    group = lax.axis_index("bucket")
    blocks = map_ref.shape[0]
    count = row_ref.shape[1]
    rows4 = eroded_ref.shape[0]
    span = count // rows4

    eroded = eroded_ref[...]
    lane = lax.broadcasted_iota(jnp.int32, (LANES, span), 1)
    six = 6 * lax.broadcasted_iota(jnp.int32, (LANES, span), 0)
    spread = jnp.where((lane >= six) & (lane < six + 6), 1.0, 0.0).astype(BF16)
    high = jnp.dot((eroded >> 3).astype(F32).astype(BF16), spread, preferred_element_type=F32)
    low = jnp.dot((eroded & 7).astype(F32).astype(BF16), spread, preferred_element_type=F32)
    number = lax.broadcasted_iota(jnp.int32, (rows4, span), 1)
    faces4 = 6 * (high * 8.0 + low).astype(jnp.int32) + number % 6
    for a in range(rows4):
        row_ref[0:1, a * span:(a + 1) * span] = faces4[a:a + 1, :]

    buckets = map_ref[...]
    digits = jnp.concatenate([(buckets >> 3).astype(F32), (buckets & 7).astype(F32)], axis=0).astype(BF16)
    step = 512
    for c in range(count // step):
        face = row_ref[0:1, c * step:(c + 1) * step]
        hot = one_hot(face & (LANES - 1), LANES)
        lo_hot[:, c * step:(c + 1) * step] = hot
        both = jnp.dot(digits, hot, preferred_element_type=F32)
        value = both[:blocks] * 8.0 + both[blocks:]
        numbers = lax.broadcasted_iota(jnp.int32, (blocks, step), 0)
        rank_ref[0:1, c * step:(c + 1) * step] = jnp.sum(
            jnp.where(numbers == (face >> 7), value, 0.0), axis=0, keepdims=True)

    tiles = count // LANES
    for t in range(tiles):
        mine = rank_ref[0:1, t * LANES:(t + 1) * LANES]
        col_ref[t * LANES:(t + 1) * LANES, :] = jnp.broadcast_to(mine, (LANES, LANES)).T
    earlier = (lax.broadcasted_iota(jnp.int32, (LANES, LANES), 0)
               < lax.broadcasted_iota(jnp.int32, (LANES, LANES), 1))
    for t in range(tiles):
        mine = rank_ref[0:1, t * LANES:(t + 1) * LANES]

        def same(block, total, mine=mine):
            other = col_ref[pl.ds(pl.multiple_of(block * LANES, LANES), LANES), :]
            hit = jnp.where(other == mine, 1.0, 0.0)
            return total + jnp.sum(hit.reshape(LANES // 8, 8, LANES), axis=0)

        total = lax.fori_loop(0, t, same, jnp.zeros((8, LANES), F32))
        other = col_ref[t * LANES:(t + 1) * LANES, :]
        hit = jnp.where((other == mine) & earlier, 1.0, 0.0)
        total = total + jnp.sum(hit.reshape(LANES // 8, 8, LANES), axis=0)
        rank_ref[1:2, t * LANES:(t + 1) * LANES] = jnp.sum(total, axis=0, keepdims=True)

    bucket = rank_ref[0:1, :].astype(jnp.int32)
    rank = rank_ref[1:2, :]
    owner = bucket >> 3
    inner = bucket & 7
    code_ref[0:1, :] = owner
    code_ref[1:2, :] = inner * SLOTS + rank.astype(jnp.int32)
    column = jnp.where((inner >> 1) == group, (inner & 1) * LANES + owner + 1, 0).astype(F32)
    placed = jnp.zeros((2 * blocks, LANES), F32)
    for c in range(count // step):
        at = slice(c * step, (c + 1) * step)
        face = row_ref[0:1, at]
        numbers = lax.broadcasted_iota(jnp.int32, (blocks, step), 0)
        mine = numbers == (face >> 7)
        left = jnp.concatenate(
            [jnp.where(mine, column[:, at], 0.0), jnp.where(mine, rank[:, at], 0.0)], axis=0).astype(BF16)
        placed = placed + lax.dot_general(left, lo_hot[:, at], NT, preferred_element_type=F32)
    slot_ref[...] = placed

    copy.wait()
    left_ref[5 * 48:, :] = jnp.ones((16, left_ref.shape[1]), BF16)
    sum_ref[...] = jnp.zeros(sum_ref.shape, F32)
    per = left_ref.shape[1] // LANES

    def pack(chunk, carry):
        for t in range(per):
            block = chunk * per + t
            lanes = pl.ds(pl.multiple_of(block * LANES, LANES), LANES)
            at = slice(t * LANES, (t + 1) * LANES)
            col = slot_ref[pl.ds(block, 1), :]
            order = slot_ref[pl.ds(blocks + block, 1), :]
            numbers = lax.broadcasted_iota(jnp.int32, (256, LANES), 0).astype(F32) + 1.0
            right_ref[:, at] = jnp.where(numbers == col, 1.0, 0.0).astype(BF16)
            node = node_ref[:, lanes]
            first = node.astype(BF16).astype(F32)
            pieces = jnp.concatenate([first, node - first], axis=0)
            for k in range(SLOTS):
                left_ref[k * 48:(k + 1) * 48, at] = jnp.where(order == float(k), pieces, 0.0).astype(BF16)
        sum_ref[...] += lax.dot_general(left_ref[...], right_ref[...], NT, preferred_element_type=F32)
        return carry

    lax.fori_loop(0, blocks // per, pack, 0)

    col_ref[0:LANES, :] = jnp.zeros((LANES, LANES), F32)
    for par in range(2):
        at = slice(par * LANES, (par + 1) * LANES)
        for k in range(SLOTS):
            geo_ref[k * 24:(k + 1) * 24, :] = (
                sum_ref[k * 48:k * 48 + 24, at] + sum_ref[k * 48 + 24:k * 48 + 48, at])
        row = [geo_ref[pl.ds(r, SLOTS, stride=24), :] for r in range(24)]
        corner = [row[3 * m:3 * m + 3] for m in range(4)]
        motion = [row[12 + 3 * m:15 + 3 * m] for m in range(4)]
        centroid = [0.25 * (corner[0][i] + corner[1][i] + corner[2][i] + corner[3][i]) for i in range(3)]
        one = [corner[2][i] - corner[0][i] for i in range(3)]
        two = [corner[3][i] - corner[1][i] for i in range(3)]
        area = [
            0.5 * (one[1] * two[2] - one[2] * two[1]),
            0.5 * (one[2] * two[0] - one[0] * two[2]),
            0.5 * (one[0] * two[1] - one[1] * two[0]),
        ]
        velocity = [0.25 * (motion[0][i] + motion[1][i] + motion[2][i] + motion[3][i]) for i in range(3)]
        for q, value in enumerate(centroid + area + velocity):
            start = par * 64 + q * SLOTS
            col_ref[start:start + SLOTS, :] = value
        col_ref[par * 64 + 45:par * 64 + 46, :] = sum_ref[240:241, at]
    out_ref[...] = col_ref[0:LANES, :].T


def force_kernel(face_ref, seg_ref, out_ref, row_ref, wide_ref):
    row_ref[...] = face_ref[...].T
    groups = seg_ref.shape[0] // 2
    for g in range(2 * groups):
        columns = seg_ref[g].T
        for q in range(6):
            wide_ref[g % 2, q, (g // 2) * LANES:(g // 2 + 1) * LANES, :] = jnp.broadcast_to(
                columns[:, q:q + 1], (LANES, LANES))
    out_ref[...] = jnp.zeros(out_ref.shape, F32)
    chunk = 64
    for par in range(2):
        count = jnp.sum(row_ref[par * 64 + 45:par * 64 + 46, :], axis=1, keepdims=True)
        stiff = jnp.broadcast_to(STIFFNESS * lax.rsqrt(jnp.maximum(count, 1.0)), (1, LANES))
        for k in range(SLOTS):
            geo = [row_ref[par * 64 + q * SLOTS + k:par * 64 + q * SLOTS + k + 1, :] for q in range(9)]

            def pairs(step, total, par=par, geo=geo, stiff=stiff):
                at = pl.ds(pl.multiple_of(step * chunk, chunk), chunk)
                seg = [wide_ref[par, q, at, :] for q in range(6)]
                normal = seg[3:6]
                off = [geo[i] - seg[i] for i in range(3)]
                dist_sq = off[0] * off[0] + off[1] * off[1] + off[2] * off[2]
                gap = off[0] * normal[0] + off[1] * normal[1] + off[2] * normal[2]
                closing = geo[6] * normal[0] + geo[7] * normal[1] + geo[8] * normal[2]
                projected = jnp.abs(geo[3] * normal[0] + geo[4] * normal[1] + geo[5] * normal[2])
                weight = jnp.exp(-0.5 * dist_sq)
                traction = weight * jnp.maximum(-gap, 0.0) * (stiff - DAMPING * closing) * projected
                return tuple(
                    total[i] + jnp.sum((traction * normal[i]).reshape(chunk // 8, 8, LANES), axis=0)
                    for i in range(3))

            zero = jnp.zeros((8, LANES), F32)
            total = lax.fori_loop(0, wide_ref.shape[2] // chunk, pairs, (zero, zero, zero))
            for i in range(3):
                force = jnp.sum(total[i], axis=0, keepdims=True)
                for x in range(out_ref.shape[0]):
                    out_ref[x, i * 10 + par * SLOTS + k:i * 10 + par * SLOTS + k + 1, :] = force


def pick_kernel(force_ref, code_ref, out_ref, row_ref):
    turned = force_ref[...].T
    for x in range(4):
        for i in range(3):
            row_ref[i * 40 + x * 10:i * 40 + x * 10 + 10, :] = turned[x * 32 + i * 10:x * 32 + i * 10 + 10, :]
    value = row_ref[...]
    first = value.astype(BF16)
    second = (value - first.astype(F32)).astype(BF16)
    left = jnp.concatenate([first.astype(F32), second.astype(F32)], axis=0).astype(BF16)
    rows = value.shape[0]
    step = 512
    for c in range(out_ref.shape[1] // step):
        at = slice(c * step, (c + 1) * step)
        hot = one_hot(code_ref[0:1, at], LANES)
        both = jnp.dot(left, hot, preferred_element_type=F32)
        found = both[:rows] + both[rows:]
        mine = lax.broadcasted_iota(jnp.int32, (40, step), 0) == code_ref[1:2, at]
        for i in range(3):
            out_ref[i:i + 1, at] = jnp.sum(
                jnp.where(mine, found[i * 40:(i + 1) * 40], 0.0), axis=0, keepdims=True)


def local(node_data, eroded, bucket_map, seg_point, seg_angle):
    owners = lax.axis_size("elem")
    groups = lax.axis_size("bucket")
    faces = node_data.shape[1]
    blocks = faces // LANES
    uncovered = 6 * eroded.shape[0]
    vmem = pl.BlockSpec(memory_space=pltpu.VMEM)

    azimuth, polar = seg_angle[:, 0], seg_angle[:, 1]
    normal = jnp.stack(
        [jnp.cos(azimuth) * jnp.sin(polar), jnp.sin(azimuth) * jnp.sin(polar), jnp.cos(polar)], axis=1)
    segs = jnp.concatenate([seg_point, normal, jnp.zeros_like(seg_angle)], axis=1)
    segs = lax.all_to_all(segs, "bucket", 0, 0, tiled=True)

    packed, code = pl.pallas_call(
        pack_kernel,
        out_shape=(
            jax.ShapeDtypeStruct((owners, LANES), F32),
            jax.ShapeDtypeStruct((2, uncovered), jnp.int32),
        ),
        in_specs=[vmem, vmem, pl.BlockSpec(memory_space=pl.ANY)],
        out_specs=(vmem, vmem),
        scratch_shapes=[
            pltpu.VMEM((24, faces), F32),
            pltpu.VMEM((1, uncovered), jnp.int32),
            pltpu.VMEM((LANES, uncovered), BF16),
            pltpu.VMEM((uncovered, LANES), F32),
            pltpu.VMEM((2, uncovered), F32),
            pltpu.VMEM((2 * blocks, LANES), F32),
            pltpu.VMEM((256, 8 * LANES), BF16),
            pltpu.VMEM((256, 8 * LANES), BF16),
            pltpu.VMEM((256, 256), F32),
            pltpu.VMEM((120, LANES), F32),
            pltpu.SemaphoreType.DMA,
        ],
        name="pack",
    )(eroded.reshape(-1, LANES), bucket_map.reshape(blocks, LANES), node_data)

    arrived = lax.all_to_all(packed.reshape(owners, 1, LANES), "elem", 0, 0, tiled=True)

    force = pl.pallas_call(
        force_kernel,
        out_shape=jax.ShapeDtypeStruct((groups, 32, LANES), F32),
        in_specs=[vmem, vmem],
        out_specs=vmem,
        scratch_shapes=[
            pltpu.VMEM((LANES, LANES), F32),
            pltpu.VMEM((2, 6, groups * LANES, LANES), F32),
        ],
        name="force",
    )(arrived.reshape(owners, LANES), segs)

    shared = lax.all_to_all(force, "bucket", 0, 0, tiled=True)
    outgoing = shared.reshape(groups * 32, owners).T
    returned = lax.all_to_all(outgoing.reshape(owners, 1, LANES), "elem", 0, 0, tiled=True)

    return pl.pallas_call(
        pick_kernel,
        out_shape=jax.ShapeDtypeStruct((3, uncovered), F32),
        in_specs=[vmem, vmem],
        out_specs=vmem,
        scratch_shapes=[pltpu.VMEM((120, LANES), F32)],
        name="pick",
    )(returned.reshape(owners, LANES), code)


def solution(mesh):
    in_specs = (
        P(None, "elem"),
        P("elem"),
        P("elem"),
        P("elem", None, "bucket"),
        P("elem", None, "bucket"),
    )
    out_specs = P(None, "elem")
    return jax.shard_map(local, mesh=mesh, in_specs=in_specs, out_specs=out_specs, check_vma=False)
```

```python
import jax
import jax.numpy as jnp
from jax import lax
from jax.experimental import pallas as pl
from jax.experimental.pallas import tpu as pltpu
from jax.sharding import PartitionSpec as P

STIFFNESS = 20.0
DAMPING = 0.5
SLOTS = 5
LANES = 128
F32 = jnp.float32
BF16 = jnp.bfloat16
NT = (((1,), (1,)), ((), ()))


def one_hot(row, size):
    numbers = lax.broadcasted_iota(jnp.int32, (size, row.shape[1]), 0)
    return jnp.where(numbers == row, 1.0, 0.0).astype(BF16)


def segment_kernel(point_ref, angle_ref, seg_ref):
    azimuth, polar = angle_ref[:, 0, :], angle_ref[:, 1, :]
    ring = jnp.sin(polar)
    for i in range(3):
        seg_ref[:, i, :] = point_ref[i]
    seg_ref[:, 3, :] = jnp.cos(azimuth) * ring
    seg_ref[:, 4, :] = jnp.sin(azimuth) * ring
    seg_ref[:, 5, :] = jnp.cos(polar)
    seg_ref[:, 6, :] = jnp.zeros_like(ring)
    seg_ref[:, 7, :] = jnp.zeros_like(ring)


def pack_kernel(eroded_ref, map_ref, node_hbm, out_ref, code_ref, node_ref, row_ref, col_ref, rank_ref, owner_hot,
                geo_ref, sem):
    copy = pltpu.make_async_copy(node_hbm, node_ref, sem)
    copy.start()
    group = lax.axis_index("bucket")
    blocks = map_ref.shape[0]
    count = row_ref.shape[1]
    tiles = count // LANES
    rows4 = eroded_ref.shape[0]
    span = count // rows4

    eroded = eroded_ref[...]
    lane = lax.broadcasted_iota(jnp.int32, (LANES, span), 1)
    six = 6 * lax.broadcasted_iota(jnp.int32, (LANES, span), 0)
    spread = jnp.where((lane >= six) & (lane < six + 6), 1.0, 0.0).astype(BF16)
    high = jnp.dot((eroded >> 3).astype(F32).astype(BF16), spread, preferred_element_type=F32)
    low = jnp.dot((eroded & 7).astype(F32).astype(BF16), spread, preferred_element_type=F32)
    number = lax.broadcasted_iota(jnp.int32, (rows4, span), 1)
    faces4 = 6 * (high * 8.0 + low).astype(jnp.int32) + number % 6
    for a in range(rows4):
        row_ref[0:1, a * span:(a + 1) * span] = faces4[a:a + 1, :]

    buckets = map_ref[...]
    digits = jnp.concatenate([(buckets & 1016).astype(F32), (buckets & 7).astype(F32)], axis=1).astype(BF16)
    step = 512
    for c in range(count // step):
        at = slice(c * step, (c + 1) * step)
        face = row_ref[0:1, at]
        hot = one_hot(face & (LANES - 1), LANES)
        value = jnp.dot(digits, jnp.concatenate([hot, hot], axis=0), preferred_element_type=F32)
        numbers = lax.broadcasted_iota(jnp.int32, (blocks, step), 0)
        rank_ref[0:1, at] = jnp.sum(jnp.where(numbers == (face >> 7), value, 0.0), axis=0, keepdims=True)

    earlier = (lax.broadcasted_iota(jnp.int32, (LANES, LANES), 0)
               < lax.broadcasted_iota(jnp.int32, (LANES, LANES), 1))
    counts, picks = [], []
    for t in range(tiles):
        at = slice(t * LANES, (t + 1) * LANES)
        mine = rank_ref[0:1, at]
        other = jnp.broadcast_to(mine, (LANES, LANES)).T
        hit = jnp.where((other == mine) & earlier, 1.0, 0.0)
        rank_ref[1:2, at] = jnp.sum(hit, axis=0, keepdims=True)
        bucket = mine.astype(jnp.int32)
        hot = one_hot(bucket >> 3, LANES)
        owner_hot[:, at] = hot
        picks.append(lax.broadcasted_iota(jnp.int32, (16, LANES), 0) == (bucket & 7))
        inner = jnp.where(picks[t], 1.0, 0.0).astype(BF16)
        counts.append(lax.dot_general(inner, hot, NT, preferred_element_type=F32))
    before = jnp.zeros((16, LANES), F32)
    for t in range(tiles):
        at = slice(t * LANES, (t + 1) * LANES)
        if t:
            before = before + counts[t - 1]
            seen = jnp.dot(before.astype(BF16), owner_hot[:, at], preferred_element_type=F32)
            rank_ref[1:2, at] += jnp.sum(jnp.where(picks[t], seen, 0.0), axis=0, keepdims=True)

    bucket = rank_ref[0:1, :].astype(jnp.int32)
    rank = rank_ref[1:2, :].astype(jnp.int32)
    owner = bucket >> 3
    inner = bucket & 7
    code_ref[0:1, :] = owner
    code_ref[1:2, :] = inner * SLOTS + rank
    column = jnp.where((inner >> 1) == group, (inner & 1) * LANES + owner, -1)
    source = jnp.zeros((16, 256), F32)
    for c in range(count // step):
        at = slice(c * step, (c + 1) * step)
        face = row_ref[0:1, at]
        numbers = lax.broadcasted_iota(jnp.int32, (16, step), 0)
        parts = jnp.where(numbers < 8, (face >> 7) + 1, face & (LANES - 1))
        left = jnp.where((numbers & 7) == rank[:, at], parts, 0).astype(F32).astype(BF16)
        source = source + lax.dot_general(left, one_hot(column[:, at], 256), NT, preferred_element_type=F32)

    copy.wait()
    for g in range(blocks // 16):
        row = [node_ref[pl.ds((r // 8) * blocks * 8 + r % 8 + g * 128, 16, stride=8), :] for r in range(24)]
        corner = [row[3 * m:3 * m + 3] for m in range(4)]
        motion = [row[12 + 3 * m:15 + 3 * m] for m in range(4)]
        centroid = [0.25 * (corner[0][i] + corner[1][i] + corner[2][i] + corner[3][i]) for i in range(3)]
        one = [corner[2][i] - corner[0][i] for i in range(3)]
        two = [corner[3][i] - corner[1][i] for i in range(3)]
        area = [
            0.5 * (one[1] * two[2] - one[2] * two[1]),
            0.5 * (one[2] * two[0] - one[0] * two[2]),
            0.5 * (one[0] * two[1] - one[1] * two[0]),
        ]
        velocity = [0.25 * (motion[0][i] + motion[1][i] + motion[2][i] + motion[3][i]) for i in range(3)]
        for q, value in enumerate(centroid + area + velocity):
            at = slice(q * blocks + g * 16, q * blocks + g * 16 + 16)
            first = value.astype(BF16)
            geo_ref[at, :LANES] = first
            geo_ref[at, LANES:] = (value - first.astype(F32)).astype(BF16)

    col_ref[...] = jnp.zeros(col_ref.shape, F32)
    geometry = geo_ref[...]
    filled = jnp.zeros((1, 256), F32)
    for k in range(SLOTS):
        high = source[k:k + 1, :].astype(jnp.int32) - 1
        low = source[8 + k:9 + k, :].astype(jnp.int32)
        filled = filled + jnp.where(high >= 0, 1.0, 0.0)
        hot = one_hot(low, LANES)
        found = jnp.dot(geometry, jnp.concatenate([hot, hot], axis=0), preferred_element_type=F32)
        mine = lax.broadcasted_iota(jnp.int32, (blocks, 256), 0) == high
        for q in range(9):
            value = jnp.sum(jnp.where(mine, found[q * blocks:(q + 1) * blocks], 0.0), axis=0, keepdims=True)
            for par in range(2):
                start = par * 64 + q * SLOTS + k
                col_ref[start:start + 1, :] = value[:, par * LANES:(par + 1) * LANES]
    for par in range(2):
        col_ref[par * 64 + 45:par * 64 + 46, :] = filled[:, par * LANES:(par + 1) * LANES]
    out_ref[...] = col_ref[...].T


def force_kernel(face_ref, seg_ref, out_ref, row_ref, wide_ref):
    row_ref[...] = face_ref[...].T
    groups = seg_ref.shape[0] // 2
    for g in range(2 * groups):
        columns = seg_ref[g].T
        for q in range(6):
            wide_ref[g % 2, q, (g // 2) * LANES:(g // 2 + 1) * LANES, :] = jnp.broadcast_to(
                columns[:, q:q + 1], (LANES, LANES))
    out_ref[...] = jnp.zeros(out_ref.shape, F32)
    chunk = 64
    for par in range(2):
        count = jnp.sum(row_ref[par * 64 + 45:par * 64 + 46, :], axis=1, keepdims=True)
        stiff = jnp.broadcast_to(STIFFNESS * lax.rsqrt(jnp.maximum(count, 1.0)), (1, LANES))
        for k in range(SLOTS):
            geo = [row_ref[par * 64 + q * SLOTS + k:par * 64 + q * SLOTS + k + 1, :] for q in range(9)]

            def pairs(step, total, par=par, geo=geo, stiff=stiff):
                at = pl.ds(pl.multiple_of(step * chunk, chunk), chunk)
                seg = [wide_ref[par, q, at, :] for q in range(6)]
                normal = seg[3:6]
                off = [geo[i] - seg[i] for i in range(3)]
                dist_sq = off[0] * off[0] + off[1] * off[1] + off[2] * off[2]
                gap = off[0] * normal[0] + off[1] * normal[1] + off[2] * normal[2]
                closing = geo[6] * normal[0] + geo[7] * normal[1] + geo[8] * normal[2]
                projected = jnp.abs(geo[3] * normal[0] + geo[4] * normal[1] + geo[5] * normal[2])
                weight = jnp.exp(-0.5 * dist_sq)
                traction = weight * jnp.maximum(-gap, 0.0) * (stiff - DAMPING * closing) * projected
                return tuple(
                    total[i] + jnp.sum((traction * normal[i]).reshape(chunk // 8, 8, LANES), axis=0)
                    for i in range(3))

            zero = jnp.zeros((8, LANES), F32)
            total = lax.fori_loop(0, wide_ref.shape[2] // chunk, pairs, (zero, zero, zero))
            for i in range(3):
                force = jnp.sum(total[i], axis=0, keepdims=True)
                for x in range(out_ref.shape[0]):
                    out_ref[x, i * 10 + par * SLOTS + k:i * 10 + par * SLOTS + k + 1, :] = force


def pick_kernel(force_ref, code_ref, out_ref, row_ref):
    turned = force_ref[...].T
    for x in range(4):
        for i in range(3):
            row_ref[i * 40 + x * 10:i * 40 + x * 10 + 10, :] = turned[x * 32 + i * 10:x * 32 + i * 10 + 10, :]
    value = row_ref[...]
    first = value.astype(BF16)
    second = (value - first.astype(F32)).astype(BF16)
    left = jnp.concatenate([first.astype(F32), second.astype(F32)], axis=0).astype(BF16)
    rows = value.shape[0]
    step = 512
    for c in range(out_ref.shape[1] // step):
        at = slice(c * step, (c + 1) * step)
        hot = one_hot(code_ref[0:1, at], LANES)
        both = jnp.dot(left, hot, preferred_element_type=F32)
        found = both[:rows] + both[rows:]
        mine = lax.broadcasted_iota(jnp.int32, (40, step), 0) == code_ref[1:2, at]
        for i in range(3):
            out_ref[i:i + 1, at] = jnp.sum(
                jnp.where(mine, found[i * 40:(i + 1) * 40], 0.0), axis=0, keepdims=True)


def local(node_data, eroded, bucket_map, seg_point, seg_angle):
    owners = lax.axis_size("elem")
    groups = lax.axis_size("bucket")
    faces = node_data.shape[1]
    blocks = faces // LANES
    uncovered = 6 * eroded.shape[0]
    vmem = pl.BlockSpec(memory_space=pltpu.VMEM)

    segs = pl.pallas_call(
        segment_kernel,
        out_shape=jax.ShapeDtypeStruct((seg_point.shape[0], 8, seg_point.shape[2]), F32),
        in_specs=[vmem, vmem],
        out_specs=vmem,
        name="segments",
    )(seg_point.transpose(1, 0, 2), seg_angle)
    segs = lax.all_to_all(segs, "bucket", 0, 0, tiled=True)

    node_tiles = node_data.reshape(3, 8, blocks, LANES).transpose(0, 2, 1, 3).reshape(24 * blocks, LANES)
    packed, code = pl.pallas_call(
        pack_kernel,
        out_shape=(
            jax.ShapeDtypeStruct((owners, LANES), F32),
            jax.ShapeDtypeStruct((2, uncovered), jnp.int32),
        ),
        in_specs=[vmem, vmem, pl.BlockSpec(memory_space=pl.ANY)],
        out_specs=(vmem, vmem),
        scratch_shapes=[
            pltpu.VMEM((24 * blocks, LANES), F32),
            pltpu.VMEM((1, uncovered), jnp.int32),
            pltpu.VMEM((LANES, LANES), F32),
            pltpu.VMEM((2, uncovered), F32),
            pltpu.VMEM((LANES, uncovered), BF16),
            pltpu.VMEM((9 * blocks, 2 * LANES), BF16),
            pltpu.SemaphoreType.DMA,
        ],
        name="pack",
    )(eroded.reshape(-1, LANES), bucket_map.reshape(blocks, LANES), node_tiles)

    arrived = lax.all_to_all(packed.reshape(owners, 1, LANES), "elem", 0, 0, tiled=True)

    force = pl.pallas_call(
        force_kernel,
        out_shape=jax.ShapeDtypeStruct((groups, 32, LANES), F32),
        in_specs=[vmem, vmem],
        out_specs=vmem,
        scratch_shapes=[
            pltpu.VMEM((LANES, LANES), F32),
            pltpu.VMEM((2, 6, groups * LANES, LANES), F32),
        ],
        name="force",
    )(arrived.reshape(owners, LANES), segs)

    shared = lax.all_to_all(force, "bucket", 0, 0, tiled=True)
    outgoing = shared.reshape(groups * 32, owners).T
    returned = lax.all_to_all(outgoing.reshape(owners, 1, LANES), "elem", 0, 0, tiled=True)

    return pl.pallas_call(
        pick_kernel,
        out_shape=jax.ShapeDtypeStruct((3, uncovered), F32),
        in_specs=[vmem, vmem],
        out_specs=vmem,
        scratch_shapes=[pltpu.VMEM((120, LANES), F32)],
        name="pick",
    )(returned.reshape(owners, LANES), code)


def solution(mesh):
    in_specs = (
        P(None, "elem"),
        P("elem"),
        P("elem"),
        P("elem", None, "bucket"),
        P("elem", None, "bucket"),
    )
    out_specs = P(None, "elem")
    return jax.shard_map(local, mesh=mesh, in_specs=in_specs, out_specs=out_specs, check_vma=False)
```

```python
import jax
import jax.numpy as jnp
from jax import lax
from jax.experimental import pallas as pl
from jax.experimental.pallas import tpu as pltpu
from jax.sharding import PartitionSpec as P

STIFFNESS = 20.0
DAMPING = 0.5
SLOTS = 5
LANES = 128
F32 = jnp.float32
BF16 = jnp.bfloat16
NT = (((1,), (1,)), ((), ()))


def one_hot(row, size):
    numbers = lax.broadcasted_iota(jnp.int32, (size, row.shape[1]), 0)
    return jnp.where(numbers == row, 1.0, 0.0).astype(BF16)


def pieces(value):
    first = value.astype(BF16).astype(F32)
    rest = value - first
    second = rest.astype(BF16).astype(F32)
    return first, second, rest - second


def coefficient_kernel(seg_ref, left_ref, normal_ref, rows_ref):
    rows_ref[...] = jnp.zeros(rows_ref.shape, F32)
    log2e = 1.4426950408889634
    order = (0, 0, 0, 1, 1, 2)
    azimuth, polar = seg_ref[:, 3, :], seg_ref[:, 4, :]
    ring = jnp.sin(polar)
    normal = [jnp.cos(azimuth) * ring, jnp.sin(azimuth) * ring, jnp.cos(polar)]
    point = [seg_ref[:, i, :] for i in range(3)]
    along = point[0] * normal[0] + point[1] * normal[1] + point[2] * normal[2]
    square = point[0] * point[0] + point[1] * point[1] + point[2] * point[2]
    terms = (
        (0, [log2e * value for value in point]),
        (0, [-value for value in normal]),
        (6, [-DAMPING * value for value in normal]),
        (3, normal),
    )
    split = [(start, [pieces(value) for value in values]) for start, values in terms]
    constant = [pieces((-0.5 * log2e) * square), pieces(along)]
    for term in range(4):
        at = term * LANES
        start, values = split[term]
        for group, piece in enumerate(order):
            for i in range(3):
                rows_ref[:, at + group * 16 + start + i, :] = values[i][piece]
        if term < 2:
            for piece in range(3):
                rows_ref[:, at + 96 + 6 + piece, :] = constant[term][piece]
    for piece in range(3):
        rows_ref[:, 96 + piece, :] = jnp.full_like(ring, -1.0)
        rows_ref[:, 2 * LANES + 96 + 3 + piece, :] = jnp.full_like(ring, 1.0)
    for i in range(3):
        normal_ref[:, i, :] = normal[i]
    for i in range(3, 8):
        normal_ref[:, i, :] = jnp.zeros_like(ring)
    for g in range(seg_ref.shape[0]):
        for term in range(4):
            turned = rows_ref[g, term * LANES:(term + 1) * LANES, :].T.astype(BF16)
            for half in range(2):
                left_ref[g % 2, (g // 2) * 2 + half, term * 64:(term + 1) * 64, :] = turned[half * 64:(half + 1) * 64]


def pack_kernel(eroded_ref, map_ref, node_hbm, out_ref, code_ref, node_ref, row_ref, col_ref, rank_ref, owner_hot,
                geo_ref, sem):
    copy = pltpu.make_async_copy(node_hbm, node_ref, sem)
    copy.start()
    group = lax.axis_index("bucket")
    blocks = map_ref.shape[0]
    count = row_ref.shape[1]
    tiles = count // LANES
    rows4 = eroded_ref.shape[0]
    span = count // rows4

    eroded = eroded_ref[...]
    lane = lax.broadcasted_iota(jnp.int32, (LANES, span), 1)
    six = 6 * lax.broadcasted_iota(jnp.int32, (LANES, span), 0)
    spread = jnp.where((lane >= six) & (lane < six + 6), 1.0, 0.0).astype(BF16)
    high = jnp.dot((eroded >> 3).astype(F32).astype(BF16), spread, preferred_element_type=F32)
    low = jnp.dot((eroded & 7).astype(F32).astype(BF16), spread, preferred_element_type=F32)
    number = lax.broadcasted_iota(jnp.int32, (rows4, span), 1)
    faces4 = 6 * (high * 8.0 + low).astype(jnp.int32) + number % 6
    for a in range(rows4):
        row_ref[0:1, a * span:(a + 1) * span] = faces4[a:a + 1, :]

    buckets = map_ref[...]
    digits = jnp.concatenate([(buckets & 1016).astype(F32), (buckets & 7).astype(F32)], axis=1).astype(BF16)
    step = 512
    for c in range(count // step):
        at = slice(c * step, (c + 1) * step)
        face = row_ref[0:1, at]
        hot = one_hot(face & (LANES - 1), LANES)
        value = jnp.dot(digits, jnp.concatenate([hot, hot], axis=0), preferred_element_type=F32)
        numbers = lax.broadcasted_iota(jnp.int32, (blocks, step), 0)
        rank_ref[0:1, at] = jnp.sum(jnp.where(numbers == (face >> 7), value, 0.0), axis=0, keepdims=True)

    earlier = (lax.broadcasted_iota(jnp.int32, (LANES, LANES), 0)
               < lax.broadcasted_iota(jnp.int32, (LANES, LANES), 1))
    counts, picks = [], []
    for t in range(tiles):
        at = slice(t * LANES, (t + 1) * LANES)
        mine = rank_ref[0:1, at]
        other = jnp.broadcast_to(mine, (LANES, LANES)).T
        hit = jnp.where((other == mine) & earlier, 1.0, 0.0)
        rank_ref[1:2, at] = jnp.sum(hit, axis=0, keepdims=True)
        bucket = mine.astype(jnp.int32)
        hot = one_hot(bucket >> 3, LANES)
        owner_hot[:, at] = hot
        picks.append(lax.broadcasted_iota(jnp.int32, (16, LANES), 0) == (bucket & 7))
        inner = jnp.where(picks[t], 1.0, 0.0).astype(BF16)
        counts.append(lax.dot_general(inner, hot, NT, preferred_element_type=F32))
    before = jnp.zeros((16, LANES), F32)
    for t in range(tiles):
        at = slice(t * LANES, (t + 1) * LANES)
        if t:
            before = before + counts[t - 1]
            seen = jnp.dot(before.astype(BF16), owner_hot[:, at], preferred_element_type=F32)
            rank_ref[1:2, at] += jnp.sum(jnp.where(picks[t], seen, 0.0), axis=0, keepdims=True)

    bucket = rank_ref[0:1, :].astype(jnp.int32)
    rank = rank_ref[1:2, :].astype(jnp.int32)
    owner = bucket >> 3
    inner = bucket & 7
    code_ref[0:1, :] = owner
    code_ref[1:2, :] = inner * SLOTS + rank
    column = jnp.where((inner >> 1) == group, (inner & 1) * LANES + owner, -1)
    source = jnp.zeros((16, 256), F32)
    for c in range(count // step):
        at = slice(c * step, (c + 1) * step)
        face = row_ref[0:1, at]
        numbers = lax.broadcasted_iota(jnp.int32, (16, step), 0)
        parts = jnp.where(numbers < 8, (face >> 7) + 1, face & (LANES - 1))
        left = jnp.where((numbers & 7) == rank[:, at], parts, 0).astype(F32).astype(BF16)
        source = source + lax.dot_general(left, one_hot(column[:, at], 256), NT, preferred_element_type=F32)

    copy.wait()
    for g in range(blocks // 16):
        row = [node_ref[pl.ds((r // 8) * blocks * 8 + r % 8 + g * 128, 16, stride=8), :] for r in range(24)]
        corner = [row[3 * m:3 * m + 3] for m in range(4)]
        motion = [row[12 + 3 * m:15 + 3 * m] for m in range(4)]
        centroid = [0.25 * (corner[0][i] + corner[1][i] + corner[2][i] + corner[3][i]) for i in range(3)]
        one = [corner[2][i] - corner[0][i] for i in range(3)]
        two = [corner[3][i] - corner[1][i] for i in range(3)]
        area = [
            0.5 * (one[1] * two[2] - one[2] * two[1]),
            0.5 * (one[2] * two[0] - one[0] * two[2]),
            0.5 * (one[0] * two[1] - one[1] * two[0]),
        ]
        velocity = [0.25 * (motion[0][i] + motion[1][i] + motion[2][i] + motion[3][i]) for i in range(3)]
        for q, value in enumerate(centroid + area + velocity):
            at = slice(q * blocks + g * 16, q * blocks + g * 16 + 16)
            first = value.astype(BF16)
            geo_ref[at, :LANES] = first
            geo_ref[at, LANES:] = (value - first.astype(F32)).astype(BF16)

    col_ref[...] = jnp.zeros(col_ref.shape, F32)
    geometry = geo_ref[...]
    filled = jnp.zeros((1, 256), F32)
    for k in range(SLOTS):
        high = source[k:k + 1, :].astype(jnp.int32) - 1
        low = source[8 + k:9 + k, :].astype(jnp.int32)
        filled = filled + jnp.where(high >= 0, 1.0, 0.0)
        hot = one_hot(low, LANES)
        found = jnp.dot(geometry, jnp.concatenate([hot, hot], axis=0), preferred_element_type=F32)
        mine = lax.broadcasted_iota(jnp.int32, (blocks, 256), 0) == high
        for q in range(9):
            value = jnp.sum(jnp.where(mine, found[q * blocks:(q + 1) * blocks], 0.0), axis=0, keepdims=True)
            for par in range(2):
                start = par * 64 + k * 12 + q
                col_ref[start:start + 1, :] = value[:, par * LANES:(par + 1) * LANES]
    for par in range(2):
        col_ref[par * 64 + 60:par * 64 + 61, :] = filled[:, par * LANES:(par + 1) * LANES]
    out_ref[...] = col_ref[...].T


def force_kernel(face_ref, left_ref, seg_ref, out_ref, row_ref, right_ref, wide_ref):
    row_ref[...] = face_ref[...].T
    groups = seg_ref.shape[0] // 2
    for g in range(2 * groups):
        columns = seg_ref[g].T
        for i in range(3):
            wide_ref[g % 2, i, (g // 2) * LANES:(g // 2 + 1) * LANES, :] = jnp.broadcast_to(
                columns[:, i:i + 1], (LANES, LANES))
    out_ref[...] = jnp.zeros(out_ref.shape, F32)
    half_log2e = 0.5 * 1.4426950408889634
    number = lax.broadcasted_iota(jnp.int32, (16, LANES), 0)
    for par in range(2):
        count = jnp.sum(row_ref[par * 64 + 60:par * 64 + 61, :], axis=1, keepdims=True)
        stiff = pieces(jnp.broadcast_to(STIFFNESS * lax.rsqrt(jnp.maximum(count, 1.0)), (1, LANES)))
        for k in range(SLOTS):
            start = par * 64 + k * 12
            face = row_ref[start:start + 16, :]
            center = [row_ref[start + i:start + i + 1, :] for i in range(3)]
            square = pieces(half_log2e * (
                center[0] * center[0] + center[1] * center[1] + center[2] * center[2]))
            extra = jnp.where((number >= 6) & (number < 9), 1.0, 0.0)
            for piece in range(3):
                extra = jnp.where(number == piece, square[piece], extra)
                extra = jnp.where(number == 3 + piece, stiff[piece], extra)
            first, second, third = pieces(face)
            blocks = (first, second, third, first, second, first, extra, jnp.zeros_like(extra))
            for group, block in enumerate(blocks):
                right_ref[par, group * 16:(group + 1) * 16, k * LANES:(k + 1) * LANES] = block.astype(BF16)
    chunks = left_ref.shape[1]
    for par in range(2):
        for first in range(0, SLOTS, 2):
            width = min(2, SLOTS - first)
            right = right_ref[par, :, first * LANES:(first + width) * LANES]
            total = [[jnp.zeros((8, LANES), F32) for _ in range(3)] for _ in range(width)]
            for chunk in range(chunks):
                found = jnp.dot(left_ref[par, chunk], right, preferred_element_type=F32)
                normal = [wide_ref[par, i, chunk * 64:(chunk + 1) * 64, :] for i in range(3)]
                for k in range(width):
                    at = slice(k * LANES, (k + 1) * LANES)
                    weight = jnp.exp2(found[0:64, at])
                    traction = (weight * jnp.maximum(found[64:128, at], 0.0) * found[128:192, at]
                                * jnp.abs(found[192:256, at]))
                    for i in range(3):
                        total[k][i] = total[k][i] + jnp.sum(
                            (traction * normal[i]).reshape(8, 8, LANES), axis=0)
            for k in range(width):
                for i in range(3):
                    force = jnp.sum(total[k][i], axis=0, keepdims=True)
                    row = i * 10 + par * SLOTS + first + k
                    for x in range(out_ref.shape[0]):
                        out_ref[x, row:row + 1, :] = force


def pick_kernel(force_ref, code_ref, out_ref, row_ref):
    turned = force_ref[...].T
    for x in range(4):
        for i in range(3):
            row_ref[i * 40 + x * 10:i * 40 + x * 10 + 10, :] = turned[x * 32 + i * 10:x * 32 + i * 10 + 10, :]
    value = row_ref[...]
    first = value.astype(BF16)
    second = (value - first.astype(F32)).astype(BF16)
    left = jnp.concatenate([first.astype(F32), second.astype(F32)], axis=0).astype(BF16)
    rows = value.shape[0]
    step = 512
    for c in range(out_ref.shape[1] // step):
        at = slice(c * step, (c + 1) * step)
        hot = one_hot(code_ref[0:1, at], LANES)
        both = jnp.dot(left, hot, preferred_element_type=F32)
        found = both[:rows] + both[rows:]
        mine = lax.broadcasted_iota(jnp.int32, (40, step), 0) == code_ref[1:2, at]
        for i in range(3):
            out_ref[i:i + 1, at] = jnp.sum(
                jnp.where(mine, found[i * 40:(i + 1) * 40], 0.0), axis=0, keepdims=True)


def step(node_data, eroded, bucket_map, seg_point, seg_angle):
    owners = lax.axis_size("elem")
    groups = lax.axis_size("bucket")
    faces = node_data.shape[1]
    blocks = faces // LANES
    uncovered = 6 * eroded.shape[0]
    vmem = pl.BlockSpec(memory_space=pltpu.VMEM)

    segs = jnp.concatenate([seg_point, seg_angle], axis=1)
    segs = lax.all_to_all(segs, "bucket", 0, 0, tiled=True)

    node_tiles = node_data.reshape(3, 8, blocks, LANES).transpose(0, 2, 1, 3).reshape(24 * blocks, LANES)
    packed, code = pl.pallas_call(
        pack_kernel,
        out_shape=(
            jax.ShapeDtypeStruct((owners, LANES), F32),
            jax.ShapeDtypeStruct((2, uncovered), jnp.int32),
        ),
        in_specs=[vmem, vmem, pl.BlockSpec(memory_space=pl.ANY)],
        out_specs=(vmem, vmem),
        scratch_shapes=[
            pltpu.VMEM((24 * blocks, LANES), F32),
            pltpu.VMEM((1, uncovered), jnp.int32),
            pltpu.VMEM((LANES, LANES), F32),
            pltpu.VMEM((2, uncovered), F32),
            pltpu.VMEM((LANES, uncovered), BF16),
            pltpu.VMEM((9 * blocks, 2 * LANES), BF16),
            pltpu.SemaphoreType.DMA,
        ],
        name="pack",
    )(eroded.reshape(-1, LANES), bucket_map.reshape(blocks, LANES), node_tiles)

    arrived = lax.all_to_all(packed.reshape(owners, 1, LANES), "elem", 0, 0, tiled=True)

    left, normal = pl.pallas_call(
        coefficient_kernel,
        out_shape=(
            jax.ShapeDtypeStruct((2, 2 * groups, 256, LANES), BF16),
            jax.ShapeDtypeStruct((2 * groups, 8, LANES), F32),
        ),
        in_specs=[vmem],
        out_specs=(vmem, vmem),
        scratch_shapes=[pltpu.VMEM((2 * groups, 4 * LANES, LANES), F32)],
        name="coefficients",
    )(segs)

    force = pl.pallas_call(
        force_kernel,
        out_shape=jax.ShapeDtypeStruct((groups, 32, LANES), F32),
        in_specs=[vmem, vmem, vmem],
        out_specs=vmem,
        scratch_shapes=[
            pltpu.VMEM((LANES, LANES), F32),
            pltpu.VMEM((2, LANES, SLOTS * LANES), BF16),
            pltpu.VMEM((2, 3, groups * LANES, LANES), F32),
        ],
        name="force",
    )(arrived.reshape(owners, LANES), left, normal)

    shared = lax.all_to_all(force, "bucket", 0, 0, tiled=True)
    outgoing = shared.reshape(groups * 32, owners).T
    returned = lax.all_to_all(outgoing.reshape(owners, 1, LANES), "elem", 0, 0, tiled=True)

    return pl.pallas_call(
        pick_kernel,
        out_shape=jax.ShapeDtypeStruct((3, uncovered), F32),
        in_specs=[vmem, vmem],
        out_specs=vmem,
        scratch_shapes=[pltpu.VMEM((120, LANES), F32)],
        name="pick",
    )(returned.reshape(owners, LANES), code)


def solution(mesh):
    in_specs = (
        P(None, "elem"),
        P("elem"),
        P("elem"),
        P("elem", None, "bucket"),
        P("elem", None, "bucket"),
    )
    out_specs = P(None, "elem")
    return jax.shard_map(step, mesh=mesh, in_specs=in_specs, out_specs=out_specs, check_vma=False)
```

```python
import jax
import jax.numpy as jnp
from jax import lax
from jax.experimental import pallas as pl
from jax.experimental.pallas import tpu as pltpu
from jax.sharding import PartitionSpec as P

STIFFNESS = 20.0
DAMPING = 0.5
SLOTS = 5
LANES = 128
F32 = jnp.float32
BF16 = jnp.bfloat16
NT = (((1,), (1,)), ((), ()))


def near(value):
    return pltpu.with_memory_space_constraint(value, pltpu.VMEM)


def one_hot(row, size):
    numbers = lax.broadcasted_iota(jnp.int32, (size, row.shape[1]), 0)
    return jnp.where(numbers == row, 1.0, 0.0).astype(BF16)


def join_kernel(point_ref, angle_ref, out_ref):
    for i in range(3):
        out_ref[:, i, :] = point_ref[i]
    for i in range(2):
        out_ref[:, 3 + i, :] = angle_ref[:, i, :]


def pieces(value):
    first = value.astype(BF16).astype(F32)
    rest = value - first
    second = rest.astype(BF16).astype(F32)
    return first, second, rest - second


def coefficient_kernel(seg_ref, left_ref, normal_ref, rows_ref):
    rows_ref[...] = jnp.zeros(rows_ref.shape, F32)
    log2e = 1.4426950408889634
    order = (0, 0, 0, 1, 1, 2)
    azimuth, polar = seg_ref[:, 3, :], seg_ref[:, 4, :]
    ring = jnp.sin(polar)
    normal = [jnp.cos(azimuth) * ring, jnp.sin(azimuth) * ring, jnp.cos(polar)]
    point = [seg_ref[:, i, :] for i in range(3)]
    along = point[0] * normal[0] + point[1] * normal[1] + point[2] * normal[2]
    square = point[0] * point[0] + point[1] * point[1] + point[2] * point[2]
    terms = (
        (0, [log2e * value for value in point]),
        (0, [-value for value in normal]),
        (6, [-DAMPING * value for value in normal]),
        (3, normal),
    )
    split = [(start, [pieces(value) for value in values]) for start, values in terms]
    constant = [pieces((-0.5 * log2e) * square), pieces(along)]
    for term in range(4):
        at = term * LANES
        start, values = split[term]
        for group, piece in enumerate(order):
            for i in range(3):
                rows_ref[:, at + group * 16 + start + i, :] = values[i][piece]
        if term < 2:
            for piece in range(3):
                rows_ref[:, at + 96 + 6 + piece, :] = constant[term][piece]
    for piece in range(3):
        rows_ref[:, 96 + piece, :] = jnp.full_like(ring, -1.0)
        rows_ref[:, 2 * LANES + 96 + 3 + piece, :] = jnp.full_like(ring, 1.0)
    for i in range(3):
        normal_ref[:, i, :] = normal[i]
    for i in range(3, 8):
        normal_ref[:, i, :] = jnp.zeros_like(ring)
    for g in range(seg_ref.shape[0]):
        for term in range(4):
            turned = rows_ref[g, term * LANES:(term + 1) * LANES, :].T.astype(BF16)
            for half in range(2):
                left_ref[g % 2, (g // 2) * 2 + half, term * 64:(term + 1) * 64, :] = turned[half * 64:(half + 1) * 64]


def pack_kernel(eroded_ref, map_ref, node_hbm, out_ref, code_ref, node_ref, row_ref, col_ref, rank_ref, owner_hot,
                geo_ref, sem):
    copy = pltpu.make_async_copy(node_hbm, node_ref, sem)
    copy.start()
    group = lax.axis_index("bucket")
    blocks = map_ref.shape[0]
    count = row_ref.shape[1]
    tiles = count // LANES
    rows4 = eroded_ref.shape[0]
    span = count // rows4

    eroded = eroded_ref[...]
    lane = lax.broadcasted_iota(jnp.int32, (LANES, span), 1)
    six = 6 * lax.broadcasted_iota(jnp.int32, (LANES, span), 0)
    spread = jnp.where((lane >= six) & (lane < six + 6), 1.0, 0.0).astype(BF16)
    high = jnp.dot((eroded >> 3).astype(F32).astype(BF16), spread, preferred_element_type=F32)
    low = jnp.dot((eroded & 7).astype(F32).astype(BF16), spread, preferred_element_type=F32)
    number = lax.broadcasted_iota(jnp.int32, (rows4, span), 1)
    faces4 = 6 * (high * 8.0 + low).astype(jnp.int32) + number % 6
    for a in range(rows4):
        row_ref[0:1, a * span:(a + 1) * span] = faces4[a:a + 1, :]

    buckets = map_ref[...]
    digits = jnp.concatenate([(buckets & 1016).astype(F32), (buckets & 7).astype(F32)], axis=1).astype(BF16)
    step = 512
    for c in range(count // step):
        at = slice(c * step, (c + 1) * step)
        face = row_ref[0:1, at]
        hot = one_hot(face & (LANES - 1), LANES)
        value = jnp.dot(digits, jnp.concatenate([hot, hot], axis=0), preferred_element_type=F32)
        numbers = lax.broadcasted_iota(jnp.int32, (blocks, step), 0)
        rank_ref[0:1, at] = jnp.sum(jnp.where(numbers == (face >> 7), value, 0.0), axis=0, keepdims=True)

    earlier = (lax.broadcasted_iota(jnp.int32, (LANES, LANES), 0)
               < lax.broadcasted_iota(jnp.int32, (LANES, LANES), 1))
    counts, picks = [], []
    for t in range(tiles):
        at = slice(t * LANES, (t + 1) * LANES)
        mine = rank_ref[0:1, at]
        other = jnp.broadcast_to(mine, (LANES, LANES)).T
        hit = jnp.where((other == mine) & earlier, 1.0, 0.0)
        rank_ref[1:2, at] = jnp.sum(hit, axis=0, keepdims=True)
        bucket = mine.astype(jnp.int32)
        hot = one_hot(bucket >> 3, LANES)
        owner_hot[:, at] = hot
        picks.append(lax.broadcasted_iota(jnp.int32, (16, LANES), 0) == (bucket & 7))
        inner = jnp.where(picks[t], 1.0, 0.0).astype(BF16)
        counts.append(lax.dot_general(inner, hot, NT, preferred_element_type=F32))
    before = jnp.zeros((16, LANES), F32)
    for t in range(tiles):
        at = slice(t * LANES, (t + 1) * LANES)
        if t:
            before = before + counts[t - 1]
            seen = jnp.dot(before.astype(BF16), owner_hot[:, at], preferred_element_type=F32)
            rank_ref[1:2, at] += jnp.sum(jnp.where(picks[t], seen, 0.0), axis=0, keepdims=True)

    bucket = rank_ref[0:1, :].astype(jnp.int32)
    rank = rank_ref[1:2, :].astype(jnp.int32)
    owner = bucket >> 3
    inner = bucket & 7
    code_ref[0:1, :] = owner
    code_ref[1:2, :] = inner * SLOTS + rank
    column = jnp.where((inner >> 1) == group, (inner & 1) * LANES + owner, -1)
    source = jnp.zeros((16, 256), F32)
    for c in range(count // step):
        at = slice(c * step, (c + 1) * step)
        face = row_ref[0:1, at]
        numbers = lax.broadcasted_iota(jnp.int32, (16, step), 0)
        parts = jnp.where(numbers < 8, (face >> 7) + 1, face & (LANES - 1))
        left = jnp.where((numbers & 7) == rank[:, at], parts, 0).astype(F32).astype(BF16)
        source = source + lax.dot_general(left, one_hot(column[:, at], 256), NT, preferred_element_type=F32)

    copy.wait()
    for g in range(blocks // 16):
        row = [node_ref[pl.ds((r // 8) * blocks * 8 + r % 8 + g * 128, 16, stride=8), :] for r in range(24)]
        corner = [row[3 * m:3 * m + 3] for m in range(4)]
        motion = [row[12 + 3 * m:15 + 3 * m] for m in range(4)]
        centroid = [0.25 * (corner[0][i] + corner[1][i] + corner[2][i] + corner[3][i]) for i in range(3)]
        one = [corner[2][i] - corner[0][i] for i in range(3)]
        two = [corner[3][i] - corner[1][i] for i in range(3)]
        area = [
            0.5 * (one[1] * two[2] - one[2] * two[1]),
            0.5 * (one[2] * two[0] - one[0] * two[2]),
            0.5 * (one[0] * two[1] - one[1] * two[0]),
        ]
        velocity = [0.25 * (motion[0][i] + motion[1][i] + motion[2][i] + motion[3][i]) for i in range(3)]
        for q, value in enumerate(centroid + area + velocity):
            at = slice(q * blocks + g * 16, q * blocks + g * 16 + 16)
            first = value.astype(BF16)
            geo_ref[at, :LANES] = first
            geo_ref[at, LANES:] = (value - first.astype(F32)).astype(BF16)

    col_ref[...] = jnp.zeros(col_ref.shape, F32)
    geometry = geo_ref[...]
    filled = jnp.zeros((1, 256), F32)
    for k in range(SLOTS):
        high = source[k:k + 1, :].astype(jnp.int32) - 1
        low = source[8 + k:9 + k, :].astype(jnp.int32)
        filled = filled + jnp.where(high >= 0, 1.0, 0.0)
        hot = one_hot(low, LANES)
        found = jnp.dot(geometry, jnp.concatenate([hot, hot], axis=0), preferred_element_type=F32)
        mine = lax.broadcasted_iota(jnp.int32, (blocks, 256), 0) == high
        for q in range(9):
            value = jnp.sum(jnp.where(mine, found[q * blocks:(q + 1) * blocks], 0.0), axis=0, keepdims=True)
            for par in range(2):
                start = par * 64 + k * 12 + q
                col_ref[start:start + 1, :] = value[:, par * LANES:(par + 1) * LANES]
    for par in range(2):
        col_ref[par * 64 + 60:par * 64 + 61, :] = filled[:, par * LANES:(par + 1) * LANES]
    out_ref[...] = col_ref[...].T


def force_kernel(face_ref, left_ref, seg_ref, out_ref, row_ref, right_ref, wide_ref):
    row_ref[...] = face_ref[...].T
    groups = seg_ref.shape[0] // 2
    for g in range(2 * groups):
        columns = seg_ref[g].T
        for i in range(3):
            wide_ref[g % 2, i, (g // 2) * LANES:(g // 2 + 1) * LANES, :] = jnp.broadcast_to(
                columns[:, i:i + 1], (LANES, LANES))
    out_ref[...] = jnp.zeros(out_ref.shape, F32)
    half_log2e = 0.5 * 1.4426950408889634
    number = lax.broadcasted_iota(jnp.int32, (16, LANES), 0)
    for par in range(2):
        count = jnp.sum(row_ref[par * 64 + 60:par * 64 + 61, :], axis=1, keepdims=True)
        stiff = pieces(jnp.broadcast_to(STIFFNESS * lax.rsqrt(jnp.maximum(count, 1.0)), (1, LANES)))
        for k in range(SLOTS):
            start = par * 64 + k * 12
            face = row_ref[start:start + 16, :]
            center = [row_ref[start + i:start + i + 1, :] for i in range(3)]
            square = pieces(half_log2e * (
                center[0] * center[0] + center[1] * center[1] + center[2] * center[2]))
            extra = jnp.where((number >= 6) & (number < 9), 1.0, 0.0)
            for piece in range(3):
                extra = jnp.where(number == piece, square[piece], extra)
                extra = jnp.where(number == 3 + piece, stiff[piece], extra)
            first, second, third = pieces(face)
            blocks = (first, second, third, first, second, first, extra, jnp.zeros_like(extra))
            for group, block in enumerate(blocks):
                right_ref[par, group * 16:(group + 1) * 16, k * LANES:(k + 1) * LANES] = block.astype(BF16)
    chunks = left_ref.shape[1]
    for par in range(2):
        for first in range(0, SLOTS, 2):
            width = min(2, SLOTS - first)
            right = right_ref[par, :, first * LANES:(first + width) * LANES]
            total = [[jnp.zeros((8, LANES), F32) for _ in range(3)] for _ in range(width)]
            for chunk in range(chunks):
                found = jnp.dot(left_ref[par, chunk], right, preferred_element_type=F32)
                normal = [wide_ref[par, i, chunk * 64:(chunk + 1) * 64, :] for i in range(3)]
                for k in range(width):
                    at = slice(k * LANES, (k + 1) * LANES)
                    weight = jnp.exp2(found[0:64, at])
                    traction = (weight * jnp.maximum(found[64:128, at], 0.0) * found[128:192, at]
                                * jnp.abs(found[192:256, at]))
                    for i in range(3):
                        total[k][i] = total[k][i] + jnp.sum(
                            (traction * normal[i]).reshape(8, 8, LANES), axis=0)
            for k in range(width):
                for i in range(3):
                    force = jnp.sum(total[k][i], axis=0, keepdims=True)
                    row = i * 10 + par * SLOTS + first + k
                    for x in range(out_ref.shape[0]):
                        out_ref[x, row:row + 1, :] = force


def pick_kernel(force_ref, code_ref, out_ref, row_ref):
    turned = force_ref[...].T
    for x in range(4):
        for i in range(3):
            row_ref[i * 40 + x * 10:i * 40 + x * 10 + 10, :] = turned[x * 32 + i * 10:x * 32 + i * 10 + 10, :]
    value = row_ref[...]
    first = value.astype(BF16)
    second = (value - first.astype(F32)).astype(BF16)
    left = jnp.concatenate([first.astype(F32), second.astype(F32)], axis=0).astype(BF16)
    rows = value.shape[0]
    step = 512
    for c in range(out_ref.shape[1] // step):
        at = slice(c * step, (c + 1) * step)
        hot = one_hot(code_ref[0:1, at], LANES)
        both = jnp.dot(left, hot, preferred_element_type=F32)
        found = both[:rows] + both[rows:]
        mine = lax.broadcasted_iota(jnp.int32, (40, step), 0) == code_ref[1:2, at]
        for i in range(3):
            out_ref[i:i + 1, at] = jnp.sum(
                jnp.where(mine, found[i * 40:(i + 1) * 40], 0.0), axis=0, keepdims=True)


def step(node_data, eroded, bucket_map, seg_point, seg_angle):
    owners = lax.axis_size("elem")
    groups = lax.axis_size("bucket")
    faces = node_data.shape[1]
    blocks = faces // LANES
    uncovered = 6 * eroded.shape[0]
    vmem = pl.BlockSpec(memory_space=pltpu.VMEM)

    segs = pl.pallas_call(
        join_kernel,
        out_shape=pltpu.VMEM((seg_point.shape[0], 5, seg_point.shape[2]), F32),
        in_specs=[vmem, vmem],
        out_specs=vmem,
        name="join",
    )(seg_point.transpose(1, 0, 2), seg_angle)
    segs = lax.all_to_all(segs, "bucket", 0, 0, tiled=True)

    node_tiles = node_data.reshape(3, 8, blocks, LANES).transpose(0, 2, 1, 3).reshape(24 * blocks, LANES)
    packed, code = pl.pallas_call(
        pack_kernel,
        out_shape=(
            pltpu.VMEM((owners, LANES), F32),
            pltpu.VMEM((2, uncovered), jnp.int32),
        ),
        in_specs=[vmem, vmem, pl.BlockSpec(memory_space=pl.ANY)],
        out_specs=(vmem, vmem),
        scratch_shapes=[
            pltpu.VMEM((24 * blocks, LANES), F32),
            pltpu.VMEM((1, uncovered), jnp.int32),
            pltpu.VMEM((LANES, LANES), F32),
            pltpu.VMEM((2, uncovered), F32),
            pltpu.VMEM((LANES, uncovered), BF16),
            pltpu.VMEM((9 * blocks, 2 * LANES), BF16),
            pltpu.SemaphoreType.DMA,
        ],
        name="pack",
    )(eroded.reshape(-1, LANES), bucket_map.reshape(blocks, LANES), node_tiles)

    arrived = lax.all_to_all(packed.reshape(owners, 1, LANES), "elem", 0, 0, tiled=True)

    left, normal = pl.pallas_call(
        coefficient_kernel,
        out_shape=(
            pltpu.VMEM((2, 2 * groups, 256, LANES), BF16),
            pltpu.VMEM((2 * groups, 8, LANES), F32),
        ),
        in_specs=[vmem],
        out_specs=(vmem, vmem),
        scratch_shapes=[pltpu.VMEM((2 * groups, 4 * LANES, LANES), F32)],
        name="coefficients",
    )(near(segs))

    force = pl.pallas_call(
        force_kernel,
        out_shape=pltpu.VMEM((groups, 32, LANES), F32),
        in_specs=[vmem, vmem, vmem],
        out_specs=vmem,
        scratch_shapes=[
            pltpu.VMEM((LANES, LANES), F32),
            pltpu.VMEM((2, LANES, SLOTS * LANES), BF16),
            pltpu.VMEM((2, 3, groups * LANES, LANES), F32),
        ],
        name="force",
    )(near(arrived.reshape(owners, LANES)), near(left), near(normal))

    shared = lax.all_to_all(force, "bucket", 0, 0, tiled=True)
    outgoing = shared.reshape(groups * 32, owners).T
    returned = lax.all_to_all(outgoing.reshape(owners, 1, LANES), "elem", 0, 0, tiled=True)

    return pl.pallas_call(
        pick_kernel,
        out_shape=jax.ShapeDtypeStruct((3, uncovered), F32),
        in_specs=[vmem, vmem],
        out_specs=vmem,
        scratch_shapes=[pltpu.VMEM((120, LANES), F32)],
        name="pick",
    )(near(returned.reshape(owners, LANES)), near(code))


def solution(mesh):
    in_specs = (
        P(None, "elem"),
        P("elem"),
        P("elem"),
        P("elem", None, "bucket"),
        P("elem", None, "bucket"),
    )
    out_specs = P(None, "elem")
    return jax.shard_map(step, mesh=mesh, in_specs=in_specs, out_specs=out_specs, check_vma=False)
```

```python
import jax
import jax.numpy as jnp
from jax import lax
from jax.experimental import pallas as pl
from jax.experimental.pallas import tpu as pltpu
from jax.sharding import PartitionSpec as P

STIFFNESS = 20.0
DAMPING = 0.5
SLOTS = 5
LANES = 128
F32 = jnp.float32
BF16 = jnp.bfloat16
NT = (((1,), (1,)), ((), ()))


def near(value):
    return pltpu.with_memory_space_constraint(value, pltpu.VMEM)


def one_hot(row, size):
    numbers = lax.broadcasted_iota(jnp.int32, (size, row.shape[1]), 0)
    return jnp.where(numbers == row, 1.0, 0.0).astype(BF16)


def join_kernel(point_ref, angle_ref, eroded_ref, map_ref, out_ref, near_eroded_ref, near_map_ref):
    near_eroded_ref[...] = eroded_ref[...]
    near_map_ref[...] = map_ref[...]
    for i in range(3):
        out_ref[:, i, :] = point_ref[i]
    for i in range(2):
        out_ref[:, 3 + i, :] = angle_ref[:, i, :]


def pieces(value):
    first = value.astype(BF16).astype(F32)
    rest = value - first
    second = rest.astype(BF16).astype(F32)
    return first, second, rest - second


def coefficient_kernel(seg_ref, left_ref, normal_ref, rows_ref):
    rows_ref[...] = jnp.zeros(rows_ref.shape, F32)
    log2e = 1.4426950408889634
    order = (0, 0, 0, 1, 1, 2)
    azimuth, polar = seg_ref[:, 3, :], seg_ref[:, 4, :]
    ring = jnp.sin(polar)
    normal = [jnp.cos(azimuth) * ring, jnp.sin(azimuth) * ring, jnp.cos(polar)]
    point = [seg_ref[:, i, :] for i in range(3)]
    along = point[0] * normal[0] + point[1] * normal[1] + point[2] * normal[2]
    square = point[0] * point[0] + point[1] * point[1] + point[2] * point[2]
    terms = (
        (0, [log2e * value for value in point]),
        (0, [-value for value in normal]),
        (6, [-DAMPING * value for value in normal]),
        (3, normal),
    )
    split = [(start, [pieces(value) for value in values]) for start, values in terms]
    constant = [pieces((-0.5 * log2e) * square), pieces(along)]
    for term in range(4):
        at = term * LANES
        start, values = split[term]
        for group, piece in enumerate(order):
            for i in range(3):
                rows_ref[:, at + group * 16 + start + i, :] = values[i][piece]
        if term < 2:
            for piece in range(3):
                rows_ref[:, at + 96 + 6 + piece, :] = constant[term][piece]
    for piece in range(3):
        rows_ref[:, 96 + piece, :] = jnp.full_like(ring, -1.0)
        rows_ref[:, 2 * LANES + 96 + 3 + piece, :] = jnp.full_like(ring, 1.0)
    for i in range(3):
        normal_ref[:, i, :] = normal[i]
    for i in range(3, 8):
        normal_ref[:, i, :] = jnp.zeros_like(ring)
    for g in range(seg_ref.shape[0]):
        for term in range(4):
            turned = rows_ref[g, term * LANES:(term + 1) * LANES, :].T.astype(BF16)
            for half in range(2):
                left_ref[g % 2, (g // 2) * 2 + half, term * 64:(term + 1) * 64, :] = turned[half * 64:(half + 1) * 64]


def pack_kernel(eroded_ref, map_ref, node_hbm, out_ref, code_ref, node_ref, row_ref, col_ref, other_ref, rank_ref,
                owner_hot, geo_ref, sem):
    copy = pltpu.make_async_copy(node_hbm, node_ref, sem)
    copy.start()
    group = lax.axis_index("bucket")
    blocks = map_ref.shape[0]
    count = row_ref.shape[1]
    tiles = count // LANES
    rows4 = eroded_ref.shape[0]
    span = count // rows4

    eroded = eroded_ref[...]
    lane = lax.broadcasted_iota(jnp.int32, (LANES, span), 1)
    six = 6 * lax.broadcasted_iota(jnp.int32, (LANES, span), 0)
    spread = jnp.where((lane >= six) & (lane < six + 6), 1.0, 0.0).astype(BF16)
    high = jnp.dot((eroded >> 3).astype(F32).astype(BF16), spread, preferred_element_type=F32)
    low = jnp.dot((eroded & 7).astype(F32).astype(BF16), spread, preferred_element_type=F32)
    number = lax.broadcasted_iota(jnp.int32, (rows4, span), 1)
    faces4 = 6 * (high * 8.0 + low).astype(jnp.int32) + number % 6
    for a in range(rows4):
        row_ref[0:1, a * span:(a + 1) * span] = faces4[a:a + 1, :]

    buckets = map_ref[...]
    digits = jnp.concatenate([(buckets & 1016).astype(F32), (buckets & 7).astype(F32)], axis=1).astype(BF16)
    step = 512
    for c in range(count // step):
        at = slice(c * step, (c + 1) * step)
        face = row_ref[0:1, at]
        hot = one_hot(face & (LANES - 1), LANES)
        value = jnp.dot(digits, jnp.concatenate([hot, hot], axis=0), preferred_element_type=F32)
        numbers = lax.broadcasted_iota(jnp.int32, (blocks, step), 0)
        rank_ref[0:1, at] = jnp.sum(jnp.where(numbers == (face >> 7), value, 0.0), axis=0, keepdims=True)

    earlier = (lax.broadcasted_iota(jnp.int32, (LANES, LANES), 0)
               < lax.broadcasted_iota(jnp.int32, (LANES, LANES), 1))
    counts, picks = [], []
    for t in range(tiles):
        at = slice(t * LANES, (t + 1) * LANES)
        mine = rank_ref[0:1, at]
        other = jnp.broadcast_to(mine, (LANES, LANES)).T
        other_ref[at, :] = other
        hit = jnp.where((other == mine) & earlier, 1.0, 0.0)
        rank_ref[1:2, at] = jnp.sum(hit, axis=0, keepdims=True)
        bucket = mine.astype(jnp.int32)
        hot = one_hot(bucket >> 3, LANES)
        owner_hot[:, at] = hot
        picks.append(lax.broadcasted_iota(jnp.int32, (16, LANES), 0) == (bucket & 7))
        inner = jnp.where(picks[t], 1.0, 0.0).astype(BF16)
        counts.append(lax.dot_general(inner, hot, NT, preferred_element_type=F32))
    before = jnp.zeros((16, LANES), F32)
    for t in range(tiles):
        at = slice(t * LANES, (t + 1) * LANES)
        if t:
            before = before + counts[t - 1]
            seen = jnp.dot(before.astype(BF16), owner_hot[:, at], preferred_element_type=F32)
            rank_ref[1:2, at] += jnp.sum(jnp.where(picks[t], seen, 0.0), axis=0, keepdims=True)

    bucket = rank_ref[0:1, :].astype(jnp.int32)
    rank = rank_ref[1:2, :].astype(jnp.int32)
    owner = bucket >> 3
    inner = bucket & 7
    code_ref[0:1, :] = owner
    code_ref[1:2, :] = inner * SLOTS + rank
    lane = lax.broadcasted_iota(jnp.int32, (1, LANES), 1)
    wanted = [(lane * 8 + group * 2 + par).astype(F32) for par in range(2)]
    pair = 2 * LANES
    sources = [jnp.zeros((16, 256), F32), jnp.zeros((16, 256), F32)]
    numbers = lax.broadcasted_iota(jnp.int32, (16, pair), 0)
    for c in range(count // pair):
        at = slice(c * pair, (c + 1) * pair)
        face = row_ref[0:1, at]
        parts = jnp.where(numbers < 8, (face >> 7) + 1, face & (LANES - 1))
        left = jnp.where((numbers & 7) == rank[:, at], parts, 0).astype(F32).astype(BF16)
        other = other_ref[at, :]
        right = jnp.concatenate([jnp.where(other == want, 1.0, 0.0).astype(BF16) for want in wanted], axis=1)
        sources[c % 2] = sources[c % 2] + jnp.dot(left, right, preferred_element_type=F32)
    source = sources[0] + sources[1]

    copy.wait()
    for g in range(blocks // 16):
        row = [node_ref[pl.ds((r // 8) * blocks * 8 + r % 8 + g * 128, 16, stride=8), :] for r in range(24)]
        corner = [row[3 * m:3 * m + 3] for m in range(4)]
        motion = [row[12 + 3 * m:15 + 3 * m] for m in range(4)]
        centroid = [0.25 * (corner[0][i] + corner[1][i] + corner[2][i] + corner[3][i]) for i in range(3)]
        one = [corner[2][i] - corner[0][i] for i in range(3)]
        two = [corner[3][i] - corner[1][i] for i in range(3)]
        area = [
            0.5 * (one[1] * two[2] - one[2] * two[1]),
            0.5 * (one[2] * two[0] - one[0] * two[2]),
            0.5 * (one[0] * two[1] - one[1] * two[0]),
        ]
        velocity = [0.25 * (motion[0][i] + motion[1][i] + motion[2][i] + motion[3][i]) for i in range(3)]
        for q, value in enumerate(centroid + area + velocity):
            at = slice(q * blocks + g * 16, q * blocks + g * 16 + 16)
            first = value.astype(BF16)
            geo_ref[at, :LANES] = first
            geo_ref[at, LANES:] = (value - first.astype(F32)).astype(BF16)

    col_ref[...] = jnp.zeros(col_ref.shape, F32)
    filled = jnp.zeros((1, 256), F32)
    for k in range(SLOTS):
        high = source[k:k + 1, :].astype(jnp.int32) - 1
        low = source[8 + k:9 + k, :].astype(jnp.int32)
        filled = filled + jnp.where(high >= 0, 1.0, 0.0)
        hot = one_hot(low, LANES)
        hot = jnp.concatenate([hot, hot], axis=0)
        mine = lax.broadcasted_iota(jnp.int32, (blocks, 256), 0) == high
        for start, end in ((0, 5), (5, 9)):
            found = jnp.dot(geo_ref[start * blocks:end * blocks, :], hot, preferred_element_type=F32)
            for q in range(start, end):
                at = (q - start) * blocks
                value = jnp.sum(jnp.where(mine, found[at:at + blocks], 0.0), axis=0, keepdims=True)
                for par in range(2):
                    row = par * 64 + k * 12 + q
                    col_ref[row:row + 1, :] = value[:, par * LANES:(par + 1) * LANES]
    for par in range(2):
        col_ref[par * 64 + 60:par * 64 + 61, :] = filled[:, par * LANES:(par + 1) * LANES]
    out_ref[...] = col_ref[...].T


def force_kernel(face_ref, left_ref, seg_ref, out_ref, row_ref, right_ref, wide_ref):
    row_ref[...] = face_ref[...].T
    groups = seg_ref.shape[0] // 2
    for g in range(2 * groups):
        columns = seg_ref[g].T
        for i in range(3):
            wide_ref[g % 2, i, (g // 2) * LANES:(g // 2 + 1) * LANES, :] = jnp.broadcast_to(
                columns[:, i:i + 1], (LANES, LANES))
    out_ref[...] = jnp.zeros(out_ref.shape, F32)
    half_log2e = 0.5 * 1.4426950408889634
    number = lax.broadcasted_iota(jnp.int32, (16, LANES), 0)
    for par in range(2):
        count = jnp.sum(row_ref[par * 64 + 60:par * 64 + 61, :], axis=1, keepdims=True)
        stiff = pieces(jnp.broadcast_to(STIFFNESS * lax.rsqrt(jnp.maximum(count, 1.0)), (1, LANES)))
        for k in range(SLOTS):
            start = par * 64 + k * 12
            face = row_ref[start:start + 16, :]
            center = [row_ref[start + i:start + i + 1, :] for i in range(3)]
            square = pieces(half_log2e * (
                center[0] * center[0] + center[1] * center[1] + center[2] * center[2]))
            extra = jnp.where((number >= 6) & (number < 9), 1.0, 0.0)
            for piece in range(3):
                extra = jnp.where(number == piece, square[piece], extra)
                extra = jnp.where(number == 3 + piece, stiff[piece], extra)
            first, second, third = pieces(face)
            blocks = (first, second, third, first, second, first, extra, jnp.zeros_like(extra))
            for group, block in enumerate(blocks):
                right_ref[par, group * 16:(group + 1) * 16, k * LANES:(k + 1) * LANES] = block.astype(BF16)
    chunks = left_ref.shape[1]
    for par in range(2):
        for first in range(0, SLOTS, 2):
            width = min(2, SLOTS - first)
            right = right_ref[par, :, first * LANES:(first + width) * LANES]
            total = [[jnp.zeros((8, LANES), F32) for i in range(3)] for k in range(width)]
            for chunk in range(chunks):
                found = jnp.dot(left_ref[par, chunk], right, preferred_element_type=F32)
                normal = [wide_ref[par, i, chunk * 64:(chunk + 1) * 64, :] for i in range(3)]
                for k in range(width):
                    at = slice(k * LANES, (k + 1) * LANES)
                    weight = jnp.exp2(found[0:64, at])
                    traction = (weight * jnp.maximum(found[64:128, at], 0.0) * found[128:192, at]
                                * jnp.abs(found[192:256, at]))
                    for i in range(3):
                        total[k][i] = total[k][i] + jnp.sum(
                            (traction * normal[i]).reshape(8, 8, LANES), axis=0)
            for k in range(width):
                for i in range(3):
                    force = jnp.sum(total[k][i], axis=0, keepdims=True)
                    row = i * 10 + par * SLOTS + first + k
                    for x in range(out_ref.shape[0]):
                        out_ref[x, row:row + 1, :] = force


def pick_kernel(force_ref, code_ref, out_ref, row_ref):
    turned = force_ref[...].T
    for x in range(4):
        for i in range(3):
            row_ref[i * 40 + x * 10:i * 40 + x * 10 + 10, :] = turned[x * 32 + i * 10:x * 32 + i * 10 + 10, :]
    value = row_ref[...]
    first = value.astype(BF16)
    left = jnp.concatenate([first, (value - first.astype(F32)).astype(BF16)], axis=1)
    step = 512
    for c in range(out_ref.shape[1] // step):
        at = slice(c * step, (c + 1) * step)
        hot = one_hot(code_ref[0:1, at], LANES)
        found = jnp.dot(left, jnp.concatenate([hot, hot], axis=0), preferred_element_type=F32)
        mine = lax.broadcasted_iota(jnp.int32, (40, step), 0) == code_ref[1:2, at]
        for i in range(3):
            out_ref[i:i + 1, at] = jnp.sum(
                jnp.where(mine, found[i * 40:(i + 1) * 40], 0.0), axis=0, keepdims=True)


def local(node_data, eroded, bucket_map, seg_point, seg_angle):
    owners = lax.axis_size("elem")
    groups = lax.axis_size("bucket")
    faces = node_data.shape[1]
    blocks = faces // LANES
    uncovered = 6 * eroded.shape[0]
    vmem = pl.BlockSpec(memory_space=pltpu.VMEM)

    segs, near_eroded, near_map = pl.pallas_call(
        join_kernel,
        out_shape=(
            pltpu.VMEM((seg_point.shape[0], 5, seg_point.shape[2]), F32),
            pltpu.VMEM((uncovered // 6 // LANES, LANES), jnp.int32),
            pltpu.VMEM((blocks, LANES), jnp.int32),
        ),
        in_specs=[vmem, vmem, vmem, vmem],
        out_specs=(vmem, vmem, vmem),
        name="join",
    )(seg_point.transpose(1, 0, 2), seg_angle, eroded.reshape(-1, LANES), bucket_map.reshape(blocks, LANES))
    segs = lax.all_to_all(segs, "bucket", 0, 0, tiled=True)

    node_tiles = node_data.reshape(3, 8, blocks, LANES).transpose(0, 2, 1, 3).reshape(24 * blocks, LANES)
    packed, code = pl.pallas_call(
        pack_kernel,
        out_shape=(
            pltpu.VMEM((owners, LANES), F32),
            pltpu.VMEM((2, uncovered), jnp.int32),
        ),
        in_specs=[vmem, vmem, pl.BlockSpec(memory_space=pl.ANY)],
        out_specs=(vmem, vmem),
        scratch_shapes=[
            pltpu.VMEM((24 * blocks, LANES), F32),
            pltpu.VMEM((1, uncovered), jnp.int32),
            pltpu.VMEM((LANES, LANES), F32),
            pltpu.VMEM((uncovered, LANES), F32),
            pltpu.VMEM((2, uncovered), F32),
            pltpu.VMEM((LANES, uncovered), BF16),
            pltpu.VMEM((9 * blocks, 2 * LANES), BF16),
            pltpu.SemaphoreType.DMA,
        ],
        name="pack",
    )(near(near_eroded), near(near_map), node_tiles)

    with jax.named_scope("dispatch"):
        arrived = lax.all_to_all(packed.reshape(owners, 1, LANES), "elem", 0, 0, tiled=True)

    with jax.named_scope("coefficients"):
        left, normal = pl.pallas_call(
            coefficient_kernel,
            out_shape=(
                pltpu.VMEM((2, 2 * groups, 256, LANES), BF16),
                pltpu.VMEM((2 * groups, 8, LANES), F32),
            ),
            in_specs=[vmem],
            out_specs=(vmem, vmem),
            scratch_shapes=[pltpu.VMEM((2 * groups, 4 * LANES, LANES), F32)],
            name="coefficients",
        )(near(segs))

    force = pl.pallas_call(
        force_kernel,
        out_shape=pltpu.VMEM((groups, 32, LANES), F32),
        in_specs=[vmem, vmem, vmem],
        out_specs=vmem,
        scratch_shapes=[
            pltpu.VMEM((LANES, LANES), F32),
            pltpu.VMEM((2, LANES, SLOTS * LANES), BF16),
            pltpu.VMEM((2, 3, groups * LANES, LANES), F32),
        ],
        name="force",
    )(near(arrived.reshape(owners, LANES)), near(left), near(normal))

    shared = lax.all_to_all(force, "bucket", 0, 0, tiled=True)
    outgoing = shared.reshape(groups * 32, owners).T
    returned = lax.all_to_all(outgoing.reshape(owners, 1, LANES), "elem", 0, 0, tiled=True)

    return pl.pallas_call(
        pick_kernel,
        out_shape=jax.ShapeDtypeStruct((3, uncovered), F32),
        in_specs=[vmem, vmem],
        out_specs=vmem,
        scratch_shapes=[pltpu.VMEM((120, LANES), F32)],
        name="pick",
    )(near(returned.reshape(owners, LANES)), near(code))


def solution(mesh):
    in_specs = (
        P(None, "elem"),
        P("elem"),
        P("elem"),
        P("elem", None, "bucket"),
        P("elem", None, "bucket"),
    )
    out_specs = P(None, "elem")
    return jax.shard_map(local, mesh=mesh, in_specs=in_specs, out_specs=out_specs, check_vma=False)
```

```python
import jax
import jax.numpy as jnp
from jax import lax
from jax.experimental import pallas as pl
from jax.experimental.pallas import tpu as pltpu
from jax.sharding import Mesh, PartitionSpec as P

STIFFNESS = 20.0
DAMPING = 0.5
SLOTS = 5
LANES = 128
F32 = jnp.float32
BF16 = jnp.bfloat16
NT = (((1,), (1,)), ((), ()))


def near(value):
    return pltpu.with_memory_space_constraint(value, pltpu.VMEM)


def one_hot(row, size):
    numbers = lax.broadcasted_iota(jnp.int32, (size, row.shape[1]), 0)
    return jnp.where(numbers == row, 1.0, 0.0).astype(BF16)


def join_kernel(point_ref, angle_ref, eroded_ref, map_ref, out_ref, near_eroded_ref, near_map_ref):
    near_eroded_ref[...] = eroded_ref[...]
    near_map_ref[...] = map_ref[...]
    for i in range(3):
        out_ref[:, i, :] = point_ref[i]
    for i in range(2):
        out_ref[:, 3 + i, :] = angle_ref[:, i, :]


def pieces(value):
    first = value.astype(BF16).astype(F32)
    rest = value - first
    second = rest.astype(BF16).astype(F32)
    return first, second, rest - second


def coefficient_kernel(seg_ref, left_ref, normal_ref, rows_ref):
    rows_ref[...] = jnp.zeros(rows_ref.shape, F32)
    log2e = 1.4426950408889634
    order = (0, 0, 0, 1, 1, 2)
    azimuth, polar = seg_ref[:, 3, :], seg_ref[:, 4, :]
    ring = jnp.sin(polar)
    normal = [jnp.cos(azimuth) * ring, jnp.sin(azimuth) * ring, jnp.cos(polar)]
    point = [seg_ref[:, i, :] for i in range(3)]
    along = point[0] * normal[0] + point[1] * normal[1] + point[2] * normal[2]
    square = point[0] * point[0] + point[1] * point[1] + point[2] * point[2]
    terms = (
        (0, [log2e * value for value in point]),
        (0, [-value for value in normal]),
        (6, [-DAMPING * value for value in normal]),
        (3, normal),
    )
    split = [(start, [pieces(value) for value in values]) for start, values in terms]
    constant = [pieces((-0.5 * log2e) * square), pieces(along)]
    for term in range(4):
        at = term * LANES
        start, values = split[term]
        for group, piece in enumerate(order):
            for i in range(3):
                rows_ref[:, at + group * 16 + start + i, :] = values[i][piece]
        if term < 2:
            for piece in range(3):
                rows_ref[:, at + 96 + 6 + piece, :] = constant[term][piece]
    for piece in range(3):
        rows_ref[:, 96 + piece, :] = jnp.full_like(ring, -1.0)
        rows_ref[:, 2 * LANES + 96 + 3 + piece, :] = jnp.full_like(ring, 1.0)
    for i in range(3):
        normal_ref[:, i, :] = normal[i]
    for i in range(3, 8):
        normal_ref[:, i, :] = jnp.zeros_like(ring)
    for g in range(seg_ref.shape[0]):
        for term in range(4):
            turned = rows_ref[g, term * LANES:(term + 1) * LANES, :].T.astype(BF16)
            for half in range(2):
                left_ref[g % 2, (g // 2) * 2 + half, term * 64:(term + 1) * 64, :] = turned[half * 64:(half + 1) * 64]


def pack_kernel(eroded_ref, map_ref, node_hbm, out_ref, code_ref, node_ref, row_ref, col_ref, other_ref, rank_ref,
                owner_hot, geo_ref, sem):
    copy = pltpu.make_async_copy(node_hbm, node_ref, sem)
    copy.start()
    group = lax.axis_index("bucket")
    blocks = map_ref.shape[0]
    count = row_ref.shape[1]
    tiles = count // LANES
    rows4 = eroded_ref.shape[0]
    span = count // rows4

    eroded = eroded_ref[...]
    lane = lax.broadcasted_iota(jnp.int32, (LANES, span), 1)
    six = 6 * lax.broadcasted_iota(jnp.int32, (LANES, span), 0)
    spread = jnp.where((lane >= six) & (lane < six + 6), 1.0, 0.0).astype(BF16)
    high = jnp.dot((eroded >> 3).astype(F32).astype(BF16), spread, preferred_element_type=F32)
    low = jnp.dot((eroded & 7).astype(F32).astype(BF16), spread, preferred_element_type=F32)
    number = lax.broadcasted_iota(jnp.int32, (rows4, span), 1)
    faces4 = 6 * (high * 8.0 + low).astype(jnp.int32) + number % 6
    for a in range(rows4):
        row_ref[0:1, a * span:(a + 1) * span] = faces4[a:a + 1, :]

    buckets = map_ref[...]
    digits = jnp.concatenate([(buckets & 1016).astype(F32), (buckets & 7).astype(F32)], axis=1).astype(BF16)
    step = 512
    for c in range(count // step):
        at = slice(c * step, (c + 1) * step)
        face = row_ref[0:1, at]
        hot = one_hot(face & (LANES - 1), LANES)
        value = jnp.dot(digits, jnp.concatenate([hot, hot], axis=0), preferred_element_type=F32)
        numbers = lax.broadcasted_iota(jnp.int32, (blocks, step), 0)
        rank_ref[0:1, at] = jnp.sum(jnp.where(numbers == (face >> 7), value, 0.0), axis=0, keepdims=True)

    earlier = (lax.broadcasted_iota(jnp.int32, (LANES, LANES), 0)
               < lax.broadcasted_iota(jnp.int32, (LANES, LANES), 1))
    counts, picks = [], []
    for t in range(tiles):
        at = slice(t * LANES, (t + 1) * LANES)
        mine = rank_ref[0:1, at]
        other = jnp.broadcast_to(mine, (LANES, LANES)).T
        other_ref[at, :] = other
        hit = jnp.where((other == mine) & earlier, 1.0, 0.0)
        rank_ref[1:2, at] = jnp.sum(hit, axis=0, keepdims=True)
        bucket = mine.astype(jnp.int32)
        hot = one_hot(bucket >> 3, LANES)
        owner_hot[:, at] = hot
        picks.append(lax.broadcasted_iota(jnp.int32, (16, LANES), 0) == (bucket & 7))
        inner = jnp.where(picks[t], 1.0, 0.0).astype(BF16)
        counts.append(lax.dot_general(inner, hot, NT, preferred_element_type=F32))
    before = jnp.zeros((16, LANES), F32)
    for t in range(tiles):
        at = slice(t * LANES, (t + 1) * LANES)
        if t:
            before = before + counts[t - 1]
            seen = jnp.dot(before.astype(BF16), owner_hot[:, at], preferred_element_type=F32)
            rank_ref[1:2, at] += jnp.sum(jnp.where(picks[t], seen, 0.0), axis=0, keepdims=True)

    bucket = rank_ref[0:1, :].astype(jnp.int32)
    rank = rank_ref[1:2, :].astype(jnp.int32)
    owner = bucket >> 3
    inner = bucket & 7
    code_ref[0:1, :] = (owner & (LANES - 2)) + (inner & 1)
    code_ref[1:2, :] = ((owner & 1) * 4 + (inner >> 1)) * SLOTS + rank
    lane = lax.broadcasted_iota(jnp.int32, (1, LANES), 1)
    wanted = [(lane * 8 + group * 2 + par).astype(F32) for par in range(2)]
    pair = 2 * LANES
    sources = [jnp.zeros((16, 256), F32), jnp.zeros((16, 256), F32)]
    numbers = lax.broadcasted_iota(jnp.int32, (16, pair), 0)
    for c in range(count // pair):
        at = slice(c * pair, (c + 1) * pair)
        face = row_ref[0:1, at]
        parts = jnp.where(numbers < 8, (face >> 7) + 1, face & (LANES - 1))
        left = jnp.where((numbers & 7) == rank[:, at], parts, 0).astype(F32).astype(BF16)
        other = other_ref[at, :]
        right = jnp.concatenate([jnp.where(other == want, 1.0, 0.0).astype(BF16) for want in wanted], axis=1)
        sources[c % 2] = sources[c % 2] + jnp.dot(left, right, preferred_element_type=F32)
    source = sources[0] + sources[1]

    copy.wait()
    for g in range(blocks // 16):
        row = [node_ref[pl.ds((r // 8) * blocks * 8 + r % 8 + g * 128, 16, stride=8), :] for r in range(24)]
        corner = [row[3 * m:3 * m + 3] for m in range(4)]
        motion = [row[12 + 3 * m:15 + 3 * m] for m in range(4)]
        centroid = [0.25 * (corner[0][i] + corner[1][i] + corner[2][i] + corner[3][i]) for i in range(3)]
        one = [corner[2][i] - corner[0][i] for i in range(3)]
        two = [corner[3][i] - corner[1][i] for i in range(3)]
        area = [
            0.5 * (one[1] * two[2] - one[2] * two[1]),
            0.5 * (one[2] * two[0] - one[0] * two[2]),
            0.5 * (one[0] * two[1] - one[1] * two[0]),
        ]
        velocity = [0.25 * (motion[0][i] + motion[1][i] + motion[2][i] + motion[3][i]) for i in range(3)]
        for q, value in enumerate(centroid + area + velocity):
            at = slice(q * blocks + g * 16, q * blocks + g * 16 + 16)
            first = value.astype(BF16)
            geo_ref[at, :LANES] = first
            geo_ref[at, LANES:] = (value - first.astype(F32)).astype(BF16)

    col_ref[...] = jnp.zeros(col_ref.shape, F32)
    filled = jnp.zeros((1, 256), F32)
    for k in range(SLOTS):
        high = source[k:k + 1, :].astype(jnp.int32) - 1
        low = source[8 + k:9 + k, :].astype(jnp.int32)
        filled = filled + jnp.where(high >= 0, 1.0, 0.0)
        hot = one_hot(low, LANES)
        hot = jnp.concatenate([hot, hot], axis=0)
        mine = lax.broadcasted_iota(jnp.int32, (blocks, 256), 0) == high
        for start, end in ((0, 5), (5, 9)):
            found = jnp.dot(geo_ref[start * blocks:end * blocks, :], hot, preferred_element_type=F32)
            for q in range(start, end):
                at = (q - start) * blocks
                value = jnp.sum(jnp.where(mine, found[at:at + blocks], 0.0), axis=0, keepdims=True)
                for par in range(2):
                    row = par * 64 + k * 12 + q
                    col_ref[row:row + 1, :] = value[:, par * LANES:(par + 1) * LANES]
    for par in range(2):
        col_ref[par * 64 + 60:par * 64 + 61, :] = filled[:, par * LANES:(par + 1) * LANES]
    out_ref[...] = col_ref[...].T


def force_kernel(face_ref, left_ref, seg_ref, out_ref, row_ref, right_ref, wide_ref):
    half = LANES // 2
    row_ref[...] = jnp.concatenate([face_ref[pl.ds(core, half, stride=2), :] for core in range(2)], axis=0).T
    groups = seg_ref.shape[0] // 2
    for g in range(2 * groups):
        columns = seg_ref[g].T
        for i in range(3):
            wide_ref[g % 2, i, (g // 2) * LANES:(g // 2 + 1) * LANES, :] = jnp.broadcast_to(
                columns[:, i:i + 1], (LANES, LANES))
    half_log2e = 0.5 * 1.4426950408889634
    number = lax.broadcasted_iota(jnp.int32, (16, LANES), 0)
    for par in range(2):
        count = jnp.sum(row_ref[par * 64 + 60:par * 64 + 61, :], axis=1, keepdims=True)
        stiff = pieces(jnp.broadcast_to(STIFFNESS * lax.rsqrt(jnp.maximum(count, 1.0)), (1, LANES)))
        for k in range(SLOTS):
            start = par * 64 + k * 12
            face = row_ref[start:start + 16, :]
            center = [row_ref[start + i:start + i + 1, :] for i in range(3)]
            square = pieces(half_log2e * (
                center[0] * center[0] + center[1] * center[1] + center[2] * center[2]))
            extra = jnp.where((number >= 6) & (number < 9), 1.0, 0.0)
            for piece in range(3):
                extra = jnp.where(number == piece, square[piece], extra)
                extra = jnp.where(number == 3 + piece, stiff[piece], extra)
            first, second, third = pieces(face)
            blocks = (first, second, third, first, second, first, extra, jnp.zeros_like(extra))
            for group, block in enumerate(blocks):
                right_ref[par, group * 16:(group + 1) * 16, k * LANES:(k + 1) * LANES] = block.astype(BF16)
    chunks = left_ref.shape[1]
    for par in range(2):
        for first in range(0, SLOTS, 2):
            width = min(2, SLOTS - first)
            right = right_ref[par, :, first * LANES:(first + width) * LANES]
            total = [[jnp.zeros((8, LANES), F32) for i in range(3)] for k in range(width)]
            for chunk in range(chunks):
                found = jnp.dot(left_ref[par, chunk], right, preferred_element_type=F32)
                normal = [wide_ref[par, i, chunk * 64:(chunk + 1) * 64, :] for i in range(3)]
                for k in range(width):
                    at = slice(k * LANES, (k + 1) * LANES)
                    weight = jnp.exp2(found[0:64, at])
                    traction = (weight * jnp.maximum(found[64:128, at], 0.0) * found[128:192, at]
                                * jnp.abs(found[192:256, at]))
                    for i in range(3):
                        total[k][i] = total[k][i] + jnp.sum(
                            (traction * normal[i]).reshape(8, 8, LANES), axis=0)
            for k in range(width):
                for i in range(3):
                    row = par * 16 + i * SLOTS + first + k
                    row_ref[row:row + 1, :] = jnp.sum(total[k][i], axis=0, keepdims=True)
        row_ref[par * 16 + 15:par * 16 + 16, :] = jnp.zeros((1, LANES), F32)
    for core in range(2):
        at = slice(core * half, (core + 1) * half)
        both = jnp.concatenate([row_ref[0:16, at], row_ref[16:32, at]], axis=1)
        for x in range(4):
            out_ref[core * 4 + x] = both


def pick_kernel(force_ref, code_ref, out_ref, row_ref):
    turned = force_ref[...].T
    for g in range(8):
        for i in range(3):
            to, start = i * 40 + g * SLOTS, g * 16 + i * SLOTS
            row_ref[to:to + SLOTS, :] = turned[start:start + SLOTS, :]
    value = row_ref[...]
    first = value.astype(BF16)
    left = jnp.concatenate([first, (value - first.astype(F32)).astype(BF16)], axis=1)
    step = 512
    for c in range(out_ref.shape[1] // step):
        at = slice(c * step, (c + 1) * step)
        hot = one_hot(code_ref[0:1, at], LANES)
        found = jnp.dot(left, jnp.concatenate([hot, hot], axis=0), preferred_element_type=F32)
        mine = lax.broadcasted_iota(jnp.int32, (40, step), 0) == code_ref[1:2, at]
        for i in range(3):
            out_ref[i:i + 1, at] = jnp.sum(
                jnp.where(mine, found[i * 40:(i + 1) * 40], 0.0), axis=0, keepdims=True)


def local(node_data, eroded, bucket_map, seg_point, seg_angle):
    owners = lax.axis_size(("chip", "core"))
    groups = lax.axis_size("bucket")
    faces = node_data.shape[1]
    blocks = faces // LANES
    uncovered = 6 * eroded.shape[0]
    vmem = pl.BlockSpec(memory_space=pltpu.VMEM)

    segs, near_eroded, near_map = pl.pallas_call(
        join_kernel,
        out_shape=(
            pltpu.VMEM((seg_point.shape[0], 5, seg_point.shape[2]), F32),
            pltpu.VMEM((uncovered // 6 // LANES, LANES), jnp.int32),
            pltpu.VMEM((blocks, LANES), jnp.int32),
        ),
        in_specs=[vmem, vmem, vmem, vmem],
        out_specs=(vmem, vmem, vmem),
        name="join",
    )(seg_point.transpose(1, 0, 2), seg_angle, eroded.reshape(-1, LANES), bucket_map.reshape(blocks, LANES))
    segs = lax.all_to_all(segs, "bucket", 0, 0, tiled=True)

    node_tiles = node_data.reshape(3, 8, blocks, LANES).transpose(0, 2, 1, 3).reshape(24 * blocks, LANES)
    packed, code = pl.pallas_call(
        pack_kernel,
        out_shape=(
            pltpu.VMEM((owners, LANES), F32),
            pltpu.VMEM((2, uncovered), jnp.int32),
        ),
        in_specs=[vmem, vmem, pl.BlockSpec(memory_space=pl.ANY)],
        out_specs=(vmem, vmem),
        scratch_shapes=[
            pltpu.VMEM((24 * blocks, LANES), F32),
            pltpu.VMEM((1, uncovered), jnp.int32),
            pltpu.VMEM((LANES, LANES), F32),
            pltpu.VMEM((uncovered, LANES), F32),
            pltpu.VMEM((2, uncovered), F32),
            pltpu.VMEM((LANES, uncovered), BF16),
            pltpu.VMEM((9 * blocks, 2 * LANES), BF16),
            pltpu.SemaphoreType.DMA,
        ],
        name="pack",
    )(near(near_eroded), near(near_map), node_tiles)

    with jax.named_scope("dispatch"):
        arrived = lax.all_to_all(packed.reshape(owners, 1, LANES), ("chip", "core"), 0, 0, tiled=True)

    with jax.named_scope("coefficients"):
        left, normal = pl.pallas_call(
            coefficient_kernel,
            out_shape=(
                pltpu.VMEM((2, 2 * groups, 256, LANES), BF16),
                pltpu.VMEM((2 * groups, 8, LANES), F32),
            ),
            in_specs=[vmem],
            out_specs=(vmem, vmem),
            scratch_shapes=[pltpu.VMEM((2 * groups, 4 * LANES, LANES), F32)],
            name="coefficients",
        )(near(segs))

    force = pl.pallas_call(
        force_kernel,
        out_shape=pltpu.VMEM((2 * groups, 16, LANES), F32),
        in_specs=[vmem, vmem, vmem],
        out_specs=vmem,
        scratch_shapes=[
            pltpu.VMEM((LANES, LANES), F32),
            pltpu.VMEM((2, LANES, SLOTS * LANES), BF16),
            pltpu.VMEM((2, 3, groups * LANES, LANES), F32),
        ],
        name="force",
    )(near(arrived.reshape(owners, LANES)), near(left), near(normal))

    shared = lax.all_to_all(force, ("core", "bucket"), 0, 0, tiled=True)
    outgoing = shared.reshape(groups * 32, 2, owners // 2).transpose(2, 1, 0)
    returned = lax.all_to_all(outgoing, "chip", 0, 0, tiled=True)

    return pl.pallas_call(
        pick_kernel,
        out_shape=jax.ShapeDtypeStruct((3, uncovered), F32),
        in_specs=[vmem, vmem],
        out_specs=vmem,
        scratch_shapes=[pltpu.VMEM((120, LANES), F32)],
        name="pick",
    )(near(returned.reshape(owners, LANES)), near(code))


def solution(mesh):
    split = Mesh(mesh.devices.reshape(-1, 2, mesh.shape["bucket"]), ("chip", "core", "bucket"))
    elem = ("chip", "core")
    in_specs = (P(None, elem), P(elem), P(elem), P(elem, None, "bucket"), P(elem, None, "bucket"))
    return jax.shard_map(local, mesh=split, in_specs=in_specs, out_specs=P(None, elem), check_vma=False)
```

```python
import functools

import jax
import jax.numpy as jnp
from jax import lax
from jax.experimental import pallas as pl
from jax.experimental.pallas import tpu as pltpu
from jax.sharding import Mesh, PartitionSpec as P

STIFFNESS = 20.0
DAMPING = 0.5
SLOTS = 5
LANES = 128
F32 = jnp.float32
BF16 = jnp.bfloat16
NT = (((1,), (1,)), ((), ()))


def near(value):
    return pltpu.with_memory_space_constraint(value, pltpu.VMEM)


def one_hot(row, size):
    numbers = lax.broadcasted_iota(jnp.int32, (size, row.shape[1]), 0)
    return jnp.where(numbers == row, 1.0, 0.0).astype(BF16)


def join_kernel(point_hbm, angle_hbm, eroded_hbm, map_hbm, node_hbm, out_hbm, near_eroded_ref, near_map_ref,
                near_node_ref, point_ref, angle_ref, out_ref, sem):
    part = near_node_ref.shape[0] // 3
    pairs = [(point_hbm, point_ref), (angle_hbm, angle_ref), (eroded_hbm, near_eroded_ref), (map_hbm, near_map_ref)]
    for i in range(3):
        at = pl.ds(i * part, part)
        pairs.append((node_hbm.at[at, :], near_node_ref.at[at, :]))
    copies = [pltpu.make_async_copy(source, target, sem.at[i]) for i, (source, target) in enumerate(pairs)]
    for copy in copies:
        copy.start()
    for copy in copies[:2]:
        copy.wait()
    for i in range(3):
        out_ref[:, i, :] = point_ref[i]
    for i in range(2):
        out_ref[:, 3 + i, :] = angle_ref[:, i, :]
    away = pltpu.make_async_copy(out_ref, out_hbm, sem.at[7])
    away.start()
    for copy in copies[2:]:
        copy.wait()
    away.wait()


def pieces(value):
    first = value.astype(BF16).astype(F32)
    rest = value - first
    second = rest.astype(BF16).astype(F32)
    return first, second, rest - second


def coefficient_kernel(seg_ref, left_ref, normal_ref, rows_ref):
    rows_ref[...] = jnp.zeros(rows_ref.shape, F32)
    log2e = 1.4426950408889634
    order = (0, 0, 0, 1, 1, 2)
    azimuth, polar = seg_ref[:, 3, :], seg_ref[:, 4, :]
    ring = jnp.sin(polar)
    normal = [jnp.cos(azimuth) * ring, jnp.sin(azimuth) * ring, jnp.cos(polar)]
    point = [seg_ref[:, i, :] for i in range(3)]
    along = point[0] * normal[0] + point[1] * normal[1] + point[2] * normal[2]
    square = point[0] * point[0] + point[1] * point[1] + point[2] * point[2]
    terms = (
        (0, [log2e * value for value in point]),
        (0, [-value for value in normal]),
        (6, [-DAMPING * value for value in normal]),
        (3, normal),
    )
    split = [(start, [pieces(value) for value in values]) for start, values in terms]
    constant = [pieces((-0.5 * log2e) * square), pieces(along)]
    for term in range(4):
        at = term * LANES
        start, values = split[term]
        for group, piece in enumerate(order):
            for i in range(3):
                rows_ref[:, at + group * 16 + start + i, :] = values[i][piece]
        if term < 2:
            for piece in range(3):
                rows_ref[:, at + 96 + 6 + piece, :] = constant[term][piece]
    for piece in range(3):
        rows_ref[:, 96 + piece, :] = jnp.full_like(ring, -1.0)
        rows_ref[:, 2 * LANES + 96 + 3 + piece, :] = jnp.full_like(ring, 1.0)
    for i in range(3):
        normal_ref[:, i, :] = normal[i]
    for i in range(3, 8):
        normal_ref[:, i, :] = jnp.zeros_like(ring)
    for g in range(seg_ref.shape[0]):
        for term in range(4):
            turned = rows_ref[g, term * LANES:(term + 1) * LANES, :].T.astype(BF16)
            for half in range(2):
                left_ref[g % 2, (g // 2) * 2 + half, term * 64:(term + 1) * 64, :] = turned[half * 64:(half + 1) * 64]


def pack_kernel(eroded_ref, map_ref, node_ref, out_ref, code_ref, row_ref, col_ref, other_ref, rank_ref, owner_hot,
                geo_ref):
    group = lax.axis_index("bucket")
    blocks = map_ref.shape[0]
    count = row_ref.shape[1]
    tiles = count // LANES
    rows4 = eroded_ref.shape[0]
    span = count // rows4

    eroded = eroded_ref[...]
    lane = lax.broadcasted_iota(jnp.int32, (LANES, span), 1)
    six = 6 * lax.broadcasted_iota(jnp.int32, (LANES, span), 0)
    spread = jnp.where((lane >= six) & (lane < six + 6), 1.0, 0.0).astype(BF16)
    high = jnp.dot((eroded >> 3).astype(F32).astype(BF16), spread, preferred_element_type=F32)
    low = jnp.dot((eroded & 7).astype(F32).astype(BF16), spread, preferred_element_type=F32)
    number = lax.broadcasted_iota(jnp.int32, (rows4, span), 1)
    faces4 = 6 * (high * 8.0 + low).astype(jnp.int32) + number % 6
    for a in range(rows4):
        row_ref[0:1, a * span:(a + 1) * span] = faces4[a:a + 1, :]

    buckets = map_ref[...]
    digits = jnp.concatenate([(buckets & 1016).astype(F32), (buckets & 7).astype(F32)], axis=1).astype(BF16)
    step = 512
    for c in range(count // step):
        at = slice(c * step, (c + 1) * step)
        face = row_ref[0:1, at]
        hot = one_hot(face & (LANES - 1), LANES)
        value = jnp.dot(digits, jnp.concatenate([hot, hot], axis=0), preferred_element_type=F32)
        numbers = lax.broadcasted_iota(jnp.int32, (blocks, step), 0)
        rank_ref[0:1, at] = jnp.sum(jnp.where(numbers == (face >> 7), value, 0.0), axis=0, keepdims=True)

    earlier = (lax.broadcasted_iota(jnp.int32, (LANES, LANES), 0)
               < lax.broadcasted_iota(jnp.int32, (LANES, LANES), 1))
    counts, picks = [], []
    for t in range(tiles):
        at = slice(t * LANES, (t + 1) * LANES)
        mine = rank_ref[0:1, at]
        other = jnp.broadcast_to(mine, (LANES, LANES)).T
        other_ref[at, :] = other
        hit = jnp.where((other == mine) & earlier, 1.0, 0.0)
        rank_ref[1:2, at] = jnp.sum(hit, axis=0, keepdims=True)
        bucket = mine.astype(jnp.int32)
        hot = one_hot(bucket >> 3, LANES)
        owner_hot[:, at] = hot
        picks.append(lax.broadcasted_iota(jnp.int32, (16, LANES), 0) == (bucket & 7))
        inner = jnp.where(picks[t], 1.0, 0.0).astype(BF16)
        counts.append(lax.dot_general(inner, hot, NT, preferred_element_type=F32))
    before = jnp.zeros((16, LANES), F32)
    for t in range(tiles):
        at = slice(t * LANES, (t + 1) * LANES)
        if t:
            before = before + counts[t - 1]
            seen = jnp.dot(before.astype(BF16), owner_hot[:, at], preferred_element_type=F32)
            rank_ref[1:2, at] += jnp.sum(jnp.where(picks[t], seen, 0.0), axis=0, keepdims=True)

    bucket = rank_ref[0:1, :].astype(jnp.int32)
    rank = rank_ref[1:2, :].astype(jnp.int32)
    owner = bucket >> 3
    inner = bucket & 7
    code_ref[0:1, :] = (owner & (LANES - 2)) + (inner & 1)
    code_ref[1:2, :] = ((owner & 1) * 4 + (inner >> 1)) * SLOTS + rank
    lane = lax.broadcasted_iota(jnp.int32, (1, LANES), 1)
    wanted = [(lane * 8 + group * 2 + par).astype(F32) for par in range(2)]
    pair = 2 * LANES
    sources = []
    numbers = lax.broadcasted_iota(jnp.int32, (16, pair), 0)
    for c in range(count // pair):
        at = slice(c * pair, (c + 1) * pair)
        face = row_ref[0:1, at]
        parts = jnp.where(numbers < 8, (face >> 7) + 1, face & (LANES - 1))
        left = jnp.where((numbers & 7) == rank[:, at], parts, 0).astype(F32).astype(BF16)
        other = other_ref[at, :]
        right = jnp.concatenate([jnp.where(other == want, 1.0, 0.0).astype(BF16) for want in wanted], axis=1)
        sources.append(jnp.dot(left, right, preferred_element_type=F32))
    source = functools.reduce(jnp.add, sources)

    for g in range(blocks // 16):
        row = [node_ref[pl.ds((r // 8) * blocks * 8 + r % 8 + g * 128, 16, stride=8), :] for r in range(24)]
        corner = [row[3 * m:3 * m + 3] for m in range(4)]
        motion = [row[12 + 3 * m:15 + 3 * m] for m in range(4)]
        centroid = [0.25 * (corner[0][i] + corner[1][i] + corner[2][i] + corner[3][i]) for i in range(3)]
        one = [corner[2][i] - corner[0][i] for i in range(3)]
        two = [corner[3][i] - corner[1][i] for i in range(3)]
        area = [
            0.5 * (one[1] * two[2] - one[2] * two[1]),
            0.5 * (one[2] * two[0] - one[0] * two[2]),
            0.5 * (one[0] * two[1] - one[1] * two[0]),
        ]
        velocity = [0.25 * (motion[0][i] + motion[1][i] + motion[2][i] + motion[3][i]) for i in range(3)]
        for q, value in enumerate(centroid + area + velocity):
            at = slice(q * blocks + g * 16, q * blocks + g * 16 + 16)
            first = value.astype(BF16)
            geo_ref[at, :LANES] = first
            geo_ref[at, LANES:] = (value - first.astype(F32)).astype(BF16)

    col_ref[...] = jnp.zeros(col_ref.shape, F32)
    filled = jnp.zeros((1, 256), F32)
    for k in range(SLOTS):
        high = source[k:k + 1, :].astype(jnp.int32) - 1
        low = source[8 + k:9 + k, :].astype(jnp.int32)
        filled = filled + jnp.where(high >= 0, 1.0, 0.0)
        hot = one_hot(low, LANES)
        hot = jnp.concatenate([hot, hot], axis=0)
        numbers = lax.broadcasted_iota(jnp.int32, (8, 256), 0)
        for start, end in ((0, 5), (5, 9)):
            found = jnp.dot(geo_ref[start * blocks:end * blocks, :], hot, preferred_element_type=F32)
            values = [jnp.zeros((8, 256), F32)] * (end - start)
            for h in range(0, blocks, 8):
                mine = numbers == high - h
                for i in range(end - start):
                    values[i] = jnp.where(mine, found[i * blocks + h:i * blocks + h + 8], values[i])
            for i in range(end - start):
                value = jnp.sum(values[i], axis=0, keepdims=True)
                for par in range(2):
                    row = par * 64 + k * 12 + start + i
                    col_ref[row:row + 1, :] = value[:, par * LANES:(par + 1) * LANES]
    for par in range(2):
        col_ref[par * 64 + 60:par * 64 + 61, :] = filled[:, par * LANES:(par + 1) * LANES]
    out_ref[...] = col_ref[...].T


def force_kernel(face_ref, left_ref, seg_ref, out_ref, row_ref, right_ref, wide_ref):
    half = LANES // 2
    row_ref[...] = jnp.concatenate([face_ref[pl.ds(core, half, stride=2), :] for core in range(2)], axis=0).T
    groups = seg_ref.shape[0] // 2
    for g in range(2 * groups):
        columns = seg_ref[g].T
        for i in range(3):
            wide_ref[g % 2, i, (g // 2) * LANES:(g // 2 + 1) * LANES, :] = jnp.broadcast_to(
                columns[:, i:i + 1], (LANES, LANES))
    half_log2e = 0.5 * 1.4426950408889634
    number = lax.broadcasted_iota(jnp.int32, (16, LANES), 0)
    for par in range(2):
        count = jnp.sum(row_ref[par * 64 + 60:par * 64 + 61, :], axis=1, keepdims=True)
        stiff = pieces(jnp.broadcast_to(STIFFNESS * lax.rsqrt(jnp.maximum(count, 1.0)), (1, LANES)))
        for k in range(SLOTS):
            start = par * 64 + k * 12
            face = row_ref[start:start + 16, :]
            center = [row_ref[start + i:start + i + 1, :] for i in range(3)]
            square = pieces(half_log2e * (
                center[0] * center[0] + center[1] * center[1] + center[2] * center[2]))
            extra = jnp.where((number >= 6) & (number < 9), 1.0, 0.0)
            for piece in range(3):
                extra = jnp.where(number == piece, square[piece], extra)
                extra = jnp.where(number == 3 + piece, stiff[piece], extra)
            first, second, third = pieces(face)
            blocks = (first, second, third, first, second, first, extra, jnp.zeros_like(extra))
            for group, block in enumerate(blocks):
                right_ref[par, group * 16:(group + 1) * 16, k * LANES:(k + 1) * LANES] = block.astype(BF16)
    chunks = left_ref.shape[1]
    for par in range(2):
        for first in range(0, SLOTS, 2):
            width = min(2, SLOTS - first)
            right = right_ref[par, :, first * LANES:(first + width) * LANES]
            total = [[jnp.zeros((8, LANES), F32) for i in range(3)] for k in range(width)]
            for chunk in range(chunks):
                found = jnp.dot(left_ref[par, chunk], right, preferred_element_type=F32)
                normal = [wide_ref[par, i, chunk * 64:(chunk + 1) * 64, :] for i in range(3)]
                for k in range(width):
                    at = slice(k * LANES, (k + 1) * LANES)
                    weight = jnp.exp2(found[0:64, at])
                    traction = (weight * jnp.maximum(found[64:128, at], 0.0) * found[128:192, at]
                                * jnp.abs(found[192:256, at]))
                    for i in range(3):
                        total[k][i] = total[k][i] + jnp.sum(
                            (traction * normal[i]).reshape(8, 8, LANES), axis=0)
            for k in range(width):
                for i in range(3):
                    row = par * 16 + i * SLOTS + first + k
                    row_ref[row:row + 1, :] = jnp.sum(total[k][i], axis=0, keepdims=True)
        row_ref[par * 16 + 15:par * 16 + 16, :] = jnp.zeros((1, LANES), F32)
    for core in range(2):
        at = slice(core * half, (core + 1) * half)
        both = jnp.concatenate([row_ref[0:16, at], row_ref[16:32, at]], axis=1)
        for x in range(4):
            out_ref[core * 4 + x] = both


def pick_kernel(force_ref, code_ref, out_ref, row_ref):
    turned = force_ref[...].T
    for g in range(8):
        for i in range(3):
            to, start = i * 40 + g * SLOTS, g * 16 + i * SLOTS
            row_ref[to:to + SLOTS, :] = turned[start:start + SLOTS, :]
    value = row_ref[...]
    first = value.astype(BF16)
    left = jnp.concatenate([first, (value - first.astype(F32)).astype(BF16)], axis=1)
    step = 512
    for c in range(out_ref.shape[1] // step):
        at = slice(c * step, (c + 1) * step)
        hot = one_hot(code_ref[0:1, at], LANES)
        found = jnp.dot(left, jnp.concatenate([hot, hot], axis=0), preferred_element_type=F32)
        mine = lax.broadcasted_iota(jnp.int32, (40, step), 0) == code_ref[1:2, at]
        for i in range(3):
            out_ref[i:i + 1, at] = jnp.sum(
                jnp.where(mine, found[i * 40:(i + 1) * 40], 0.0), axis=0, keepdims=True)


def local(node_data, eroded, bucket_map, seg_point, seg_angle):
    owners = lax.axis_size(("chip", "core"))
    groups = lax.axis_size("bucket")
    faces = node_data.shape[1]
    blocks = faces // LANES
    uncovered = 6 * eroded.shape[0]
    vmem = pl.BlockSpec(memory_space=pltpu.VMEM)
    anywhere = pl.BlockSpec(memory_space=pl.ANY)

    node_tiles = node_data.reshape(3, 8, blocks, LANES).transpose(0, 2, 1, 3).reshape(24 * blocks, LANES)
    segs, near_eroded, near_map, near_node = pl.pallas_call(
        join_kernel,
        out_shape=(
            jax.ShapeDtypeStruct((seg_point.shape[0], 5, seg_point.shape[2]), F32),
            pltpu.VMEM((uncovered // 6 // LANES, LANES), jnp.int32),
            pltpu.VMEM((blocks, LANES), jnp.int32),
            pltpu.VMEM((24 * blocks, LANES), F32),
        ),
        in_specs=[anywhere] * 5,
        out_specs=(anywhere, vmem, vmem, vmem),
        scratch_shapes=[
            pltpu.VMEM((3, seg_point.shape[0], seg_point.shape[2]), F32),
            pltpu.VMEM(seg_angle.shape, F32),
            pltpu.VMEM((seg_point.shape[0], 5, seg_point.shape[2]), F32),
            pltpu.SemaphoreType.DMA((8,)),
        ],
        name="join",
    )(seg_point.transpose(1, 0, 2), seg_angle, eroded.reshape(-1, LANES), bucket_map.reshape(blocks, LANES), node_tiles)
    segs = lax.all_to_all(segs, "bucket", 0, 0, tiled=True)

    packed, code = pl.pallas_call(
        pack_kernel,
        out_shape=(
            pltpu.VMEM((owners, LANES), F32),
            pltpu.VMEM((2, uncovered), jnp.int32),
        ),
        in_specs=[vmem, vmem, vmem],
        out_specs=(vmem, vmem),
        scratch_shapes=[
            pltpu.VMEM((1, uncovered), jnp.int32),
            pltpu.VMEM((LANES, LANES), F32),
            pltpu.VMEM((uncovered, LANES), F32),
            pltpu.VMEM((2, uncovered), F32),
            pltpu.VMEM((LANES, uncovered), BF16),
            pltpu.VMEM((9 * blocks, 2 * LANES), BF16),
        ],
        name="pack",
    )(near(near_eroded), near(near_map), near(near_node))

    with jax.named_scope("dispatch"):
        arrived = lax.all_to_all(packed.reshape(owners, 1, LANES), ("chip", "core"), 0, 0, tiled=True)

    with jax.named_scope("coefficients"):
        left, normal = pl.pallas_call(
            coefficient_kernel,
            out_shape=(
                pltpu.VMEM((2, 2 * groups, 256, LANES), BF16),
                pltpu.VMEM((2 * groups, 8, LANES), F32),
            ),
            in_specs=[vmem],
            out_specs=(vmem, vmem),
            scratch_shapes=[pltpu.VMEM((2 * groups, 4 * LANES, LANES), F32)],
            name="coefficients",
        )(near(segs))

    force = pl.pallas_call(
        force_kernel,
        out_shape=pltpu.VMEM((2 * groups, 16, LANES), F32),
        in_specs=[vmem, vmem, vmem],
        out_specs=vmem,
        scratch_shapes=[
            pltpu.VMEM((LANES, LANES), F32),
            pltpu.VMEM((2, LANES, SLOTS * LANES), BF16),
            pltpu.VMEM((2, 3, groups * LANES, LANES), F32),
        ],
        name="force",
    )(near(arrived.reshape(owners, LANES)), near(left), near(normal))

    shared = lax.all_to_all(force, ("core", "bucket"), 0, 0, tiled=True)
    outgoing = shared.reshape(groups * 32, 2, owners // 2).transpose(2, 1, 0)
    returned = lax.all_to_all(outgoing, "chip", 0, 0, tiled=True)

    return pl.pallas_call(
        pick_kernel,
        out_shape=jax.ShapeDtypeStruct((3, uncovered), F32),
        in_specs=[vmem, vmem],
        out_specs=vmem,
        scratch_shapes=[pltpu.VMEM((120, LANES), F32)],
        name="pick",
    )(near(returned.reshape(owners, LANES)), near(code))


def solution(mesh):
    split = Mesh(mesh.devices.reshape(-1, 2, mesh.shape["bucket"]), ("chip", "core", "bucket"))
    elem = ("chip", "core")
    in_specs = (P(None, elem), P(elem), P(elem), P(elem, None, "bucket"), P(elem, None, "bucket"))
    return jax.shard_map(local, mesh=split, in_specs=in_specs, out_specs=P(None, elem), check_vma=False)
```

```python
import functools

import jax
import jax.numpy as jnp
from jax import lax
from jax.experimental import pallas as pl
from jax.experimental.pallas import tpu as pltpu
from jax.sharding import Mesh, PartitionSpec as P

STIFFNESS = 20.0
DAMPING = 0.5
SLOTS = 5
LANES = 128
F32 = jnp.float32
BF16 = jnp.bfloat16
NT = (((1,), (1,)), ((), ()))


def near(value):
    return pltpu.with_memory_space_constraint(value, pltpu.VMEM)


def one_hot(row, size):
    numbers = lax.broadcasted_iota(jnp.int32, (size, row.shape[1]), 0)
    return jnp.where(numbers == row, 1.0, 0.0).astype(BF16)


def start_kernel(point_hbm, angle_hbm, eroded_hbm, map_hbm, node_hbm, out_hbm, node_ref, row_ref, bucket_ref, hot_ref,
                 count_ref, point_ref, angle_ref, eroded_ref, map_ref, out_ref, sem):
    part = node_ref.shape[0] // 3
    pairs = [(eroded_hbm, eroded_ref), (map_hbm, map_ref), (point_hbm, point_ref), (angle_hbm, angle_ref)]
    for i in range(3):
        at = pl.ds(i * part, part)
        pairs.append((node_hbm.at[at, :], node_ref.at[at, :]))
    copies = [pltpu.make_async_copy(source, target, sem.at[i]) for i, (source, target) in enumerate(pairs)]
    for copy in copies:
        copy.start()
    blocks = map_ref.shape[0]
    count = row_ref.shape[1]
    rows4 = eroded_ref.shape[0]
    span = count // rows4
    copies[0].wait()

    eroded = eroded_ref[...]
    lane = lax.broadcasted_iota(jnp.int32, (LANES, span), 1)
    six = 6 * lax.broadcasted_iota(jnp.int32, (LANES, span), 0)
    spread = jnp.where((lane >= six) & (lane < six + 6), 1.0, 0.0).astype(BF16)
    high = jnp.dot((eroded >> 3).astype(F32).astype(BF16), spread, preferred_element_type=F32)
    low = jnp.dot((eroded & 7).astype(F32).astype(BF16), spread, preferred_element_type=F32)
    number = lax.broadcasted_iota(jnp.int32, (rows4, span), 1)
    faces4 = 6 * (high * 8.0 + low).astype(jnp.int32) + number % 6
    for a in range(rows4):
        row_ref[0:1, a * span:(a + 1) * span] = faces4[a:a + 1, :]
    copies[1].wait()
    buckets = map_ref[...]
    digits = jnp.concatenate([(buckets & 1016).astype(F32), (buckets & 7).astype(F32)], axis=1).astype(BF16)
    step = 512
    for c in range(count // step):
        at = slice(c * step, (c + 1) * step)
        face = row_ref[0:1, at]
        hot = one_hot(face & (LANES - 1), LANES)
        value = jnp.dot(digits, jnp.concatenate([hot, hot], axis=0), preferred_element_type=F32)
        numbers = lax.broadcasted_iota(jnp.int32, (blocks, step), 0)
        bucket_ref[0:1, at] = jnp.sum(jnp.where(numbers == (face >> 7), value, 0.0), axis=0, keepdims=True)
    total = jnp.zeros((16, LANES), F32)
    for t in range(count // LANES):
        at = slice(t * LANES, (t + 1) * LANES)
        bucket = bucket_ref[0:1, at].astype(jnp.int32)
        hot = one_hot(bucket >> 3, LANES)
        hot_ref[:, at] = hot
        inner = one_hot(bucket & 7, 16)
        found = lax.dot_general(inner, hot, NT, preferred_element_type=F32)
        count_ref[t * 16:(t + 1) * 16, :] = found
        total = total + found

    copies[2].wait()
    copies[3].wait()
    for core in range(2):
        at = slice(core * 8, core * 8 + 8)
        for i in range(3):
            out_ref[at, i, :] = point_ref[i]
        for i in range(2):
            out_ref[at, 3 + i, :] = angle_ref[:, i, :]
        out_ref[at, 5, :] = total[0:8]
    away = pltpu.make_async_copy(out_ref, out_hbm, sem.at[7])
    away.start()
    for copy in copies[4:]:
        copy.wait()
    away.wait()


def pieces(value):
    first = value.astype(BF16).astype(F32)
    rest = value - first
    second = rest.astype(BF16).astype(F32)
    return first, second, rest - second


def coefficient_kernel(seg_ref, left_ref, normal_ref, rows_ref):
    rows_ref[...] = jnp.zeros(rows_ref.shape, F32)
    log2e = 1.4426950408889634
    order = (0, 0, 0, 1, 1, 2)
    azimuth, polar = seg_ref[:, 3, :], seg_ref[:, 4, :]
    ring = jnp.sin(polar)
    normal = [jnp.cos(azimuth) * ring, jnp.sin(azimuth) * ring, jnp.cos(polar)]
    point = [seg_ref[:, i, :] for i in range(3)]
    along = point[0] * normal[0] + point[1] * normal[1] + point[2] * normal[2]
    square = point[0] * point[0] + point[1] * point[1] + point[2] * point[2]
    terms = (
        (0, [log2e * value for value in point]),
        (0, [-value for value in normal]),
        (6, [-DAMPING * value for value in normal]),
        (3, normal),
    )
    split = [(start, [pieces(value) for value in values]) for start, values in terms]
    constant = [pieces((-0.5 * log2e) * square), pieces(along)]
    for term in range(4):
        at = term * LANES
        start, values = split[term]
        for group, piece in enumerate(order):
            for i in range(3):
                rows_ref[:, at + group * 16 + start + i, :] = values[i][piece]
        if term < 2:
            for piece in range(3):
                rows_ref[:, at + 96 + 6 + piece, :] = constant[term][piece]
    for piece in range(3):
        rows_ref[:, 96 + piece, :] = jnp.full_like(ring, -1.0)
        rows_ref[:, 2 * LANES + 96 + 3 + piece, :] = jnp.full_like(ring, 1.0)
    for i in range(3):
        normal_ref[:, i, :] = normal[i]
    for i in range(3, 8):
        normal_ref[:, i, :] = jnp.zeros_like(ring)
    for g in range(seg_ref.shape[0]):
        inner = slice(g // 8 * LANES, (g // 8 + 1) * LANES)
        for term in range(4):
            turned = rows_ref[g, term * LANES:(term + 1) * LANES, :].T.astype(BF16)
            for half in range(2):
                left_ref[g % 2, (g % 8) // 2 * 2 + half, term * 64:(term + 1) * 64, inner] = (
                    turned[half * 64:(half + 1) * 64])


def pack_kernel(row_ref, bucket_ref, hot_ref, count_ref, node_ref, col_ref, code_ref, other_ref, rank_ref, geo_ref):
    group = lax.axis_index("bucket")
    count = row_ref.shape[1]
    tiles = count // LANES
    blocks = geo_ref.shape[0] // 9

    earlier = (lax.broadcasted_iota(jnp.int32, (LANES, LANES), 0)
               < lax.broadcasted_iota(jnp.int32, (LANES, LANES), 1))
    before = jnp.zeros((16, LANES), F32)
    for t in range(tiles):
        at = slice(t * LANES, (t + 1) * LANES)
        mine = bucket_ref[0:1, at]
        other = jnp.broadcast_to(mine, (LANES, LANES)).T
        other_ref[at, :] = other
        hit = jnp.where((other == mine) & earlier, 1.0, 0.0)
        rank = jnp.sum(hit, axis=0, keepdims=True)
        if t:
            before = before + count_ref[(t - 1) * 16:t * 16, :]
            seen = jnp.dot(before.astype(BF16), hot_ref[:, at], preferred_element_type=F32)
            picked = lax.broadcasted_iota(jnp.int32, (16, LANES), 0) == (mine.astype(jnp.int32) & 7)
            rank = rank + jnp.sum(jnp.where(picked, seen, 0.0), axis=0, keepdims=True)
        rank_ref[0:1, at] = rank

    bucket = bucket_ref[0:1, :].astype(jnp.int32)
    rank = rank_ref[0:1, :].astype(jnp.int32)
    code_ref[0:1, :] = bucket >> 3
    code_ref[1:2, :] = (bucket & 7) * SLOTS + rank
    lane = lax.broadcasted_iota(jnp.int32, (1, LANES), 1)
    wanted = [(lane * 8 + group * 2 + par).astype(F32) for par in range(2)]
    pair = 2 * LANES
    sources = []
    numbers = lax.broadcasted_iota(jnp.int32, (16, pair), 0)
    for c in range(count // pair):
        at = slice(c * pair, (c + 1) * pair)
        face = row_ref[0:1, at]
        parts = jnp.where(numbers < 8, (face >> 7) + 1, face & (LANES - 1))
        left = jnp.where((numbers & 7) == rank[:, at], parts, 0).astype(F32).astype(BF16)
        other = other_ref[at, :]
        right = jnp.concatenate([jnp.where(other == want, 1.0, 0.0).astype(BF16) for want in wanted], axis=1)
        sources.append(jnp.dot(left, right, preferred_element_type=F32))
    source = functools.reduce(jnp.add, sources)

    for g in range(blocks // 16):
        row = [node_ref[pl.ds((r // 8) * blocks * 8 + r % 8 + g * 128, 16, stride=8), :] for r in range(24)]
        corner = [row[3 * m:3 * m + 3] for m in range(4)]
        motion = [row[12 + 3 * m:15 + 3 * m] for m in range(4)]
        centroid = [0.25 * (corner[0][i] + corner[1][i] + corner[2][i] + corner[3][i]) for i in range(3)]
        one = [corner[2][i] - corner[0][i] for i in range(3)]
        two = [corner[3][i] - corner[1][i] for i in range(3)]
        area = [
            0.5 * (one[1] * two[2] - one[2] * two[1]),
            0.5 * (one[2] * two[0] - one[0] * two[2]),
            0.5 * (one[0] * two[1] - one[1] * two[0]),
        ]
        velocity = [0.25 * (motion[0][i] + motion[1][i] + motion[2][i] + motion[3][i]) for i in range(3)]
        for q, value in enumerate(centroid + area + velocity):
            at = slice(q * blocks + g * 16, q * blocks + g * 16 + 16)
            first = value.astype(BF16)
            geo_ref[at, :LANES] = first
            geo_ref[at, LANES:] = (value - first.astype(F32)).astype(BF16)

    col_ref[...] = jnp.zeros(col_ref.shape, F32)
    filled = jnp.zeros((1, 256), F32)
    for k in range(SLOTS):
        high = source[k:k + 1, :].astype(jnp.int32) - 1
        low = source[8 + k:9 + k, :].astype(jnp.int32)
        filled = filled + jnp.where(high >= 0, 1.0, 0.0)
        hot = one_hot(low, LANES)
        hot = jnp.concatenate([hot, hot], axis=0)
        numbers = lax.broadcasted_iota(jnp.int32, (8, 256), 0)
        for start, end in ((0, 5), (5, 9)):
            found = jnp.dot(geo_ref[start * blocks:end * blocks, :], hot, preferred_element_type=F32)
            values = [jnp.zeros((8, 256), F32)] * (end - start)
            for h in range(0, blocks, 8):
                mine = numbers == high - h
                for i in range(end - start):
                    values[i] = jnp.where(mine, found[i * blocks + h:i * blocks + h + 8], values[i])
            for i in range(end - start):
                value = jnp.sum(values[i], axis=0, keepdims=True)
                for par in range(2):
                    row = par * 64 + k * 12 + start + i
                    col_ref[row:row + 1, :] = value[:, par * LANES:(par + 1) * LANES]
    for par in range(2):
        col_ref[par * 64 + 60:par * 64 + 61, :] = filled[:, par * LANES:(par + 1) * LANES]


def send_kernel(col_ref, seg_ref, out_ref, all_ref):
    all_ref[...] = col_ref[...]
    peer = (1 - lax.axis_index("core")) * 8 + lax.axis_index("bucket") * 2
    for par in range(2):
        all_ref[par * 64 + 61:par * 64 + 62, :] = seg_ref[peer + par, 5:6, :]
    out_ref[...] = all_ref[...].T


def force_kernel(face_ref, left_ref, seg_ref, out_ref, row_ref, right_ref, wide_ref):
    half = LANES // 2
    row_ref[...] = jnp.concatenate([face_ref[pl.ds(core, half, stride=2), :] for core in range(2)], axis=0).T
    lane = lax.broadcasted_iota(jnp.int32, (LANES, LANES), 1)
    lower = lane < half
    columns = seg_ref[...].reshape(LANES, LANES).T
    for par in range(2):
        for x in range(4):
            for i in range(3):
                pair = [columns[:, g * 8 + i:g * 8 + i + 1] for g in (x * 2 + par, 8 + x * 2 + par)]
                wide = [jnp.broadcast_to(value, (LANES, LANES)) for value in pair]
                wide_ref[par, i, x * LANES:(x + 1) * LANES, :] = jnp.where(lower, wide[0], wide[1])
    first_core = lower[0:1, :]
    half_log2e = 0.5 * 1.4426950408889634
    number = lax.broadcasted_iota(jnp.int32, (16, LANES), 0)
    number_lane = lax.broadcasted_iota(jnp.int32, (16, LANES), 1)
    for par in range(2):
        count = row_ref[par * 64 + 60:par * 64 + 61, :] + row_ref[par * 64 + 61:par * 64 + 62, :]
        sums = [jnp.sum(jnp.where(mine, count, 0.0), axis=1, keepdims=True) for mine in (first_core, ~first_core)]
        count = jnp.where(first_core, sums[0], sums[1])
        stiff = pieces(STIFFNESS * lax.rsqrt(jnp.maximum(count, 1.0)))
        for k in range(SLOTS):
            start = par * 64 + k * 12
            face = row_ref[start:start + 16, :]
            center = [row_ref[start + i:start + i + 1, :] for i in range(3)]
            square = pieces(half_log2e * (
                center[0] * center[0] + center[1] * center[1] + center[2] * center[2]))
            extra = jnp.where((number >= 6) & (number < 9), 1.0, 0.0)
            for piece in range(3):
                extra = jnp.where(number == piece, square[piece], extra)
                extra = jnp.where(number == 3 + piece, stiff[piece], extra)
            first, second, third = pieces(face)
            blocks = (first, second, third, first, second, first, extra, jnp.zeros_like(extra))
            for group, block in enumerate(blocks):
                for core, mine in enumerate((number_lane < half, number_lane >= half)):
                    at = core * LANES + group * 16
                    right_ref[par, at:at + 16, k * LANES:(k + 1) * LANES] = jnp.where(mine, block, 0.0).astype(BF16)
    chunks = left_ref.shape[1]
    for par in range(2):
        for first in range(0, SLOTS, 2):
            width = min(2, SLOTS - first)
            right = right_ref[par, :, first * LANES:(first + width) * LANES]
            total = [[jnp.zeros((8, LANES), F32) for i in range(3)] for k in range(width)]
            for chunk in range(chunks):
                found = jnp.dot(left_ref[par, chunk], right, preferred_element_type=F32)
                normal = [wide_ref[par, i, chunk * 64:(chunk + 1) * 64, :] for i in range(3)]
                for k in range(width):
                    at = slice(k * LANES, (k + 1) * LANES)
                    weight = jnp.exp2(found[0:64, at])
                    traction = (weight * jnp.maximum(found[64:128, at], 0.0) * found[128:192, at]
                                * jnp.abs(found[192:256, at]))
                    for i in range(3):
                        total[k][i] = total[k][i] + jnp.sum(
                            (traction * normal[i]).reshape(8, 8, LANES), axis=0)
            for k in range(width):
                for i in range(3):
                    row = par * 16 + i * SLOTS + first + k
                    row_ref[row:row + 1, :] = jnp.sum(total[k][i], axis=0, keepdims=True)
        row_ref[par * 16 + 15:par * 16 + 16, :] = jnp.zeros((1, LANES), F32)
    for x in range(4):
        out_ref[x] = row_ref[0:32, :]


def pick_kernel(force_ref, code_ref, out_ref, row_ref):
    turned = force_ref[...].T
    for g in range(8):
        for i in range(3):
            to, start = i * 40 + g * SLOTS, g * 16 + i * SLOTS
            row_ref[to:to + SLOTS, :] = turned[start:start + SLOTS, :]
    value = row_ref[...]
    first = value.astype(BF16)
    left = jnp.concatenate([first, (value - first.astype(F32)).astype(BF16)], axis=1)
    step = 512
    for c in range(out_ref.shape[1] // step):
        at = slice(c * step, (c + 1) * step)
        hot = one_hot(code_ref[0:1, at], LANES)
        found = jnp.dot(left, jnp.concatenate([hot, hot], axis=0), preferred_element_type=F32)
        mine = lax.broadcasted_iota(jnp.int32, (40, step), 0) == code_ref[1:2, at]
        for i in range(3):
            out_ref[i:i + 1, at] = jnp.sum(
                jnp.where(mine, found[i * 40:(i + 1) * 40], 0.0), axis=0, keepdims=True)


def local(node_data, eroded, bucket_map, seg_point, seg_angle):
    owners = lax.axis_size(("chip", "core"))
    groups = lax.axis_size("bucket")
    faces = node_data.shape[1]
    blocks = faces // LANES
    uncovered = 6 * eroded.shape[0]
    vmem = pl.BlockSpec(memory_space=pltpu.VMEM)
    anywhere = pl.BlockSpec(memory_space=pl.ANY)

    node_tiles = node_data.reshape(3, 8, blocks, LANES).transpose(0, 2, 1, 3).reshape(24 * blocks, LANES)
    local_buckets, width = seg_point.shape[0], seg_point.shape[2]
    segs, node, row, bucket, hot, counts = pl.pallas_call(
        start_kernel,
        out_shape=(
            jax.ShapeDtypeStruct((2 * local_buckets, 6, width), F32),
            pltpu.VMEM((24 * blocks, LANES), F32),
            pltpu.VMEM((1, uncovered), jnp.int32),
            pltpu.VMEM((1, uncovered), F32),
            pltpu.VMEM((LANES, uncovered), BF16),
            pltpu.VMEM((uncovered // 8, LANES), F32),
        ),
        in_specs=[anywhere] * 5,
        out_specs=(anywhere, vmem, vmem, vmem, vmem, vmem),
        scratch_shapes=[
            pltpu.VMEM((3, local_buckets, width), F32),
            pltpu.VMEM(seg_angle.shape, F32),
            pltpu.VMEM((uncovered // 6 // LANES, LANES), jnp.int32),
            pltpu.VMEM((blocks, LANES), jnp.int32),
            pltpu.VMEM((2 * local_buckets, 6, width), F32),
            pltpu.SemaphoreType.DMA((8,)),
        ],
        name="start",
    )(seg_point.transpose(1, 0, 2), seg_angle, eroded.reshape(-1, LANES), bucket_map.reshape(blocks, LANES), node_tiles)
    segs = lax.all_to_all(segs, ("core", "bucket"), 0, 0, tiled=True)

    columns, code = pl.pallas_call(
        pack_kernel,
        out_shape=(pltpu.VMEM((LANES, owners), F32), pltpu.VMEM((2, uncovered), jnp.int32)),
        in_specs=[vmem] * 5,
        out_specs=(vmem, vmem),
        scratch_shapes=[
            pltpu.VMEM((uncovered, LANES), F32),
            pltpu.VMEM((1, uncovered), F32),
            pltpu.VMEM((9 * blocks, 2 * LANES), BF16),
        ],
        name="pack",
    )(near(row), near(bucket), near(hot), near(counts), near(node))

    packed = pl.pallas_call(
        send_kernel,
        out_shape=jax.ShapeDtypeStruct((owners, LANES), F32),
        in_specs=[vmem, vmem],
        out_specs=vmem,
        scratch_shapes=[pltpu.VMEM((LANES, owners), F32)],
        name="send",
    )(near(columns), near(segs))
    arrived = lax.all_to_all(packed.reshape(owners // 2, 2, LANES), "chip", 0, 0, tiled=True)

    with jax.named_scope("coefficients"):
        left, normal = pl.pallas_call(
            coefficient_kernel,
            out_shape=(
                pltpu.VMEM((2, 2 * groups, 256, 2 * LANES), BF16),
                pltpu.VMEM((4 * groups, 8, LANES), F32),
            ),
            in_specs=[vmem],
            out_specs=(vmem, vmem),
            scratch_shapes=[pltpu.VMEM((4 * groups, 4 * LANES, LANES), F32)],
            name="coefficients",
        )(near(segs))

    force = pl.pallas_call(
        force_kernel,
        out_shape=pltpu.VMEM((groups, 32, LANES), F32),
        in_specs=[vmem, vmem, vmem],
        out_specs=vmem,
        scratch_shapes=[
            pltpu.VMEM((LANES, LANES), F32),
            pltpu.VMEM((2, 2 * LANES, SLOTS * LANES), BF16),
            pltpu.VMEM((2, 3, groups * LANES, LANES), F32),
        ],
        name="force",
    )(near(arrived.reshape(owners, LANES)), near(left), near(normal))

    shared = lax.all_to_all(force, "bucket", 0, 0, tiled=True)
    outgoing = shared.reshape(groups * 32, 2, owners // 2).transpose(2, 1, 0)
    returned = lax.all_to_all(outgoing, "chip", 0, 0, tiled=True)

    return pl.pallas_call(
        pick_kernel,
        out_shape=jax.ShapeDtypeStruct((3, uncovered), F32),
        in_specs=[vmem, vmem],
        out_specs=vmem,
        scratch_shapes=[pltpu.VMEM((120, LANES), F32)],
        name="pick",
    )(near(returned.reshape(owners, LANES)), near(code))


def solution(mesh):
    split = Mesh(mesh.devices.reshape(-1, 2, mesh.shape["bucket"]), ("chip", "core", "bucket"))
    elem = ("chip", "core")
    in_specs = (P(None, elem), P(elem), P(elem), P(elem, None, "bucket"), P(elem, None, "bucket"))
    return jax.shard_map(local, mesh=split, in_specs=in_specs, out_specs=P(None, elem), check_vma=False)
```

```python
import functools

import jax
import jax.numpy as jnp
from jax import lax
from jax.experimental import pallas as pl
from jax.experimental.pallas import tpu as pltpu
from jax.sharding import Mesh, PartitionSpec as P

STIFFNESS = 20.0
DAMPING = 0.5
SLOTS = 5
LANES = 128
F32 = jnp.float32
BF16 = jnp.bfloat16
NT = (((1,), (1,)), ((), ()))


def near(value):
    return pltpu.with_memory_space_constraint(value, pltpu.VMEM)


def one_hot(row, size):
    numbers = lax.broadcasted_iota(jnp.int32, (size, row.shape[1]), 0)
    return jnp.where(numbers == row, 1.0, 0.0).astype(BF16)


def start_kernel(point_hbm, angle_hbm, eroded_hbm, map_hbm, node_hbm, out_hbm, node_ref, row_ref, bucket_ref, point_ref,
                 angle_ref, eroded_ref, map_ref, out_ref, sem):
    part = node_ref.shape[0] // 3
    pairs = [(eroded_hbm, eroded_ref), (map_hbm, map_ref), (point_hbm, point_ref), (angle_hbm, angle_ref)]
    for i in range(3):
        at = pl.ds(i * part, part)
        pairs.append((node_hbm.at[at, :], node_ref.at[at, :]))
    copies = [pltpu.make_async_copy(source, target, sem.at[i]) for i, (source, target) in enumerate(pairs)]
    for copy in copies:
        copy.start()

    copies[2].wait()
    copies[3].wait()
    for i in range(3):
        out_ref[:, i, :] = point_ref[i]
    for i in range(2):
        out_ref[:, 3 + i, :] = angle_ref[:, i, :]
    away = pltpu.make_async_copy(out_ref, out_hbm, sem.at[7])
    away.start()
    blocks = map_ref.shape[0]
    count = row_ref.shape[1]
    rows4 = eroded_ref.shape[0]
    span = count // rows4
    copies[0].wait()

    eroded = eroded_ref[...]
    lane = lax.broadcasted_iota(jnp.int32, (LANES, span), 1)
    six = 6 * lax.broadcasted_iota(jnp.int32, (LANES, span), 0)
    spread = jnp.where((lane >= six) & (lane < six + 6), 1.0, 0.0).astype(BF16)
    high = jnp.dot((eroded >> 3).astype(F32).astype(BF16), spread, preferred_element_type=F32)
    low = jnp.dot((eroded & 7).astype(F32).astype(BF16), spread, preferred_element_type=F32)
    number = lax.broadcasted_iota(jnp.int32, (rows4, span), 1)
    faces4 = 6 * (high * 8.0 + low).astype(jnp.int32) + number % 6
    for a in range(rows4):
        row_ref[0:1, a * span:(a + 1) * span] = faces4[a:a + 1, :]
    copies[1].wait()
    buckets = map_ref[...]
    digits = jnp.concatenate([(buckets & 1016).astype(F32), (buckets & 7).astype(F32)], axis=1).astype(BF16)
    step = 512
    for c in range(count // step):
        at = slice(c * step, (c + 1) * step)
        face = row_ref[0:1, at]
        hot = one_hot(face & (LANES - 1), LANES)
        value = jnp.dot(digits, jnp.concatenate([hot, hot], axis=0), preferred_element_type=F32)
        numbers = lax.broadcasted_iota(jnp.int32, (blocks, step), 0)
        bucket_ref[0:1, at] = jnp.sum(jnp.where(numbers == (face >> 7), value, 0.0), axis=0, keepdims=True)
    for copy in copies[4:]:
        copy.wait()
    away.wait()


def pieces(value):
    first = value.astype(BF16).astype(F32)
    rest = value - first
    second = rest.astype(BF16).astype(F32)
    return first, second, rest - second


def coefficient_kernel(seg_ref, left_ref, normal_ref, rows_ref):
    rows_ref[...] = jnp.zeros(rows_ref.shape, F32)
    log2e = 1.4426950408889634
    order = (0, 0, 0, 1, 1, 2)
    azimuth, polar = seg_ref[:, 3, :], seg_ref[:, 4, :]
    ring = jnp.sin(polar)
    normal = [jnp.cos(azimuth) * ring, jnp.sin(azimuth) * ring, jnp.cos(polar)]
    point = [seg_ref[:, i, :] for i in range(3)]
    along = point[0] * normal[0] + point[1] * normal[1] + point[2] * normal[2]
    square = point[0] * point[0] + point[1] * point[1] + point[2] * point[2]
    terms = (
        (0, [log2e * value for value in point]),
        (0, [-value for value in normal]),
        (6, [-DAMPING * value for value in normal]),
        (3, normal),
    )
    split = [(start, [pieces(value) for value in values]) for start, values in terms]
    constant = [pieces((-0.5 * log2e) * square), pieces(along)]
    for term in range(4):
        at = term * LANES
        start, values = split[term]
        for group, piece in enumerate(order):
            for i in range(3):
                rows_ref[:, at + group * 16 + start + i, :] = values[i][piece]
        if term < 2:
            for piece in range(3):
                rows_ref[:, at + 96 + 6 + piece, :] = constant[term][piece]
    for piece in range(3):
        rows_ref[:, 96 + piece, :] = jnp.full_like(ring, -1.0)
        rows_ref[:, 2 * LANES + 96 + 3 + piece, :] = jnp.full_like(ring, 1.0)
    for i in range(3):
        normal_ref[:, i, :] = normal[i]
    for i in range(3, 8):
        normal_ref[:, i, :] = jnp.zeros_like(ring)
    for g in range(seg_ref.shape[0]):
        for term in range(4):
            turned = rows_ref[g, term * LANES:(term + 1) * LANES, :].T.astype(BF16)
            for half in range(2):
                left_ref[g % 2, (g // 2) * 2 + half, term * 64:(term + 1) * 64, :] = turned[half * 64:(half + 1) * 64]


def pack_kernel(row_ref, bucket_ref, node_ref, out_ref, code_ref, col_ref, other_ref, rank_ref, owner_hot, geo_ref):
    group = lax.axis_index("bucket")
    count = row_ref.shape[1]
    tiles = count // LANES
    blocks = geo_ref.shape[0] // 9

    earlier = (lax.broadcasted_iota(jnp.int32, (LANES, LANES), 0)
               < lax.broadcasted_iota(jnp.int32, (LANES, LANES), 1))
    counts, picks = [], []
    for t in range(tiles):
        at = slice(t * LANES, (t + 1) * LANES)
        mine = bucket_ref[0:1, at]
        other = jnp.broadcast_to(mine, (LANES, LANES)).T
        other_ref[at, :] = other
        hit = jnp.where((other == mine) & earlier, 1.0, 0.0)
        rank_ref[0:1, at] = jnp.sum(hit, axis=0, keepdims=True)
        bucket = mine.astype(jnp.int32)
        hot = one_hot(bucket >> 3, LANES)
        owner_hot[:, at] = hot
        picks.append(lax.broadcasted_iota(jnp.int32, (16, LANES), 0) == (bucket & 7))
        inner = jnp.where(picks[t], 1.0, 0.0).astype(BF16)
        counts.append(lax.dot_general(inner, hot, NT, preferred_element_type=F32))
    before = jnp.zeros((16, LANES), F32)
    for t in range(tiles):
        at = slice(t * LANES, (t + 1) * LANES)
        if t:
            before = before + counts[t - 1]
            seen = jnp.dot(before.astype(BF16), owner_hot[:, at], preferred_element_type=F32)
            rank_ref[0:1, at] += jnp.sum(jnp.where(picks[t], seen, 0.0), axis=0, keepdims=True)

    bucket = bucket_ref[0:1, :].astype(jnp.int32)
    rank = rank_ref[0:1, :].astype(jnp.int32)
    owner = bucket >> 3
    inner = bucket & 7
    code_ref[0:1, :] = (owner & (LANES - 2)) + (inner & 1)
    code_ref[1:2, :] = ((owner & 1) * 4 + (inner >> 1)) * SLOTS + rank
    lane = lax.broadcasted_iota(jnp.int32, (1, LANES), 1)
    wanted = [(lane * 8 + group * 2 + par).astype(F32) for par in range(2)]
    pair = 2 * LANES
    sources = []
    numbers = lax.broadcasted_iota(jnp.int32, (16, pair), 0)
    for c in range(count // pair):
        at = slice(c * pair, (c + 1) * pair)
        face = row_ref[0:1, at]
        parts = jnp.where(numbers < 8, (face >> 7) + 1, face & (LANES - 1))
        left = jnp.where((numbers & 7) == rank[:, at], parts, 0).astype(F32).astype(BF16)
        other = other_ref[at, :]
        right = jnp.concatenate([jnp.where(other == want, 1.0, 0.0).astype(BF16) for want in wanted], axis=1)
        sources.append(jnp.dot(left, right, preferred_element_type=F32))
    source = functools.reduce(jnp.add, sources)

    for g in range(blocks // 16):
        row = [node_ref[pl.ds((r // 8) * blocks * 8 + r % 8 + g * 128, 16, stride=8), :] for r in range(24)]
        corner = [row[3 * m:3 * m + 3] for m in range(4)]
        motion = [row[12 + 3 * m:15 + 3 * m] for m in range(4)]
        centroid = [0.25 * (corner[0][i] + corner[1][i] + corner[2][i] + corner[3][i]) for i in range(3)]
        one = [corner[2][i] - corner[0][i] for i in range(3)]
        two = [corner[3][i] - corner[1][i] for i in range(3)]
        area = [
            0.5 * (one[1] * two[2] - one[2] * two[1]),
            0.5 * (one[2] * two[0] - one[0] * two[2]),
            0.5 * (one[0] * two[1] - one[1] * two[0]),
        ]
        velocity = [0.25 * (motion[0][i] + motion[1][i] + motion[2][i] + motion[3][i]) for i in range(3)]
        for q, value in enumerate(centroid + area + velocity):
            at = slice(q * blocks + g * 16, q * blocks + g * 16 + 16)
            first = value.astype(BF16)
            geo_ref[at, :LANES] = first
            geo_ref[at, LANES:] = (value - first.astype(F32)).astype(BF16)

    col_ref[...] = jnp.zeros(col_ref.shape, F32)
    filled = jnp.zeros((1, 256), F32)
    for k in range(SLOTS):
        high = source[k:k + 1, :].astype(jnp.int32) - 1
        low = source[8 + k:9 + k, :].astype(jnp.int32)
        filled = filled + jnp.where(high >= 0, 1.0, 0.0)
        hot = one_hot(low, LANES)
        hot = jnp.concatenate([hot, hot], axis=0)
        numbers = lax.broadcasted_iota(jnp.int32, (8, 256), 0)
        for start, end in ((0, 5), (5, 9)):
            found = jnp.dot(geo_ref[start * blocks:end * blocks, :], hot, preferred_element_type=F32)
            values = [jnp.zeros((8, 256), F32)] * (end - start)
            for h in range(0, blocks, 8):
                mine = numbers == high - h
                for i in range(end - start):
                    values[i] = jnp.where(mine, found[i * blocks + h:i * blocks + h + 8], values[i])
            for i in range(end - start):
                value = jnp.sum(values[i], axis=0, keepdims=True)
                for par in range(2):
                    row = par * 64 + k * 12 + start + i
                    col_ref[row:row + 1, :] = value[:, par * LANES:(par + 1) * LANES]
    for par in range(2):
        col_ref[par * 64 + 60:par * 64 + 61, :] = filled[:, par * LANES:(par + 1) * LANES]
    out_ref[...] = col_ref[...].T


def force_kernel(face_ref, left_ref, seg_ref, out_ref, row_ref, right_ref, wide_ref):
    half = LANES // 2
    row_ref[...] = jnp.concatenate([face_ref[pl.ds(core, half, stride=2), :] for core in range(2)], axis=0).T
    groups = seg_ref.shape[0] // 2
    for g in range(2 * groups):
        columns = seg_ref[g].T
        for i in range(3):
            wide_ref[g % 2, i, (g // 2) * LANES:(g // 2 + 1) * LANES, :] = jnp.broadcast_to(
                columns[:, i:i + 1], (LANES, LANES))
    half_log2e = 0.5 * 1.4426950408889634
    number = lax.broadcasted_iota(jnp.int32, (16, LANES), 0)
    for par in range(2):
        count = jnp.sum(row_ref[par * 64 + 60:par * 64 + 61, :], axis=1, keepdims=True)
        stiff = pieces(jnp.broadcast_to(STIFFNESS * lax.rsqrt(jnp.maximum(count, 1.0)), (1, LANES)))
        for k in range(SLOTS):
            start = par * 64 + k * 12
            face = row_ref[start:start + 16, :]
            center = [row_ref[start + i:start + i + 1, :] for i in range(3)]
            square = pieces(half_log2e * (
                center[0] * center[0] + center[1] * center[1] + center[2] * center[2]))
            extra = jnp.where((number >= 6) & (number < 9), 1.0, 0.0)
            for piece in range(3):
                extra = jnp.where(number == piece, square[piece], extra)
                extra = jnp.where(number == 3 + piece, stiff[piece], extra)
            first, second, third = pieces(face)
            blocks = (first, second, third, first, second, first, extra, jnp.zeros_like(extra))
            for group, block in enumerate(blocks):
                right_ref[par, group * 16:(group + 1) * 16, k * LANES:(k + 1) * LANES] = block.astype(BF16)
    chunks = left_ref.shape[1]
    for par in range(2):
        for first in range(0, SLOTS, 2):
            width = min(2, SLOTS - first)
            right = right_ref[par, :, first * LANES:(first + width) * LANES]
            total = [[jnp.zeros((8, LANES), F32) for i in range(3)] for k in range(width)]
            for chunk in range(chunks):
                found = jnp.dot(left_ref[par, chunk], right, preferred_element_type=F32)
                normal = [wide_ref[par, i, chunk * 64:(chunk + 1) * 64, :] for i in range(3)]
                for k in range(width):
                    at = slice(k * LANES, (k + 1) * LANES)
                    weight = jnp.exp2(found[0:64, at])
                    traction = (weight * jnp.maximum(found[64:128, at], 0.0) * found[128:192, at]
                                * jnp.abs(found[192:256, at]))
                    for i in range(3):
                        total[k][i] = total[k][i] + jnp.sum(
                            (traction * normal[i]).reshape(8, 8, LANES), axis=0)
            for k in range(width):
                for i in range(3):
                    row = par * 16 + i * SLOTS + first + k
                    row_ref[row:row + 1, :] = jnp.sum(total[k][i], axis=0, keepdims=True)
        row_ref[par * 16 + 15:par * 16 + 16, :] = jnp.zeros((1, LANES), F32)
    for core in range(2):
        at = slice(core * half, (core + 1) * half)
        both = jnp.concatenate([row_ref[0:16, at], row_ref[16:32, at]], axis=1)
        for x in range(4):
            out_ref[core * 4 + x] = both


def pick_kernel(force_ref, code_ref, out_ref, row_ref):
    turned = force_ref[...].T
    for g in range(8):
        for i in range(3):
            to, start = i * 40 + g * SLOTS, g * 16 + i * SLOTS
            row_ref[to:to + SLOTS, :] = turned[start:start + SLOTS, :]
    value = row_ref[...]
    first = value.astype(BF16)
    left = jnp.concatenate([first, (value - first.astype(F32)).astype(BF16)], axis=1)
    step = 512
    for c in range(out_ref.shape[1] // step):
        at = slice(c * step, (c + 1) * step)
        hot = one_hot(code_ref[0:1, at], LANES)
        found = jnp.dot(left, jnp.concatenate([hot, hot], axis=0), preferred_element_type=F32)
        mine = lax.broadcasted_iota(jnp.int32, (40, step), 0) == code_ref[1:2, at]
        for i in range(3):
            out_ref[i:i + 1, at] = jnp.sum(
                jnp.where(mine, found[i * 40:(i + 1) * 40], 0.0), axis=0, keepdims=True)


def local(node_data, eroded, bucket_map, seg_point, seg_angle):
    owners = lax.axis_size(("chip", "core"))
    groups = lax.axis_size("bucket")
    faces = node_data.shape[1]
    blocks = faces // LANES
    uncovered = 6 * eroded.shape[0]
    vmem = pl.BlockSpec(memory_space=pltpu.VMEM)
    anywhere = pl.BlockSpec(memory_space=pl.ANY)

    node_tiles = node_data.reshape(3, 8, blocks, LANES).transpose(0, 2, 1, 3).reshape(24 * blocks, LANES)
    buckets, width = seg_point.shape[0], seg_point.shape[2]
    segs, node, row, bucket = pl.pallas_call(
        start_kernel,
        out_shape=(
            jax.ShapeDtypeStruct((buckets, 5, width), F32),
            pltpu.VMEM((24 * blocks, LANES), F32),
            pltpu.VMEM((1, uncovered), jnp.int32),
            pltpu.VMEM((1, uncovered), F32),
        ),
        in_specs=[anywhere] * 5,
        out_specs=(anywhere, vmem, vmem, vmem),
        scratch_shapes=[
            pltpu.VMEM((3, buckets, width), F32),
            pltpu.VMEM(seg_angle.shape, F32),
            pltpu.VMEM((uncovered // 6 // LANES, LANES), jnp.int32),
            pltpu.VMEM((blocks, LANES), jnp.int32),
            pltpu.VMEM((buckets, 5, width), F32),
            pltpu.SemaphoreType.DMA((8,)),
        ],
        name="start",
    )(seg_point.transpose(1, 0, 2), seg_angle, eroded.reshape(-1, LANES), bucket_map.reshape(blocks, LANES), node_tiles)
    segs = lax.all_to_all(segs, "bucket", 0, 0, tiled=True)

    packed, code = pl.pallas_call(
        pack_kernel,
        out_shape=(jax.ShapeDtypeStruct((owners, LANES), F32), pltpu.VMEM((2, uncovered), jnp.int32)),
        in_specs=[vmem] * 3,
        out_specs=(vmem, vmem),
        scratch_shapes=[
            pltpu.VMEM((LANES, owners), F32),
            pltpu.VMEM((uncovered, LANES), F32),
            pltpu.VMEM((1, uncovered), F32),
            pltpu.VMEM((LANES, uncovered), BF16),
            pltpu.VMEM((9 * blocks, 2 * LANES), BF16),
        ],
        name="pack",
    )(near(row), near(bucket), near(node))

    with jax.named_scope("dispatch"):
        arrived = lax.all_to_all(packed.reshape(owners, 1, LANES), ("chip", "core"), 0, 0, tiled=True)

    with jax.named_scope("coefficients"):
        left, normal = pl.pallas_call(
            coefficient_kernel,
            out_shape=(
                pltpu.VMEM((2, 2 * groups, 256, LANES), BF16),
                pltpu.VMEM((2 * groups, 8, LANES), F32),
            ),
            in_specs=[vmem],
            out_specs=(vmem, vmem),
            scratch_shapes=[pltpu.VMEM((2 * groups, 4 * LANES, LANES), F32)],
            name="coefficients",
        )(near(segs))

    force = pl.pallas_call(
        force_kernel,
        out_shape=pltpu.VMEM((2 * groups, 16, LANES), F32),
        in_specs=[vmem, vmem, vmem],
        out_specs=vmem,
        scratch_shapes=[
            pltpu.VMEM((LANES, LANES), F32),
            pltpu.VMEM((2, LANES, SLOTS * LANES), BF16),
            pltpu.VMEM((2, 3, groups * LANES, LANES), F32),
        ],
        name="force",
    )(near(arrived.reshape(owners, LANES)), near(left), near(normal))

    shared = lax.all_to_all(force, ("core", "bucket"), 0, 0, tiled=True)
    outgoing = shared.reshape(groups * 32, 2, owners // 2).transpose(2, 1, 0)
    returned = lax.all_to_all(outgoing, "chip", 0, 0, tiled=True)

    return pl.pallas_call(
        pick_kernel,
        out_shape=jax.ShapeDtypeStruct((3, uncovered), F32),
        in_specs=[vmem, vmem],
        out_specs=vmem,
        scratch_shapes=[pltpu.VMEM((120, LANES), F32)],
        name="pick",
    )(near(returned.reshape(owners, LANES)), near(code))


def solution(mesh):
    split = Mesh(mesh.devices.reshape(-1, 2, mesh.shape["bucket"]), ("chip", "core", "bucket"))
    elem = ("chip", "core")
    in_specs = (P(None, elem), P(elem), P(elem), P(elem, None, "bucket"), P(elem, None, "bucket"))
    return jax.shard_map(local, mesh=split, in_specs=in_specs, out_specs=P(None, elem), check_vma=False)
```

```python
import functools

import jax
import jax.numpy as jnp
from jax import lax
from jax.experimental import pallas as pl
from jax.experimental.pallas import tpu as pltpu
from jax.sharding import Mesh, PartitionSpec as P

STIFFNESS = 20.0
DAMPING = 0.5
SLOTS = 5
LANES = 128
F32 = jnp.float32
BF16 = jnp.bfloat16
NT = (((1,), (1,)), ((), ()))


def near(value):
    return pltpu.with_memory_space_constraint(value, pltpu.VMEM)


def one_hot(row, size):
    numbers = lax.broadcasted_iota(jnp.int32, (size, row.shape[1]), 0)
    return jnp.where(numbers == row, 1.0, 0.0).astype(BF16)


def start_kernel(point_hbm, angle_hbm, eroded_hbm, map_hbm, node_hbm, out_hbm, node_ref, row_ref, bucket_ref, point_ref,
                 angle_ref, eroded_ref, map_ref, out_ref, sem):
    part = node_ref.shape[0] // 3
    pairs = [(eroded_hbm, eroded_ref), (map_hbm, map_ref), (point_hbm, point_ref), (angle_hbm, angle_ref)]
    for i in range(3):
        at = pl.ds(i * part, part)
        pairs.append((node_hbm.at[at, :], node_ref.at[at, :]))
    copies = [pltpu.make_async_copy(source, target, sem.at[i]) for i, (source, target) in enumerate(pairs)]
    for copy in copies:
        copy.start()

    copies[2].wait()
    copies[3].wait()
    for i in range(3):
        out_ref[:, i, :] = point_ref[i]
    for i in range(2):
        out_ref[:, 3 + i, :] = angle_ref[:, i, :]
    away = pltpu.make_async_copy(out_ref, out_hbm, sem.at[7])
    away.start()
    blocks = map_ref.shape[0]
    count = row_ref.shape[1]
    rows4 = eroded_ref.shape[0]
    span = count // rows4
    copies[0].wait()

    eroded = eroded_ref[...]
    lane = lax.broadcasted_iota(jnp.int32, (LANES, span), 1)
    six = 6 * lax.broadcasted_iota(jnp.int32, (LANES, span), 0)
    spread = jnp.where((lane >= six) & (lane < six + 6), 1.0, 0.0).astype(BF16)
    high = jnp.dot((eroded >> 3).astype(F32).astype(BF16), spread, preferred_element_type=F32)
    low = jnp.dot((eroded & 7).astype(F32).astype(BF16), spread, preferred_element_type=F32)
    number = lax.broadcasted_iota(jnp.int32, (rows4, span), 1)
    faces4 = 6 * (high * 8.0 + low).astype(jnp.int32) + number % 6
    for a in range(rows4):
        row_ref[0:1, a * span:(a + 1) * span] = faces4[a:a + 1, :]
    copies[1].wait()
    buckets = map_ref[...]
    digits = jnp.concatenate([(buckets & 1016).astype(F32), (buckets & 7).astype(F32)], axis=1).astype(BF16)
    step = 512
    for c in range(count // step):
        at = slice(c * step, (c + 1) * step)
        face = row_ref[0:1, at]
        hot = one_hot(face & (LANES - 1), LANES)
        value = jnp.dot(digits, jnp.concatenate([hot, hot], axis=0), preferred_element_type=F32)
        numbers = lax.broadcasted_iota(jnp.int32, (blocks, step), 0)
        bucket_ref[0:1, at] = jnp.sum(jnp.where(numbers == (face >> 7), value, 0.0), axis=0, keepdims=True)
    for copy in copies[4:]:
        copy.wait()
    away.wait()


def pieces(value):
    first = value.astype(BF16).astype(F32)
    rest = value - first
    second = rest.astype(BF16).astype(F32)
    return first, second, rest - second


def coefficient_kernel(seg_ref, left_ref, normal_ref, rows_ref):
    rows_ref[...] = jnp.zeros(rows_ref.shape, F32)
    log2e = 1.4426950408889634
    order = (0, 0, 0, 1, 1, 2)
    azimuth, polar = seg_ref[:, 3, :], seg_ref[:, 4, :]
    ring = jnp.sin(polar)
    normal = [jnp.cos(azimuth) * ring, jnp.sin(azimuth) * ring, jnp.cos(polar)]
    point = [seg_ref[:, i, :] for i in range(3)]
    along = point[0] * normal[0] + point[1] * normal[1] + point[2] * normal[2]
    square = point[0] * point[0] + point[1] * point[1] + point[2] * point[2]
    terms = (
        (0, [log2e * value for value in point]),
        (0, [-value for value in normal]),
        (6, [-DAMPING * value for value in normal]),
        (3, normal),
    )
    split = [(start, [pieces(value) for value in values]) for start, values in terms]
    constant = [pieces((-0.5 * log2e) * square), pieces(along)]
    for term in range(4):
        at = term * LANES
        start, values = split[term]
        for group, piece in enumerate(order):
            for i in range(3):
                rows_ref[:, at + group * 16 + start + i, :] = values[i][piece]
        if term < 2:
            for piece in range(3):
                rows_ref[:, at + 96 + 6 + piece, :] = constant[term][piece]
    for piece in range(3):
        rows_ref[:, 96 + piece, :] = jnp.full_like(ring, -1.0)
        rows_ref[:, 2 * LANES + 96 + 3 + piece, :] = jnp.full_like(ring, 1.0)
    for i in range(3):
        normal_ref[:, i, :] = normal[i]
    for i in range(3, 8):
        normal_ref[:, i, :] = jnp.zeros_like(ring)
    for g in range(seg_ref.shape[0]):
        for term in range(4):
            turned = rows_ref[g, term * LANES:(term + 1) * LANES, :].T.astype(BF16)
            for half in range(2):
                left_ref[g % 2, (g // 2) * 2 + half, term * 64:(term + 1) * 64, :] = turned[half * 64:(half + 1) * 64]


def pack_kernel(row_ref, bucket_ref, node_ref, out_ref, code_ref, col_ref, other_ref, rank_ref, owner_hot, geo_ref):
    group = lax.axis_index("bucket")
    count = row_ref.shape[1]
    tiles = count // LANES
    blocks = geo_ref.shape[0] // 9

    earlier = (lax.broadcasted_iota(jnp.int32, (LANES, LANES), 0)
               < lax.broadcasted_iota(jnp.int32, (LANES, LANES), 1))
    counts, picks = [], []
    for t in range(tiles):
        at = slice(t * LANES, (t + 1) * LANES)
        mine = bucket_ref[0:1, at]
        other = jnp.broadcast_to(mine, (LANES, LANES)).T
        other_ref[at, :] = other
        hit = jnp.where((other == mine) & earlier, 1.0, 0.0)
        rank_ref[0:1, at] = jnp.sum(hit, axis=0, keepdims=True)
        bucket = mine.astype(jnp.int32)
        hot = one_hot(bucket >> 3, LANES)
        owner_hot[:, at] = hot
        picks.append(lax.broadcasted_iota(jnp.int32, (16, LANES), 0) == (bucket & 7))
        inner = jnp.where(picks[t], 1.0, 0.0).astype(BF16)
        counts.append(lax.dot_general(inner, hot, NT, preferred_element_type=F32))
    before = jnp.zeros((16, LANES), F32)
    for t in range(tiles):
        at = slice(t * LANES, (t + 1) * LANES)
        if t:
            before = before + counts[t - 1]
            seen = jnp.dot(before.astype(BF16), owner_hot[:, at], preferred_element_type=F32)
            rank_ref[0:1, at] += jnp.sum(jnp.where(picks[t], seen, 0.0), axis=0, keepdims=True)

    bucket = bucket_ref[0:1, :].astype(jnp.int32)
    rank = rank_ref[0:1, :].astype(jnp.int32)
    owner = bucket >> 3
    inner = bucket & 7
    code_ref[0:1, :] = (owner & (LANES - 2)) + (inner & 1)
    code_ref[1:2, :] = ((owner & 1) * 4 + (inner >> 1)) * SLOTS + rank
    lane = lax.broadcasted_iota(jnp.int32, (1, LANES), 1)
    wanted = [(lane * 8 + group * 2 + par).astype(F32) for par in range(2)]
    pair = 2 * LANES
    sources = []
    numbers = lax.broadcasted_iota(jnp.int32, (16, pair), 0)
    for c in range(count // pair):
        at = slice(c * pair, (c + 1) * pair)
        face = row_ref[0:1, at]
        parts = jnp.where(numbers < 8, (face >> 7) + 1, face & (LANES - 1))
        left = jnp.where((numbers & 7) == rank[:, at], parts, 0).astype(F32).astype(BF16)
        other = other_ref[at, :]
        right = jnp.concatenate([jnp.where(other == want, 1.0, 0.0).astype(BF16) for want in wanted], axis=1)
        sources.append(jnp.dot(left, right, preferred_element_type=F32))
    source = functools.reduce(jnp.add, sources)

    for g in range(blocks // 16):
        row = [node_ref[pl.ds((r // 8) * blocks * 8 + r % 8 + g * 128, 16, stride=8), :] for r in range(24)]
        corner = [row[3 * m:3 * m + 3] for m in range(4)]
        motion = [row[12 + 3 * m:15 + 3 * m] for m in range(4)]
        centroid = [0.25 * (corner[0][i] + corner[1][i] + corner[2][i] + corner[3][i]) for i in range(3)]
        one = [corner[2][i] - corner[0][i] for i in range(3)]
        two = [corner[3][i] - corner[1][i] for i in range(3)]
        area = [
            0.5 * (one[1] * two[2] - one[2] * two[1]),
            0.5 * (one[2] * two[0] - one[0] * two[2]),
            0.5 * (one[0] * two[1] - one[1] * two[0]),
        ]
        velocity = [0.25 * (motion[0][i] + motion[1][i] + motion[2][i] + motion[3][i]) for i in range(3)]
        for q, value in enumerate(centroid + area + velocity):
            at = slice(q * blocks + g * 16, q * blocks + g * 16 + 16)
            first = value.astype(BF16)
            geo_ref[at, :LANES] = first
            geo_ref[at, LANES:] = (value - first.astype(F32)).astype(BF16)

    col_ref[...] = jnp.zeros(col_ref.shape, F32)
    filled = jnp.zeros((1, 256), F32)
    for k in range(SLOTS):
        high = source[k:k + 1, :].astype(jnp.int32) - 1
        low = source[8 + k:9 + k, :].astype(jnp.int32)
        filled = filled + jnp.where(high >= 0, 1.0, 0.0)
        hot = one_hot(low, LANES)
        hot = jnp.concatenate([hot, hot], axis=0)
        numbers = lax.broadcasted_iota(jnp.int32, (8, 256), 0)
        for start, end in ((0, 5), (5, 9)):
            found = jnp.dot(geo_ref[start * blocks:end * blocks, :], hot, preferred_element_type=F32)
            values = [jnp.zeros((8, 256), F32)] * (end - start)
            for h in range(0, blocks, 8):
                mine = numbers == high - h
                for i in range(end - start):
                    values[i] = jnp.where(mine, found[i * blocks + h:i * blocks + h + 8], values[i])
            for i in range(end - start):
                value = jnp.sum(values[i], axis=0, keepdims=True)
                for par in range(2):
                    row = par * 64 + k * 12 + start + i
                    col_ref[row:row + 1, :] = value[:, par * LANES:(par + 1) * LANES]
    for par in range(2):
        col_ref[par * 64 + 60:par * 64 + 61, :] = filled[:, par * LANES:(par + 1) * LANES]
    out_ref[...] = col_ref[...].T


def force_kernel(face_ref, left_ref, seg_ref, out_ref, row_ref, right_ref, wide_ref):
    half = LANES // 2
    row_ref[...] = jnp.concatenate([face_ref[pl.ds(core, half, stride=2), :] for core in range(2)], axis=0).T
    half_log2e = 0.5 * 1.4426950408889634
    number = lax.broadcasted_iota(jnp.int32, (16, LANES), 0)
    for par in range(2):
        count = jnp.sum(row_ref[par * 64 + 60:par * 64 + 61, :], axis=1, keepdims=True)
        stiff = pieces(jnp.broadcast_to(STIFFNESS * lax.rsqrt(jnp.maximum(count, 1.0)), (1, LANES)))
        for k in range(SLOTS):
            start = par * 64 + k * 12
            face = row_ref[start:start + 16, :]
            center = [row_ref[start + i:start + i + 1, :] for i in range(3)]
            square = pieces(half_log2e * (
                center[0] * center[0] + center[1] * center[1] + center[2] * center[2]))
            extra = jnp.where((number >= 6) & (number < 9), 1.0, 0.0)
            for piece in range(3):
                extra = jnp.where(number == piece, square[piece], extra)
                extra = jnp.where(number == 3 + piece, stiff[piece], extra)
            first, second, third = pieces(face)
            blocks = (first, second, third, first, second, first, extra, jnp.zeros_like(extra))
            for group, block in enumerate(blocks):
                right_ref[par, group * 16:(group + 1) * 16, k * LANES:(k + 1) * LANES] = block.astype(BF16)
    chunks = left_ref.shape[1]
    for par in range(2):
        for first in range(0, SLOTS, 2):
            width = min(2, SLOTS - first)
            right = right_ref[par, :, first * LANES:(first + width) * LANES]
            total = [[jnp.zeros((8, LANES), F32) for i in range(3)] for k in range(width)]
            for chunk in range(chunks):
                if first == 0 and chunk % 2 == 0:
                    columns = seg_ref[chunk + par].T
                    for i in range(3):
                        wide_ref[par, i, chunk * 64:chunk * 64 + LANES, :] = jnp.broadcast_to(
                            columns[:, i:i + 1], (LANES, LANES))
                found = jnp.dot(left_ref[par, chunk], right, preferred_element_type=F32)
                normal = [wide_ref[par, i, chunk * 64:(chunk + 1) * 64, :] for i in range(3)]
                for k in range(width):
                    at = slice(k * LANES, (k + 1) * LANES)
                    weight = jnp.exp2(found[0:64, at])
                    traction = (weight * jnp.maximum(found[64:128, at], 0.0) * found[128:192, at]
                                * jnp.abs(found[192:256, at]))
                    for i in range(3):
                        total[k][i] = total[k][i] + jnp.sum(
                            (traction * normal[i]).reshape(8, 8, LANES), axis=0)
            for k in range(width):
                for i in range(3):
                    row = par * 16 + i * SLOTS + first + k
                    row_ref[row:row + 1, :] = jnp.sum(total[k][i], axis=0, keepdims=True)
        row_ref[par * 16 + 15:par * 16 + 16, :] = jnp.zeros((1, LANES), F32)
    for core in range(2):
        at = slice(core * half, (core + 1) * half)
        both = jnp.concatenate([row_ref[0:16, at], row_ref[16:32, at]], axis=1)
        for x in range(4):
            out_ref[core * 4 + x] = both


def pick_kernel(force_ref, code_ref, out_ref, row_ref):
    turned = force_ref[...].T
    for g in range(8):
        for i in range(3):
            to, start = i * 40 + g * SLOTS, g * 16 + i * SLOTS
            row_ref[to:to + SLOTS, :] = turned[start:start + SLOTS, :]
    value = row_ref[...]
    first = value.astype(BF16)
    left = jnp.concatenate([first, (value - first.astype(F32)).astype(BF16)], axis=1)
    step = 512
    for c in range(out_ref.shape[1] // step):
        at = slice(c * step, (c + 1) * step)
        hot = one_hot(code_ref[0:1, at], LANES)
        found = jnp.dot(left, jnp.concatenate([hot, hot], axis=0), preferred_element_type=F32)
        mine = lax.broadcasted_iota(jnp.int32, (40, step), 0) == code_ref[1:2, at]
        for i in range(3):
            out_ref[i:i + 1, at] = jnp.sum(
                jnp.where(mine, found[i * 40:(i + 1) * 40], 0.0), axis=0, keepdims=True)


def local(node_data, eroded, bucket_map, seg_point, seg_angle):
    owners = lax.axis_size(("chip", "core"))
    groups = lax.axis_size("bucket")
    faces = node_data.shape[1]
    blocks = faces // LANES
    uncovered = 6 * eroded.shape[0]
    vmem = pl.BlockSpec(memory_space=pltpu.VMEM)
    anywhere = pl.BlockSpec(memory_space=pl.ANY)

    node_tiles = node_data.reshape(3, 8, blocks, LANES).transpose(0, 2, 1, 3).reshape(24 * blocks, LANES)
    buckets, width = seg_point.shape[0], seg_point.shape[2]
    segs, node, row, bucket = pl.pallas_call(
        start_kernel,
        out_shape=(
            jax.ShapeDtypeStruct((buckets, 5, width), F32),
            pltpu.VMEM((24 * blocks, LANES), F32),
            pltpu.VMEM((1, uncovered), jnp.int32),
            pltpu.VMEM((1, uncovered), F32),
        ),
        in_specs=[anywhere] * 5,
        out_specs=(anywhere, vmem, vmem, vmem),
        scratch_shapes=[
            pltpu.VMEM((3, buckets, width), F32),
            pltpu.VMEM(seg_angle.shape, F32),
            pltpu.VMEM((uncovered // 6 // LANES, LANES), jnp.int32),
            pltpu.VMEM((blocks, LANES), jnp.int32),
            pltpu.VMEM((buckets, 5, width), F32),
            pltpu.SemaphoreType.DMA((8,)),
        ],
        name="start",
    )(seg_point.transpose(1, 0, 2), seg_angle, eroded.reshape(-1, LANES), bucket_map.reshape(blocks, LANES), node_tiles)
    segs = lax.all_to_all(segs, "bucket", 0, 0, tiled=True)

    packed, code = pl.pallas_call(
        pack_kernel,
        out_shape=(jax.ShapeDtypeStruct((owners, LANES), F32), pltpu.VMEM((2, uncovered), jnp.int32)),
        in_specs=[vmem] * 3,
        out_specs=(vmem, vmem),
        scratch_shapes=[
            pltpu.VMEM((LANES, owners), F32),
            pltpu.VMEM((uncovered, LANES), F32),
            pltpu.VMEM((1, uncovered), F32),
            pltpu.VMEM((LANES, uncovered), BF16),
            pltpu.VMEM((9 * blocks, 2 * LANES), BF16),
        ],
        name="pack",
    )(near(row), near(bucket), near(node))

    with jax.named_scope("dispatch"):
        arrived = lax.all_to_all(packed.reshape(owners, 1, LANES), ("chip", "core"), 0, 0, tiled=True)

    with jax.named_scope("coefficients"):
        left, normal = pl.pallas_call(
            coefficient_kernel,
            out_shape=(
                pltpu.VMEM((2, 2 * groups, 256, LANES), BF16),
                pltpu.VMEM((2 * groups, 8, LANES), F32),
            ),
            in_specs=[vmem],
            out_specs=(vmem, vmem),
            scratch_shapes=[pltpu.VMEM((2 * groups, 4 * LANES, LANES), F32)],
            name="coefficients",
        )(near(segs))

    force = pl.pallas_call(
        force_kernel,
        out_shape=pltpu.VMEM((2 * groups, 16, LANES), F32),
        in_specs=[vmem, vmem, vmem],
        out_specs=vmem,
        scratch_shapes=[
            pltpu.VMEM((LANES, LANES), F32),
            pltpu.VMEM((2, LANES, SLOTS * LANES), BF16),
            pltpu.VMEM((2, 3, groups * LANES, LANES), F32),
        ],
        name="force",
    )(near(arrived.reshape(owners, LANES)), near(left), near(normal))

    shared = lax.all_to_all(force, ("core", "bucket"), 0, 0, tiled=True)
    outgoing = shared.reshape(groups * 32, 2, owners // 2).transpose(2, 1, 0)
    returned = lax.all_to_all(outgoing, "chip", 0, 0, tiled=True)

    return pl.pallas_call(
        pick_kernel,
        out_shape=jax.ShapeDtypeStruct((3, uncovered), F32),
        in_specs=[vmem, vmem],
        out_specs=vmem,
        scratch_shapes=[pltpu.VMEM((120, LANES), F32)],
        name="pick",
    )(near(returned.reshape(owners, LANES)), near(code))


def solution(mesh):
    split = Mesh(mesh.devices.reshape(-1, 2, mesh.shape["bucket"]), ("chip", "core", "bucket"))
    elem = ("chip", "core")
    in_specs = (P(None, elem), P(elem), P(elem), P(elem, None, "bucket"), P(elem, None, "bucket"))
    return jax.shard_map(local, mesh=split, in_specs=in_specs, out_specs=P(None, elem), check_vma=False)
```

```python
import functools

import jax
import jax.numpy as jnp
from jax import lax
from jax.experimental import pallas as pl
from jax.experimental.pallas import tpu as pltpu
from jax.sharding import Mesh, PartitionSpec as P

STIFFNESS = 20.0
DAMPING = 0.5
SLOTS = 5
LANES = 128
F32 = jnp.float32
BF16 = jnp.bfloat16
NT = (((1,), (1,)), ((), ()))


def near(value):
    return pltpu.with_memory_space_constraint(value, pltpu.VMEM)


def one_hot(row, size):
    numbers = lax.broadcasted_iota(jnp.int32, (size, row.shape[1]), 0)
    return jnp.where(numbers == row, 1.0, 0.0).astype(BF16)


def start_kernel(point_hbm, angle_hbm, eroded_hbm, map_hbm, node_hbm, out_hbm, node_ref, row_ref, bucket_ref, point_ref,
                 angle_ref, eroded_ref, map_ref, out_ref, sem):
    part = node_ref.shape[0] // 3
    pairs = [(eroded_hbm, eroded_ref), (map_hbm, map_ref), (point_hbm, point_ref), (angle_hbm, angle_ref)]
    for i in range(3):
        at = pl.ds(i * part, part)
        pairs.append((node_hbm.at[at, :], node_ref.at[at, :]))
    copies = [pltpu.make_async_copy(source, target, sem.at[i]) for i, (source, target) in enumerate(pairs)]
    for copy in copies:
        copy.start()

    copies[2].wait()
    copies[3].wait()
    for i in range(3):
        out_ref[:, i, :] = point_ref[i]
    for i in range(2):
        out_ref[:, 3 + i, :] = angle_ref[:, i, :]
    away = pltpu.make_async_copy(out_ref, out_hbm, sem.at[7])
    away.start()
    blocks = map_ref.shape[0]
    count = row_ref.shape[1]
    rows4 = eroded_ref.shape[0]
    span = count // rows4
    copies[0].wait()

    eroded = eroded_ref[...]
    lane = lax.broadcasted_iota(jnp.int32, (LANES, span), 1)
    six = 6 * lax.broadcasted_iota(jnp.int32, (LANES, span), 0)
    spread = jnp.where((lane >= six) & (lane < six + 6), 1.0, 0.0).astype(BF16)
    high = jnp.dot((eroded >> 3).astype(F32).astype(BF16), spread, preferred_element_type=F32)
    low = jnp.dot((eroded & 7).astype(F32).astype(BF16), spread, preferred_element_type=F32)
    number = lax.broadcasted_iota(jnp.int32, (rows4, span), 1)
    faces4 = 6 * (high * 8.0 + low).astype(jnp.int32) + number % 6
    for a in range(rows4):
        row_ref[0:1, a * span:(a + 1) * span] = faces4[a:a + 1, :]
    copies[1].wait()
    buckets = map_ref[...]
    digits = jnp.concatenate([(buckets & 1016).astype(F32), (buckets & 7).astype(F32)], axis=1).astype(BF16)
    step = 512
    for c in range(count // step):
        at = slice(c * step, (c + 1) * step)
        face = row_ref[0:1, at]
        hot = one_hot(face & (LANES - 1), LANES)
        value = jnp.dot(digits, jnp.concatenate([hot, hot], axis=0), preferred_element_type=F32)
        numbers = lax.broadcasted_iota(jnp.int32, (blocks, step), 0)
        bucket_ref[0:1, at] = jnp.sum(jnp.where(numbers == (face >> 7), value, 0.0), axis=0, keepdims=True)
    for copy in copies[4:]:
        copy.wait()
    away.wait()


def pieces(value):
    first = value.astype(BF16).astype(F32)
    rest = value - first
    second = rest.astype(BF16).astype(F32)
    return first, second, rest - second


def coefficient_kernel(seg_ref, left_ref, normal_ref, rows_ref):
    rows_ref[...] = jnp.zeros(rows_ref.shape, F32)
    log2e = 1.4426950408889634
    order = (0, 0, 0, 1, 1, 2)
    azimuth, polar = seg_ref[:, 3, :], seg_ref[:, 4, :]
    ring = jnp.sin(polar)
    normal = [jnp.cos(azimuth) * ring, jnp.sin(azimuth) * ring, jnp.cos(polar)]
    point = [seg_ref[:, i, :] for i in range(3)]
    along = point[0] * normal[0] + point[1] * normal[1] + point[2] * normal[2]
    square = point[0] * point[0] + point[1] * point[1] + point[2] * point[2]
    terms = (
        (0, [log2e * value for value in point]),
        (0, [-value for value in normal]),
        (6, [-DAMPING * value for value in normal]),
        (3, normal),
    )
    split = [(start, [pieces(value) for value in values]) for start, values in terms]
    constant = [pieces((-0.5 * log2e) * square), pieces(along)]
    for term in range(4):
        at = term * LANES
        start, values = split[term]
        for group, piece in enumerate(order):
            for i in range(3):
                rows_ref[:, at + group * 16 + start + i, :] = values[i][piece]
        if term < 2:
            for piece in range(3):
                rows_ref[:, at + 96 + 6 + piece, :] = constant[term][piece]
    for piece in range(3):
        rows_ref[:, 96 + piece, :] = jnp.full_like(ring, -1.0)
        rows_ref[:, 2 * LANES + 96 + 3 + piece, :] = jnp.full_like(ring, 1.0)
    for i in range(3):
        normal_ref[:, i, :] = normal[i]
    for i in range(3, 8):
        normal_ref[:, i, :] = jnp.zeros_like(ring)
    for g in range(seg_ref.shape[0]):
        for term in range(4):
            turned = rows_ref[g, term * LANES:(term + 1) * LANES, :].T.astype(BF16)
            for half in range(2):
                left_ref[g % 2, (g // 2) * 2 + half, term * 64:(term + 1) * 64, :] = turned[half * 64:(half + 1) * 64]


def pack_kernel(row_ref, bucket_ref, node_ref, out_ref, code_ref, col_ref, other_ref, rank_ref, owner_hot, geo_ref):
    group = lax.axis_index("bucket")
    count = row_ref.shape[1]
    tiles = count // LANES
    blocks = geo_ref.shape[0] // 9

    earlier = (lax.broadcasted_iota(jnp.int32, (LANES, LANES), 0)
               < lax.broadcasted_iota(jnp.int32, (LANES, LANES), 1))
    counts, picks = [], []
    for t in range(tiles):
        at = slice(t * LANES, (t + 1) * LANES)
        mine = bucket_ref[0:1, at]
        other = jnp.broadcast_to(mine, (LANES, LANES)).T
        other_ref[at, :] = other
        hit = jnp.where((other == mine) & earlier, 1.0, 0.0)
        rank_ref[0:1, at] = jnp.sum(hit, axis=0, keepdims=True)
        bucket = mine.astype(jnp.int32)
        hot = one_hot(bucket >> 3, LANES)
        owner_hot[:, at] = hot
        picks.append(lax.broadcasted_iota(jnp.int32, (16, LANES), 0) == (bucket & 7))
        inner = jnp.where(picks[t], 1.0, 0.0).astype(BF16)
        counts.append(lax.dot_general(inner, hot, NT, preferred_element_type=F32))
    before = jnp.zeros((16, LANES), F32)
    for t in range(tiles):
        at = slice(t * LANES, (t + 1) * LANES)
        if t:
            before = before + counts[t - 1]
            seen = jnp.dot(before.astype(BF16), owner_hot[:, at], preferred_element_type=F32)
            rank_ref[0:1, at] += jnp.sum(jnp.where(picks[t], seen, 0.0), axis=0, keepdims=True)

    bucket = bucket_ref[0:1, :].astype(jnp.int32)
    rank = rank_ref[0:1, :].astype(jnp.int32)
    owner = bucket >> 3
    inner = bucket & 7
    code_ref[0:1, :] = (owner & (LANES - 2)) + (inner & 1)
    code_ref[1:2, :] = ((owner & 1) * 4 + (inner >> 1)) * SLOTS + rank
    lane = lax.broadcasted_iota(jnp.int32, (1, LANES), 1)
    wanted = [(lane * 8 + group * 2 + par).astype(F32) for par in range(2)]
    pair = 2 * LANES
    sources = []
    numbers = lax.broadcasted_iota(jnp.int32, (16, pair), 0)
    for c in range(count // pair):
        at = slice(c * pair, (c + 1) * pair)
        face = row_ref[0:1, at]
        parts = jnp.where(numbers < 8, (face >> 7) + 1, face & (LANES - 1))
        left = jnp.where((numbers & 7) == rank[:, at], parts, 0).astype(F32).astype(BF16)
        other = other_ref[at, :]
        right = jnp.concatenate([jnp.where(other == want, 1.0, 0.0).astype(BF16) for want in wanted], axis=1)
        sources.append(jnp.dot(left, right, preferred_element_type=F32))
    source = functools.reduce(jnp.add, sources)

    for g in range(blocks // 16):
        row = [node_ref[pl.ds((r // 8) * blocks * 8 + r % 8 + g * 128, 16, stride=8), :] for r in range(24)]
        corner = [row[3 * m:3 * m + 3] for m in range(4)]
        motion = [row[12 + 3 * m:15 + 3 * m] for m in range(4)]
        centroid = [0.25 * (corner[0][i] + corner[1][i] + corner[2][i] + corner[3][i]) for i in range(3)]
        one = [corner[2][i] - corner[0][i] for i in range(3)]
        two = [corner[3][i] - corner[1][i] for i in range(3)]
        area = [
            0.5 * (one[1] * two[2] - one[2] * two[1]),
            0.5 * (one[2] * two[0] - one[0] * two[2]),
            0.5 * (one[0] * two[1] - one[1] * two[0]),
        ]
        velocity = [0.25 * (motion[0][i] + motion[1][i] + motion[2][i] + motion[3][i]) for i in range(3)]
        for q, value in enumerate(centroid + area + velocity):
            at = slice(q * blocks + g * 16, q * blocks + g * 16 + 16)
            first = value.astype(BF16)
            geo_ref[at, :LANES] = first
            geo_ref[at, LANES:] = (value - first.astype(F32)).astype(BF16)

    col_ref[...] = jnp.zeros(col_ref.shape, F32)
    filled = jnp.zeros((1, 256), F32)
    for k in range(SLOTS):
        high = source[k:k + 1, :].astype(jnp.int32) - 1
        low = source[8 + k:9 + k, :].astype(jnp.int32)
        filled = filled + jnp.where(high >= 0, 1.0, 0.0)
        hot = one_hot(low, LANES)
        hot = jnp.concatenate([hot, hot], axis=0)
        numbers = lax.broadcasted_iota(jnp.int32, (8, 256), 0)
        for start, end in ((0, 5), (5, 9)):
            found = jnp.dot(geo_ref[start * blocks:end * blocks, :], hot, preferred_element_type=F32)
            values = [jnp.zeros((8, 256), F32)] * (end - start)
            for h in range(0, blocks, 8):
                mine = numbers == high - h
                for i in range(end - start):
                    values[i] = jnp.where(mine, found[i * blocks + h:i * blocks + h + 8], values[i])
            for i in range(end - start):
                value = jnp.sum(values[i], axis=0, keepdims=True)
                for par in range(2):
                    row = par * 64 + k * 12 + start + i
                    col_ref[row:row + 1, :] = value[:, par * LANES:(par + 1) * LANES]
    for par in range(2):
        col_ref[par * 64 + 60:par * 64 + 61, :] = filled[:, par * LANES:(par + 1) * LANES]
    out_ref[...] = col_ref[...].T


def force_kernel(face_ref, left_ref, seg_ref, out_ref, row_ref, right_ref, wide_ref):
    half = LANES // 2
    row_ref[...] = jnp.concatenate([face_ref[pl.ds(core, half, stride=2), :] for core in range(2)], axis=0).T
    groups = seg_ref.shape[0] // 2
    for g in range(2 * groups):
        columns = seg_ref[g].T
        for i in range(3):
            wide_ref[g % 2, i, (g // 2) * LANES:(g // 2 + 1) * LANES, :] = jnp.broadcast_to(
                columns[:, i:i + 1], (LANES, LANES))
    half_log2e = 0.5 * 1.4426950408889634
    number = lax.broadcasted_iota(jnp.int32, (16, LANES), 0)
    for par in range(2):
        count = jnp.sum(row_ref[par * 64 + 60:par * 64 + 61, :], axis=1, keepdims=True)
        stiff = pieces(jnp.broadcast_to(STIFFNESS * lax.rsqrt(jnp.maximum(count, 1.0)), (1, LANES)))
        for k in range(SLOTS):
            start = par * 64 + k * 12
            face = row_ref[start:start + 16, :]
            center = [row_ref[start + i:start + i + 1, :] for i in range(3)]
            square = pieces(half_log2e * (
                center[0] * center[0] + center[1] * center[1] + center[2] * center[2]))
            extra = jnp.where((number >= 6) & (number < 9), 1.0, 0.0)
            for piece in range(3):
                extra = jnp.where(number == piece, square[piece], extra)
                extra = jnp.where(number == 3 + piece, stiff[piece], extra)
            first, second, third = pieces(face)
            blocks = (first, second, third, first, second, first, extra, jnp.zeros_like(extra))
            for group, block in enumerate(blocks):
                right_ref[par, group * 16:(group + 1) * 16, k * LANES:(k + 1) * LANES] = block.astype(BF16)
    chunks = left_ref.shape[1]
    for par in range(2):
        for first in range(0, SLOTS, 2):
            width = min(2, SLOTS - first)
            right = right_ref[par, :, first * LANES:(first + width) * LANES]
            total = [[jnp.zeros((8, LANES), F32) for i in range(3)] for k in range(width)]
            for chunk in range(chunks):
                found = jnp.dot(left_ref[par, chunk], right, preferred_element_type=F32)
                normal = [wide_ref[par, i, chunk * 64:(chunk + 1) * 64, :] for i in range(3)]
                for k in range(width):
                    at = slice(k * LANES, (k + 1) * LANES)
                    weight = jnp.exp2(found[0:64, at])
                    traction = (weight * jnp.maximum(found[64:128, at], 0.0) * found[128:192, at]
                                * jnp.abs(found[192:256, at]))
                    for i in range(3):
                        total[k][i] = total[k][i] + jnp.sum(
                            (traction * normal[i]).reshape(8, 8, LANES), axis=0)
            for k in range(width):
                for i in range(3):
                    row = par * 16 + i * SLOTS + first + k
                    row_ref[row:row + 1, :] = jnp.sum(total[k][i], axis=0, keepdims=True)
        row_ref[par * 16 + 15:par * 16 + 16, :] = jnp.zeros((1, LANES), F32)
    for core in range(2):
        at = slice(core * half, (core + 1) * half)
        both = jnp.concatenate([row_ref[0:16, at], row_ref[16:32, at]], axis=1)
        for x in range(4):
            out_ref[core * 4 + x] = both


def pick_kernel(force_ref, code_ref, out_ref, row_ref):
    turned = force_ref[...].T
    for g in range(8):
        for i in range(3):
            to, start = i * 40 + g * SLOTS, g * 16 + i * SLOTS
            row_ref[to:to + SLOTS, :] = turned[start:start + SLOTS, :]
    value = row_ref[...]
    first = value.astype(BF16)
    left = jnp.concatenate([first, (value - first.astype(F32)).astype(BF16)], axis=1)
    step = 512
    for c in range(out_ref.shape[1] // step):
        at = slice(c * step, (c + 1) * step)
        hot = one_hot(code_ref[0:1, at], LANES)
        found = jnp.dot(left, jnp.concatenate([hot, hot], axis=0), preferred_element_type=F32)
        mine = lax.broadcasted_iota(jnp.int32, (40, step), 0) == code_ref[1:2, at]
        for i in range(3):
            out_ref[i:i + 1, at] = jnp.sum(
                jnp.where(mine, found[i * 40:(i + 1) * 40], 0.0), axis=0, keepdims=True)


def local(node_data, eroded, bucket_map, seg_point, seg_angle):
    owners = lax.axis_size(("chip", "core"))
    groups = lax.axis_size("bucket")
    faces = node_data.shape[1]
    blocks = faces // LANES
    uncovered = 6 * eroded.shape[0]
    vmem = pl.BlockSpec(memory_space=pltpu.VMEM)
    anywhere = pl.BlockSpec(memory_space=pl.ANY)

    node_tiles = node_data.reshape(3, 8, blocks, LANES).transpose(0, 2, 1, 3).reshape(24 * blocks, LANES)
    buckets, width = seg_point.shape[0], seg_point.shape[2]
    segs, node, row, bucket = pl.pallas_call(
        start_kernel,
        out_shape=(
            jax.ShapeDtypeStruct((buckets, 5, width), F32),
            pltpu.VMEM((24 * blocks, LANES), F32),
            pltpu.VMEM((1, uncovered), jnp.int32),
            pltpu.VMEM((1, uncovered), F32),
        ),
        in_specs=[anywhere] * 5,
        out_specs=(anywhere, vmem, vmem, vmem),
        scratch_shapes=[
            pltpu.VMEM((3, buckets, width), F32),
            pltpu.VMEM(seg_angle.shape, F32),
            pltpu.VMEM((uncovered // 6 // LANES, LANES), jnp.int32),
            pltpu.VMEM((blocks, LANES), jnp.int32),
            pltpu.VMEM((buckets, 5, width), F32),
            pltpu.SemaphoreType.DMA((8,)),
        ],
        name="start",
    )(seg_point.transpose(1, 0, 2), seg_angle, eroded.reshape(-1, LANES), bucket_map.reshape(blocks, LANES), node_tiles)
    segs = lax.all_to_all(segs, "bucket", 0, 0, tiled=True)

    packed, code = pl.pallas_call(
        pack_kernel,
        out_shape=(pltpu.VMEM((owners, LANES), F32), pltpu.VMEM((2, uncovered), jnp.int32)),
        in_specs=[vmem] * 3,
        out_specs=(vmem, vmem),
        scratch_shapes=[
            pltpu.VMEM((LANES, owners), F32),
            pltpu.VMEM((uncovered, LANES), F32),
            pltpu.VMEM((1, uncovered), F32),
            pltpu.VMEM((LANES, uncovered), BF16),
            pltpu.VMEM((9 * blocks, 2 * LANES), BF16),
        ],
        name="pack",
    )(near(row), near(bucket), near(node))

    with jax.named_scope("coefficients"):
        left, normal = pl.pallas_call(
            coefficient_kernel,
            out_shape=(
                pltpu.VMEM((2, 2 * groups, 256, LANES), BF16),
                pltpu.VMEM((2 * groups, 8, LANES), F32),
            ),
            in_specs=[vmem],
            out_specs=(vmem, vmem),
            scratch_shapes=[pltpu.VMEM((2 * groups, 4 * LANES, LANES), F32)],
            name="coefficients",
        )(near(segs))

    packed, left, normal = lax.optimization_barrier((packed, left, normal))
    with jax.named_scope("dispatch"):
        arrived = lax.all_to_all(packed.reshape(owners, 1, LANES), ("chip", "core"), 0, 0, tiled=True)

    force = pl.pallas_call(
        force_kernel,
        out_shape=pltpu.VMEM((2 * groups, 16, LANES), F32),
        in_specs=[vmem, vmem, vmem],
        out_specs=vmem,
        scratch_shapes=[
            pltpu.VMEM((LANES, LANES), F32),
            pltpu.VMEM((2, LANES, SLOTS * LANES), BF16),
            pltpu.VMEM((2, 3, groups * LANES, LANES), F32),
        ],
        name="force",
    )(near(arrived.reshape(owners, LANES)), near(left), near(normal))

    shared = lax.all_to_all(force, ("core", "bucket"), 0, 0, tiled=True)
    outgoing = shared.reshape(groups * 32, 2, owners // 2).transpose(2, 1, 0)
    returned = lax.all_to_all(outgoing, "chip", 0, 0, tiled=True)

    return pl.pallas_call(
        pick_kernel,
        out_shape=jax.ShapeDtypeStruct((3, uncovered), F32),
        in_specs=[vmem, vmem],
        out_specs=vmem,
        scratch_shapes=[pltpu.VMEM((120, LANES), F32)],
        name="pick",
    )(near(returned.reshape(owners, LANES)), near(code))


def solution(mesh):
    split = Mesh(mesh.devices.reshape(-1, 2, mesh.shape["bucket"]), ("chip", "core", "bucket"))
    elem = ("chip", "core")
    in_specs = (P(None, elem), P(elem), P(elem), P(elem, None, "bucket"), P(elem, None, "bucket"))
    return jax.shard_map(local, mesh=split, in_specs=in_specs, out_specs=P(None, elem), check_vma=False)
```

```python
import functools

import jax
import jax.numpy as jnp
from jax import lax
from jax.experimental import pallas as pl
from jax.experimental.pallas import tpu as pltpu
from jax.sharding import Mesh, PartitionSpec as P

STIFFNESS = 20.0
DAMPING = 0.5
SLOTS = 5
LANES = 128
F32 = jnp.float32
BF16 = jnp.bfloat16
NT = (((1,), (1,)), ((), ()))


def near(value):
    return pltpu.with_memory_space_constraint(value, pltpu.VMEM)


def one_hot(row, size):
    numbers = lax.broadcasted_iota(jnp.int32, (size, row.shape[1]), 0)
    return jnp.where(numbers == row, 1.0, 0.0).astype(BF16)


def start_kernel(point_hbm, angle_hbm, eroded_hbm, map_hbm, node_hbm, out_hbm, node_ref, row_ref, bucket_ref, point_ref,
                 angle_ref, eroded_ref, map_ref, out_ref, sem):
    part = node_ref.shape[0] // 3
    pairs = [(point_hbm, point_ref), (angle_hbm, angle_ref), (eroded_hbm, eroded_ref), (map_hbm, map_ref)]
    for i in range(3):
        at = pl.ds(i * part, part)
        pairs.append((node_hbm.at[at, :], node_ref.at[at, :]))
    copies = [pltpu.make_async_copy(source, target, sem.at[i]) for i, (source, target) in enumerate(pairs)]
    for copy in copies:
        copy.start()

    copies[0].wait()
    copies[1].wait()
    for i in range(3):
        out_ref[:, i, :] = point_ref[i]
    for i in range(2):
        out_ref[:, 3 + i, :] = angle_ref[:, i, :]
    away = pltpu.make_async_copy(out_ref, out_hbm, sem.at[7])
    away.start()
    copies[2].wait()
    blocks = map_ref.shape[0]
    count = row_ref.shape[1]
    rows4 = eroded_ref.shape[0]
    span = count // rows4

    eroded = eroded_ref[...]
    lane = lax.broadcasted_iota(jnp.int32, (LANES, span), 1)
    six = 6 * lax.broadcasted_iota(jnp.int32, (LANES, span), 0)
    spread = jnp.where((lane >= six) & (lane < six + 6), 1.0, 0.0).astype(BF16)
    high = jnp.dot((eroded >> 3).astype(F32).astype(BF16), spread, preferred_element_type=F32)
    low = jnp.dot((eroded & 7).astype(F32).astype(BF16), spread, preferred_element_type=F32)
    number = lax.broadcasted_iota(jnp.int32, (rows4, span), 1)
    faces4 = 6 * (high * 8.0 + low).astype(jnp.int32) + number % 6
    for a in range(rows4):
        row_ref[0:1, a * span:(a + 1) * span] = faces4[a:a + 1, :]
    copies[3].wait()
    buckets = map_ref[...]
    digits = jnp.concatenate([(buckets & 1016).astype(F32), (buckets & 7).astype(F32)], axis=1).astype(BF16)
    step = 512
    for c in range(count // step):
        at = slice(c * step, (c + 1) * step)
        face = row_ref[0:1, at]
        hot = one_hot(face & (LANES - 1), LANES)
        value = jnp.dot(digits, jnp.concatenate([hot, hot], axis=0), preferred_element_type=F32)
        numbers = lax.broadcasted_iota(jnp.int32, (blocks, step), 0)
        bucket_ref[0:1, at] = jnp.sum(jnp.where(numbers == (face >> 7), value, 0.0), axis=0, keepdims=True)
    for copy in copies[4:]:
        copy.wait()
    away.wait()


def pieces(value):
    first = value.astype(BF16).astype(F32)
    rest = value - first
    second = rest.astype(BF16).astype(F32)
    return first, second, rest - second


def coefficient_kernel(seg_ref, left_ref, normal_ref, rows_ref):
    rows_ref[...] = jnp.zeros(rows_ref.shape, F32)
    log2e = 1.4426950408889634
    order = (0, 0, 0, 1, 1, 2)
    azimuth, polar = seg_ref[:, 3, :], seg_ref[:, 4, :]
    ring = jnp.sin(polar)
    normal = [jnp.cos(azimuth) * ring, jnp.sin(azimuth) * ring, jnp.cos(polar)]
    point = [seg_ref[:, i, :] for i in range(3)]
    along = point[0] * normal[0] + point[1] * normal[1] + point[2] * normal[2]
    square = point[0] * point[0] + point[1] * point[1] + point[2] * point[2]
    terms = (
        (0, [log2e * value for value in point]),
        (0, [-value for value in normal]),
        (6, [-DAMPING * value for value in normal]),
        (3, normal),
    )
    split = [(start, [pieces(value) for value in values]) for start, values in terms]
    constant = [pieces((-0.5 * log2e) * square), pieces(along)]
    for term in range(4):
        at = term * LANES
        start, values = split[term]
        for group, piece in enumerate(order):
            for i in range(3):
                rows_ref[:, at + group * 16 + start + i, :] = values[i][piece]
        if term < 2:
            for piece in range(3):
                rows_ref[:, at + 96 + 6 + piece, :] = constant[term][piece]
    for piece in range(3):
        rows_ref[:, 96 + piece, :] = jnp.full_like(ring, -1.0)
        rows_ref[:, 2 * LANES + 96 + 3 + piece, :] = jnp.full_like(ring, 1.0)
    for i in range(3):
        normal_ref[:, i, :] = normal[i]
    for i in range(3, 8):
        normal_ref[:, i, :] = jnp.zeros_like(ring)
    for g in range(seg_ref.shape[0]):
        for term in range(4):
            turned = rows_ref[g, term * LANES:(term + 1) * LANES, :].T.astype(BF16)
            for half in range(2):
                left_ref[g % 2, (g // 2) * 2 + half, term * 64:(term + 1) * 64, :] = turned[half * 64:(half + 1) * 64]


def pack_kernel(row_ref, bucket_ref, node_ref, out_ref, code_ref, col_ref, other_ref, rank_ref, owner_hot, geo_ref):
    group = lax.axis_index("bucket")
    count = row_ref.shape[1]
    tiles = count // LANES
    blocks = geo_ref.shape[0] // 9

    earlier = (lax.broadcasted_iota(jnp.int32, (LANES, LANES), 0)
               < lax.broadcasted_iota(jnp.int32, (LANES, LANES), 1))
    counts, picks = [], []
    for t in range(tiles):
        at = slice(t * LANES, (t + 1) * LANES)
        mine = bucket_ref[0:1, at]
        other = jnp.broadcast_to(mine, (LANES, LANES)).T
        other_ref[at, :] = other
        hit = jnp.where((other == mine) & earlier, 1.0, 0.0)
        rank_ref[0:1, at] = jnp.sum(hit, axis=0, keepdims=True)
        bucket = mine.astype(jnp.int32)
        hot = one_hot(bucket >> 3, LANES)
        owner_hot[:, at] = hot
        picks.append(lax.broadcasted_iota(jnp.int32, (16, LANES), 0) == (bucket & 7))
        inner = jnp.where(picks[t], 1.0, 0.0).astype(BF16)
        counts.append(lax.dot_general(inner, hot, NT, preferred_element_type=F32))
    before = jnp.zeros((16, LANES), F32)
    for t in range(tiles):
        at = slice(t * LANES, (t + 1) * LANES)
        if t:
            before = before + counts[t - 1]
            seen = jnp.dot(before.astype(BF16), owner_hot[:, at], preferred_element_type=F32)
            rank_ref[0:1, at] += jnp.sum(jnp.where(picks[t], seen, 0.0), axis=0, keepdims=True)

    bucket = bucket_ref[0:1, :].astype(jnp.int32)
    rank = rank_ref[0:1, :].astype(jnp.int32)
    owner = bucket >> 3
    inner = bucket & 7
    code_ref[0:1, :] = (owner & (LANES - 2)) + (inner & 1)
    code_ref[1:2, :] = ((owner & 1) * 4 + (inner >> 1)) * SLOTS + rank
    lane = lax.broadcasted_iota(jnp.int32, (1, LANES), 1)
    wanted = [(lane * 8 + group * 2 + par).astype(F32) for par in range(2)]
    pair = 2 * LANES
    sources = []
    numbers = lax.broadcasted_iota(jnp.int32, (16, pair), 0)
    for c in range(count // pair):
        at = slice(c * pair, (c + 1) * pair)
        face = row_ref[0:1, at]
        parts = jnp.where(numbers < 8, (face >> 7) + 1, face & (LANES - 1))
        left = jnp.where((numbers & 7) == rank[:, at], parts, 0).astype(F32).astype(BF16)
        other = other_ref[at, :]
        right = jnp.concatenate([jnp.where(other == want, 1.0, 0.0).astype(BF16) for want in wanted], axis=1)
        sources.append(jnp.dot(left, right, preferred_element_type=F32))
    source = functools.reduce(jnp.add, sources)

    for g in range(blocks // 16):
        row = [node_ref[pl.ds((r // 8) * blocks * 8 + r % 8 + g * 128, 16, stride=8), :] for r in range(24)]
        corner = [row[3 * m:3 * m + 3] for m in range(4)]
        motion = [row[12 + 3 * m:15 + 3 * m] for m in range(4)]
        centroid = [0.25 * (corner[0][i] + corner[1][i] + corner[2][i] + corner[3][i]) for i in range(3)]
        one = [corner[2][i] - corner[0][i] for i in range(3)]
        two = [corner[3][i] - corner[1][i] for i in range(3)]
        area = [
            0.5 * (one[1] * two[2] - one[2] * two[1]),
            0.5 * (one[2] * two[0] - one[0] * two[2]),
            0.5 * (one[0] * two[1] - one[1] * two[0]),
        ]
        velocity = [0.25 * (motion[0][i] + motion[1][i] + motion[2][i] + motion[3][i]) for i in range(3)]
        for q, value in enumerate(centroid + area + velocity):
            at = slice(q * blocks + g * 16, q * blocks + g * 16 + 16)
            first = value.astype(BF16)
            geo_ref[at, :LANES] = first
            geo_ref[at, LANES:] = (value - first.astype(F32)).astype(BF16)

    col_ref[...] = jnp.zeros(col_ref.shape, F32)
    filled = jnp.zeros((1, 256), F32)
    for k in range(SLOTS):
        high = source[k:k + 1, :].astype(jnp.int32) - 1
        low = source[8 + k:9 + k, :].astype(jnp.int32)
        filled = filled + jnp.where(high >= 0, 1.0, 0.0)
        hot = one_hot(low, LANES)
        hot = jnp.concatenate([hot, hot], axis=0)
        numbers = lax.broadcasted_iota(jnp.int32, (8, 256), 0)
        for start, end in ((0, 5), (5, 9)):
            found = jnp.dot(geo_ref[start * blocks:end * blocks, :], hot, preferred_element_type=F32)
            values = [jnp.zeros((8, 256), F32)] * (end - start)
            for h in range(0, blocks, 8):
                mine = numbers == high - h
                for i in range(end - start):
                    values[i] = jnp.where(mine, found[i * blocks + h:i * blocks + h + 8], values[i])
            for i in range(end - start):
                value = jnp.sum(values[i], axis=0, keepdims=True)
                for par in range(2):
                    row = par * 64 + k * 12 + start + i
                    col_ref[row:row + 1, :] = value[:, par * LANES:(par + 1) * LANES]
    for par in range(2):
        col_ref[par * 64 + 60:par * 64 + 61, :] = filled[:, par * LANES:(par + 1) * LANES]
    out_ref[...] = col_ref[...].T


def force_kernel(face_ref, left_ref, seg_ref, out_ref, row_ref, right_ref, wide_ref):
    half = LANES // 2
    row_ref[...] = jnp.concatenate([face_ref[pl.ds(core, half, stride=2), :] for core in range(2)], axis=0).T
    groups = seg_ref.shape[0] // 2
    for g in range(2 * groups):
        columns = seg_ref[g].T
        for i in range(3):
            wide_ref[g % 2, i, (g // 2) * LANES:(g // 2 + 1) * LANES, :] = jnp.broadcast_to(
                columns[:, i:i + 1], (LANES, LANES))
    half_log2e = 0.5 * 1.4426950408889634
    number = lax.broadcasted_iota(jnp.int32, (16, LANES), 0)
    for par in range(2):
        count = jnp.sum(row_ref[par * 64 + 60:par * 64 + 61, :], axis=1, keepdims=True)
        stiff = pieces(jnp.broadcast_to(STIFFNESS * lax.rsqrt(jnp.maximum(count, 1.0)), (1, LANES)))
        for k in range(SLOTS):
            start = par * 64 + k * 12
            face = row_ref[start:start + 16, :]
            center = [row_ref[start + i:start + i + 1, :] for i in range(3)]
            square = pieces(half_log2e * (
                center[0] * center[0] + center[1] * center[1] + center[2] * center[2]))
            extra = jnp.where((number >= 6) & (number < 9), 1.0, 0.0)
            for piece in range(3):
                extra = jnp.where(number == piece, square[piece], extra)
                extra = jnp.where(number == 3 + piece, stiff[piece], extra)
            first, second, third = pieces(face)
            blocks = (first, second, third, first, second, first, extra, jnp.zeros_like(extra))
            for group, block in enumerate(blocks):
                right_ref[par, group * 16:(group + 1) * 16, k * LANES:(k + 1) * LANES] = block.astype(BF16)
    chunks = left_ref.shape[1]
    for par in range(2):
        for first in range(0, SLOTS, 2):
            width = min(2, SLOTS - first)
            right = right_ref[par, :, first * LANES:(first + width) * LANES]
            total = [[jnp.zeros((8, LANES), F32) for i in range(3)] for k in range(width)]
            for chunk in range(chunks):
                found = jnp.dot(left_ref[par, chunk], right, preferred_element_type=F32)
                normal = [wide_ref[par, i, chunk * 64:(chunk + 1) * 64, :] for i in range(3)]
                for k in range(width):
                    at = slice(k * LANES, (k + 1) * LANES)
                    weight = jnp.exp2(found[0:64, at])
                    traction = (weight * jnp.maximum(found[64:128, at], 0.0) * found[128:192, at]
                                * jnp.abs(found[192:256, at]))
                    for i in range(3):
                        total[k][i] = total[k][i] + jnp.sum(
                            (traction * normal[i]).reshape(8, 8, LANES), axis=0)
            for k in range(width):
                for i in range(3):
                    row = par * 16 + i * SLOTS + first + k
                    row_ref[row:row + 1, :] = jnp.sum(total[k][i], axis=0, keepdims=True)
        row_ref[par * 16 + 15:par * 16 + 16, :] = jnp.zeros((1, LANES), F32)
    for core in range(2):
        at = slice(core * half, (core + 1) * half)
        both = jnp.concatenate([row_ref[0:16, at], row_ref[16:32, at]], axis=1)
        for x in range(4):
            out_ref[core * 4 + x] = both


def pick_kernel(force_ref, code_ref, out_ref, row_ref):
    turned = force_ref[...].T
    for g in range(8):
        for i in range(3):
            to, start = i * 40 + g * SLOTS, g * 16 + i * SLOTS
            row_ref[to:to + SLOTS, :] = turned[start:start + SLOTS, :]
    value = row_ref[...]
    first = value.astype(BF16)
    left = jnp.concatenate([first, (value - first.astype(F32)).astype(BF16)], axis=1)
    step = 512
    for c in range(out_ref.shape[1] // step):
        at = slice(c * step, (c + 1) * step)
        hot = one_hot(code_ref[0:1, at], LANES)
        found = jnp.dot(left, jnp.concatenate([hot, hot], axis=0), preferred_element_type=F32)
        mine = lax.broadcasted_iota(jnp.int32, (40, step), 0) == code_ref[1:2, at]
        for i in range(3):
            out_ref[i:i + 1, at] = jnp.sum(
                jnp.where(mine, found[i * 40:(i + 1) * 40], 0.0), axis=0, keepdims=True)


def local(node_data, eroded, bucket_map, seg_point, seg_angle):
    owners = lax.axis_size(("chip", "core"))
    groups = lax.axis_size("bucket")
    faces = node_data.shape[1]
    blocks = faces // LANES
    uncovered = 6 * eroded.shape[0]
    vmem = pl.BlockSpec(memory_space=pltpu.VMEM)
    anywhere = pl.BlockSpec(memory_space=pl.ANY)

    node_tiles = node_data.reshape(3, 8, blocks, LANES).transpose(0, 2, 1, 3).reshape(24 * blocks, LANES)
    buckets, width = seg_point.shape[0], seg_point.shape[2]
    segs, node, row, bucket = pl.pallas_call(
        start_kernel,
        out_shape=(
            jax.ShapeDtypeStruct((buckets, 5, width), F32),
            pltpu.VMEM((24 * blocks, LANES), F32),
            pltpu.VMEM((1, uncovered), jnp.int32),
            pltpu.VMEM((1, uncovered), F32),
        ),
        in_specs=[anywhere] * 5,
        out_specs=(anywhere, vmem, vmem, vmem),
        scratch_shapes=[
            pltpu.VMEM((3, buckets, width), F32),
            pltpu.VMEM(seg_angle.shape, F32),
            pltpu.VMEM((uncovered // 6 // LANES, LANES), jnp.int32),
            pltpu.VMEM((blocks, LANES), jnp.int32),
            pltpu.VMEM((buckets, 5, width), F32),
            pltpu.SemaphoreType.DMA((8,)),
        ],
        name="start",
    )(seg_point.transpose(1, 0, 2), seg_angle, eroded.reshape(-1, LANES), bucket_map.reshape(blocks, LANES), node_tiles)
    segs = lax.all_to_all(segs, "bucket", 0, 0, tiled=True)

    packed, code = pl.pallas_call(
        pack_kernel,
        out_shape=(jax.ShapeDtypeStruct((owners, LANES), F32), pltpu.VMEM((2, uncovered), jnp.int32)),
        in_specs=[vmem] * 3,
        out_specs=(vmem, vmem),
        scratch_shapes=[
            pltpu.VMEM((LANES, owners), F32),
            pltpu.VMEM((uncovered, LANES), F32),
            pltpu.VMEM((1, uncovered), F32),
            pltpu.VMEM((LANES, uncovered), BF16),
            pltpu.VMEM((9 * blocks, 2 * LANES), BF16),
        ],
        name="pack",
    )(near(row), near(bucket), near(node))

    with jax.named_scope("dispatch"):
        arrived = lax.all_to_all(packed.reshape(owners, 1, LANES), ("chip", "core"), 0, 0, tiled=True)

    with jax.named_scope("coefficients"):
        left, normal = pl.pallas_call(
            coefficient_kernel,
            out_shape=(
                pltpu.VMEM((2, 2 * groups, 256, LANES), BF16),
                pltpu.VMEM((2 * groups, 8, LANES), F32),
            ),
            in_specs=[vmem],
            out_specs=(vmem, vmem),
            scratch_shapes=[pltpu.VMEM((2 * groups, 4 * LANES, LANES), F32)],
            name="coefficients",
        )(near(segs))

    force = pl.pallas_call(
        force_kernel,
        out_shape=pltpu.VMEM((2 * groups, 16, LANES), F32),
        in_specs=[vmem, vmem, vmem],
        out_specs=vmem,
        scratch_shapes=[
            pltpu.VMEM((LANES, LANES), F32),
            pltpu.VMEM((2, LANES, SLOTS * LANES), BF16),
            pltpu.VMEM((2, 3, groups * LANES, LANES), F32),
        ],
        name="force",
    )(near(arrived.reshape(owners, LANES)), near(left), near(normal))

    shared = lax.all_to_all(force, ("core", "bucket"), 0, 0, tiled=True)
    outgoing = shared.reshape(groups * 32, 2, owners // 2).transpose(2, 1, 0)
    returned = lax.all_to_all(outgoing, "chip", 0, 0, tiled=True)

    return pl.pallas_call(
        pick_kernel,
        out_shape=jax.ShapeDtypeStruct((3, uncovered), F32),
        in_specs=[vmem, vmem],
        out_specs=vmem,
        scratch_shapes=[pltpu.VMEM((120, LANES), F32)],
        name="pick",
    )(near(returned.reshape(owners, LANES)), near(code))


def solution(mesh):
    split = Mesh(mesh.devices.reshape(-1, 2, mesh.shape["bucket"]), ("chip", "core", "bucket"))
    elem = ("chip", "core")
    in_specs = (P(None, elem), P(elem), P(elem), P(elem, None, "bucket"), P(elem, None, "bucket"))
    return jax.shard_map(local, mesh=split, in_specs=in_specs, out_specs=P(None, elem), check_vma=False)
```
